8 devices in a mesh: fsdp: 8 (over z, y, x, core).
Axes of the slice: x: 2, y: 2, z: 1, core: 2. Of those that a mesh axis runs over, the one named last changes fastest.
Arguments:
- tok_ids: int32 [32768], P('fsdp')
- tok_labels: int32 [32768], P('fsdp')
- loss_mask: int32 [32768], P('fsdp')
- emb_table: bfloat16 [4096, 512], P('fsdp')
- gain_mlp: float32 [512], replicated
- gain_head: float32 [512], replicated
- w_gate: bfloat16 [512, 1792], P('fsdp')
- w_up: bfloat16 [512, 1792], P('fsdp')
- w_down: bfloat16 [1792, 512], P('fsdp')
Outputs:
- output 1: float32 [], replicated
- output 2: float32 [4096, 512], P('fsdp')
- output 3: float32 [512, 1792], P('fsdp')
- output 4: float32 [512, 1792], P('fsdp')
- output 5: float32 [1792, 512], P('fsdp')
All inputs are finite; a program needn't handle non-finite values.
Results may differ from the reference program's by a relative error of at most 0.00735108.
Values are sent between devices in bfloat16 or wider.
A program may use at most 1 GiB of HBM per device.

```python
import jax
import jax.numpy as jnp
from jax import lax

VOCAB = 4096
D_MODEL = 512
D_FF = 1792
TOK_DEV = 4096
GROUP_SIZE = 8
T_GLOBAL = TOK_DEV * GROUP_SIZE
NORM_EPS = 1e-6
ROW_CONTRACT = (((1,), (1,)), ((), ()))
TOK_CONTRACT = (((0,), (0,)), ((), ()))


def draw_tokens(tok_key):
    key_ids, key_lab, key_pad, key_cut = jax.random.split(tok_key, 4)
    tok_ids = jax.random.randint(key_ids, (T_GLOBAL,), 0, VOCAB, dtype=jnp.int32)
    tok_ids = tok_ids.at[0].set(0).at[1].set(VOCAB - 1)
    tok_labels = jax.random.randint(key_lab, (T_GLOBAL,), 0, VOCAB, dtype=jnp.int32)
    tok_labels = tok_labels.at[0].set(VOCAB - 1).at[1].set(0)
    pad_len = jax.random.randint(key_pad, (GROUP_SIZE, 1), 0, TOK_DEV // 2 + 1, dtype=jnp.int32)
    keep_tail = jnp.arange(TOK_DEV)[None, :] < TOK_DEV - pad_len
    cut_draw = jax.random.randint(key_cut, (GROUP_SIZE, TOK_DEV), 0, 16, dtype=jnp.int32)
    loss_mask = (keep_tail & (cut_draw != 0)).astype(jnp.int32).reshape(T_GLOBAL)
    return tok_ids, tok_labels, loss_mask.at[0].set(1)


def setup_inputs(seed: int = 0) -> dict:
    root_key = jax.random.key(seed)
    key_tok, key_emb, key_g1, key_g2, key_gate, key_up, key_down = jax.random.split(root_key, 7)
    tok_ids, tok_labels, loss_mask = draw_tokens(key_tok)
    emb_table = (jax.random.normal(key_emb, (VOCAB, D_MODEL), jnp.float32) * D_MODEL ** -0.5).astype(jnp.bfloat16)
    gain_mlp = 1.0 + 0.5 * jax.random.normal(key_g1, (D_MODEL,), jnp.float32)
    gain_head = 1.0 + 0.5 * jax.random.normal(key_g2, (D_MODEL,), jnp.float32)
    w_gate = (jax.random.normal(key_gate, (D_MODEL, D_FF), jnp.float32) * D_MODEL ** -0.5).astype(jnp.bfloat16)
    w_up = (jax.random.normal(key_up, (D_MODEL, D_FF), jnp.float32) * D_MODEL ** -0.5).astype(jnp.bfloat16)
    w_down = (jax.random.normal(key_down, (D_FF, D_MODEL), jnp.float32) * 1.5 * (D_FF * D_MODEL) ** -0.5).astype(jnp.bfloat16)
    return {"tok_ids": tok_ids, "tok_labels": tok_labels, "loss_mask": loss_mask, "emb_table": emb_table, "gain_mlp": gain_mlp, "gain_head": gain_head, "w_gate": w_gate, "w_up": w_up, "w_down": w_down}


def rms_scale(rows_wide, norm_gain):
    inv_rms = lax.rsqrt(jnp.mean(rows_wide * rows_wide, axis=-1, keepdims=True) + NORM_EPS)
    return (rows_wide * inv_rms * norm_gain).astype(jnp.bfloat16), inv_rms


def rms_back(rows_wide, inv_rms, norm_gain, grad_out):
    scaled_grad = grad_out * norm_gain
    return inv_rms * (scaled_grad - rows_wide * (inv_rms * inv_rms) * jnp.mean(scaled_grad * rows_wide, axis=-1, keepdims=True))


def mlp_forward(emb_rows, gain_mlp, gain_head, w_gate, w_up, w_down):
    emb_wide = emb_rows.astype(jnp.float32)
    a_norm, inv_first = rms_scale(emb_wide, gain_mlp)
    gate_wide = jnp.dot(a_norm, w_gate, preferred_element_type=jnp.float32).astype(jnp.bfloat16).astype(jnp.float32)
    up_wide = jnp.dot(a_norm, w_up, preferred_element_type=jnp.float32).astype(jnp.bfloat16).astype(jnp.float32)
    gate_sig = jax.nn.sigmoid(gate_wide)
    act_rows = (gate_wide * gate_sig * up_wide).astype(jnp.bfloat16)
    hid_wide = (emb_wide + jnp.dot(act_rows, w_down, preferred_element_type=jnp.float32)).astype(jnp.bfloat16).astype(jnp.float32)
    h_norm, inv_second = rms_scale(hid_wide, gain_head)
    return (emb_wide, inv_first, a_norm, gate_wide, up_wide, gate_sig, act_rows, hid_wide, inv_second), h_norm


def head_forward(h_norm, emb_table, tok_labels, tok_coef):
    logits = lax.dot_general(h_norm, emb_table, ROW_CONTRACT, preferred_element_type=jnp.float32)
    row_max = jnp.max(logits, axis=-1, keepdims=True)
    exp_rows = jnp.exp(logits - row_max)
    sum_exp = jnp.sum(exp_rows, axis=-1, keepdims=True)
    is_label = jnp.arange(logits.shape[1])[None, :] == tok_labels[:, None]
    picked = jnp.sum(jnp.where(is_label, logits, 0.0), axis=-1)
    tok_loss = row_max[:, 0] + jnp.log(sum_exp[:, 0]) - picked
    d_logits = ((exp_rows / sum_exp - is_label.astype(jnp.float32)) * tok_coef[:, None]).astype(jnp.bfloat16)
    return jnp.sum(tok_coef * tok_loss), d_logits


def mlp_backward(saved, d_hidden, gain_mlp, w_gate, w_up, w_down):
    emb_wide, inv_first, a_norm, gate_wide, up_wide, gate_sig, act_rows = saved[:7]
    hid_grad = d_hidden.astype(jnp.bfloat16)
    d_act = lax.dot_general(hid_grad, w_down, ROW_CONTRACT, preferred_element_type=jnp.float32)
    grad_down = lax.dot_general(act_rows, hid_grad, TOK_CONTRACT, preferred_element_type=jnp.float32)
    d_up = (d_act * gate_wide * gate_sig).astype(jnp.bfloat16)
    d_gate = (d_act * up_wide * gate_sig * (1.0 + gate_wide * (1.0 - gate_sig))).astype(jnp.bfloat16)
    grad_gate = lax.dot_general(a_norm, d_gate, TOK_CONTRACT, preferred_element_type=jnp.float32)
    grad_up = lax.dot_general(a_norm, d_up, TOK_CONTRACT, preferred_element_type=jnp.float32)
    d_anorm = lax.dot_general(d_gate, w_gate, ROW_CONTRACT, preferred_element_type=jnp.float32) + lax.dot_general(d_up, w_up, ROW_CONTRACT, preferred_element_type=jnp.float32)
    grad_x = d_hidden + rms_back(emb_wide, inv_first, gain_mlp, d_anorm)
    return grad_x, grad_gate, grad_up, grad_down


def block_grads(tok_ids, tok_labels, tok_coef, emb_table, gain_mlp, gain_head, w_gate, w_up, w_down):
    saved, h_norm = mlp_forward(jnp.take(emb_table, tok_ids, axis=0), gain_mlp, gain_head, w_gate, w_up, w_down)
    loss_part, d_logits = head_forward(h_norm, emb_table, tok_labels, tok_coef)
    d_hnorm = jnp.dot(d_logits, emb_table, preferred_element_type=jnp.float32)
    head_grad = lax.dot_general(d_logits, h_norm, TOK_CONTRACT, preferred_element_type=jnp.float32)
    d_hidden = rms_back(saved[7], saved[8], gain_head, d_hnorm)
    grad_x, grad_gate, grad_up, grad_down = mlp_backward(saved, d_hidden, gain_mlp, w_gate, w_up, w_down)
    grad_table = head_grad + jax.ops.segment_sum(grad_x, tok_ids, num_segments=emb_table.shape[0])
    return loss_part, grad_table, grad_gate, grad_up, grad_down


def reference(tok_ids, tok_labels, loss_mask, emb_table, gain_mlp, gain_head, w_gate, w_up, w_down):
    mask_wide = loss_mask.astype(jnp.float32)
    tok_coef = (mask_wide / jnp.sum(mask_wide)).reshape(GROUP_SIZE, TOK_DEV)

    def scan_step(acc_state, block_in):
        step_out = block_grads(block_in[0], block_in[1], block_in[2], emb_table, gain_mlp, gain_head, w_gate, w_up, w_down)
        return tuple(prev_val + new_val for prev_val, new_val in zip(acc_state, step_out)), None

    init_state = (jnp.zeros((), jnp.float32), jnp.zeros((VOCAB, D_MODEL), jnp.float32), jnp.zeros((D_MODEL, D_FF), jnp.float32), jnp.zeros((D_MODEL, D_FF), jnp.float32), jnp.zeros((D_FF, D_MODEL), jnp.float32))
    blocks = (tok_ids.reshape(GROUP_SIZE, TOK_DEV), tok_labels.reshape(GROUP_SIZE, TOK_DEV), tok_coef)
    final_state, _ = lax.scan(scan_step, init_state, blocks)
    loss_val, grad_table, grad_gate, grad_up, grad_down = final_state
    return (loss_val, grad_table, grad_gate, grad_up, grad_down)
```

```python
import functools

import jax
import jax.numpy as jnp
from jax import lax
from jax.experimental import pallas as pl
from jax.experimental.pallas import tpu as pltpu
from jax.sharding import PartitionSpec as P


NORM_EPS = 1e-6
N_DEV = 8
F32, BF16, I32 = jnp.float32, jnp.bfloat16, jnp.int32
MESH = pl.DeviceIdType.MESH
VMEM_MAX = 66_000_000


def dot_nn(a, b):
    return jnp.dot(a, b, preferred_element_type=F32)


def dot_nt(a, b):
    return lax.dot_general(a, b, (((1,), (1,)), ((), ())), preferred_element_type=F32)


def dot_tn(a, b):
    return lax.dot_general(a, b, (((0,), (0,)), ((), ())), preferred_element_type=F32)


def flip(me, bit):
    return me + bit - 2 * bit * lax.rem(me // bit, 2)


def barrier_with(peers):
    sem = pltpu.get_barrier_semaphore()
    for peer in peers:
        pl.semaphore_signal(sem, inc=1, device_id=(peer,), device_id_type=MESH)
    pl.semaphore_wait(sem, len(peers))


class Gather:
    def __init__(self, slot, half, send_sem, recv_sem, me, own=None):
        self.slot, self.half, self.ss, self.rs, self.me = slot, half, send_sem, recv_sem, me
        self.own = slot(me) if own is None else own
        self.pc, self.px, self.py = flip(me, 1), flip(me, 2), flip(me, 4)
        self.pd = flip(self.px, 4)

    def copy(self, kind, src, dst, peer):
        return pltpu.make_async_remote_copy(
            src_ref=src, dst_ref=dst, send_sem=self.ss(kind), recv_sem=self.rs(kind), device_id=(peer,), device_id_type=MESH
        )

    def describe(self, kind):
        me, px, py, pd, pc = self.me, self.px, self.py, self.pd, self.pc
        if kind == 0:
            return self.copy(0, self.own, self.slot(me), px)
        if kind == 1:
            return self.copy(1, self.own, self.slot(me), py)
        if kind == 2:
            return self.copy(2, self.half(px, 0), self.half(px, 0), py)
        if kind == 3:
            return self.copy(3, self.half(py, 1), self.half(py, 1), px)
        if kind == 4:
            return self.copy(4, self.own, self.slot(me), pc)
        if kind == 5:
            return self.copy(5, self.slot(px), self.slot(px), pc)
        if kind == 6:
            return self.copy(6, self.slot(py), self.slot(py), pc)
        return self.copy(kind, self.half(pd, kind - 7), self.half(pd, kind - 7), pc)

    def start(self):
        for kind in (0, 1, 4):
            self.describe(kind).start()

    def forward_near(self):
        self.describe(0).wait_recv()
        self.describe(2).start()
        self.describe(5).start()
        self.describe(1).wait_recv()
        self.describe(3).start()
        self.describe(6).start()

    def forward_far(self):
        self.describe(2).wait_recv()
        self.describe(7).start()
        self.describe(3).wait_recv()
        self.describe(8).start()

    def wait_recv(self, *kinds):
        for kind in kinds:
            self.describe(kind).wait_recv()

    def wait_sends(self):
        for kind in range(9):
            self.describe(kind).wait_send()


def gather_kernel(tok, wg, wu, wd, emb, tok_o, wg_o, wu_o, wd_o, emb_o, send_sem, recv_sem, local_sem):
    me = lax.axis_index("fsdp")
    rows = wg.shape[1]
    slices = wg.shape[0]
    barrier_with([flip(me, 1), flip(me, 2), flip(me, 4)])

    def lead(out, size):
        return (lambda d: out.at[d]), (lambda d, i: out.at[d, pl.ds(i * (size // 2), size // 2)])

    def column(out):
        half = slices // 2
        return (lambda d: out.at[:, pl.ds(d * rows, rows), :]), (lambda d, i: out.at[pl.ds(i * half, half), pl.ds(d * rows, rows), :])

    views = [
        (tok, lead(tok_o, tok.shape[0])),
        (wg, column(wg_o)),
        (wu, column(wu_o)),
        (wd, lead(wd_o, wd.shape[0])),
        (emb, lead(emb_o, emb.shape[0])),
    ]
    gathers, locals_ = [], []
    for k, (src, (slot, half)) in enumerate(views):
        gathers.append(Gather(slot, half, lambda c, k=k: send_sem.at[k, c], lambda c, k=k: recv_sem.at[k, c], me, own=src))
        locals_.append(pltpu.make_async_copy(src, slot(me), local_sem.at[k]))
    for gather, local in zip(gathers, locals_):
        gather.start()
        local.start()
    for gather in gathers:
        gather.forward_near()
    for gather in gathers:
        gather.forward_far()
    for gather, local in zip(gathers, locals_):
        gather.wait_recv(4, 5, 6, 7, 8)
        gather.wait_sends()
        local.wait()


def gather_all(tok, wg, wu, wd, emb):
    slices, rows, width = wg.shape
    any_spec = pl.BlockSpec(memory_space=pl.ANY)
    vmem = pl.BlockSpec(memory_space=pltpu.VMEM)
    return pl.pallas_call(
        gather_kernel,
        out_shape=(
            jax.ShapeDtypeStruct((N_DEV,) + tok.shape, tok.dtype),
            jax.ShapeDtypeStruct((slices, rows * N_DEV, width), wg.dtype),
            jax.ShapeDtypeStruct((slices, rows * N_DEV, width), wu.dtype),
            jax.ShapeDtypeStruct((N_DEV,) + wd.shape, wd.dtype),
            jax.ShapeDtypeStruct((N_DEV,) + emb.shape, emb.dtype),
        ),
        in_specs=[vmem] * 5,
        out_specs=(any_spec,) * 5,
        scratch_shapes=[pltpu.SemaphoreType.DMA((5, 9)), pltpu.SemaphoreType.DMA((5, 9)), pltpu.SemaphoreType.DMA((5,))],
        compiler_params=pltpu.CompilerParams(collective_id=0, has_side_effects=True),
        name="gather",
    )(tok, wg, wu, wd, emb)


def count_kernel(cols, bounds, keys, out, other):
    n_keys = keys.shape[0]
    n_src = N_DEV
    per = n_keys // n_src
    first = bounds[2 * n_src] * cols
    tiles = cols // 128
    size = out.shape[0]
    BLK = 256

    def clear(i, _):
        out[pl.ds(i * BLK, BLK), :] = jnp.zeros((BLK, 128), F32)
        other[pl.ds(i * BLK, BLK), :] = jnp.zeros((BLK, 128), F32)
        return 0

    lax.fori_loop(0, size // BLK, clear, 0)
    lanes = lax.broadcasted_iota(I32, (1, 128), 1)
    unroll = 8
    cols_log = cols.bit_length() - 1

    for src in range(n_src):
        begin = bounds[src] + src * per
        end = bounds[n_src + src] + src * per

        def step(i, _):
            pos = begin + i * unroll
            found = []
            for k in range(unroll):
                inside = pos + k < end
                key = keys[jnp.minimum(pos + k, n_keys - 1)] - first
                key = jnp.where(inside, key, 0)
                lane = jnp.where(inside, key & 127, -1)
                row = key >> cols_log
                found.append((((row >> 3) * tiles + ((key & (cols - 1)) >> 7)) * 8 + (row & 7), lane))
            for k, (place, lane) in enumerate(found):
                ref = out if k % 2 == 0 else other
                at = (pl.ds(place, 1), slice(None))
                ref[at] = ref[at] + jnp.where(lanes == lane, 1.0, 0.0)
            return 0

        lax.fori_loop(0, (end - begin + unroll - 1) // unroll, step, 0)

    def merge(i, _):
        at = pl.ds(i * BLK, BLK)
        out[at, :] = out[at, :] + other[at, :]
        return 0

    lax.fori_loop(0, size // BLK, merge, 0)


def count(keys, bounds, rows, cols):
    smem = pl.BlockSpec(memory_space=pltpu.SMEM)
    tall = (rows * cols // 128, 128)
    return pl.pallas_call(
        functools.partial(count_kernel, cols),
        out_shape=jax.ShapeDtypeStruct(tall, F32),
        in_specs=[smem, smem],
        out_specs=pl.BlockSpec(memory_space=pltpu.VMEM),
        scratch_shapes=[pltpu.VMEM(tall, F32)],
        compiler_params=pltpu.CompilerParams(vmem_limit_bytes=40_000_000),
        cost_estimate=pl.CostEstimate(flops=20_000_000_000, bytes_accessed=8_000_000, transcendentals=0),
        name="count",
    )(bounds, keys).reshape(rows // 8, cols // 128, 8, 128)


def step_kernel(
    coef_ref, emb_hbm, wg_hbm, wu_hbm, wd_hbm, crow_hbm, ccol_hbm, g1_ref, g2_ref,
    loss_o, de_o, dwg_o, dwu_o, dwd_o,
    emb, wg, wu, wd, crow, ccol, hn, dh, a_all, p_own, q_own, p_all, q_all, logits, dlog, h_wide, dh_wide, acc, stat, stat_col,
    dwg, dwu, load_sem, col_sem, hs, hr, ds_, dr, st_s, st_r, ws, wr,
):
    me = lax.axis_index("fsdp")
    n, rows, width = emb.shape
    fs = wg.shape[2]
    out_rows = dwg_o.shape[1]
    coef = coef_ref[0, 0]
    RB = 64
    lt = rows // 128
    peers = [lax.rem(me + k, n) for k in range(1, n)]

    loads = [
        pltpu.make_async_copy(src, dst, load_sem.at[k])
        for k, (src, dst) in enumerate([(emb_hbm, emb), (wg_hbm, wg), (wu_hbm, wu), (wd_hbm, wd), (crow_hbm, crow)])
    ]
    for load in loads:
        load.start()

    def col_load(dev, slot):
        return pltpu.make_async_copy(ccol_hbm.at[:, pl.ds(dev * lt, lt)], ccol.at[slot], col_sem.at[slot])

    barrier_with(peers)

    def gather_of(buf, ss, rs):
        half = rows // 2
        return Gather(lambda d: buf.at[d], lambda d, i: buf.at[d, pl.ds(i * half, half)], lambda c: ss.at[c], lambda c: rs.at[c], me)

    hn_g, dh_g = gather_of(hn, hs, hr), gather_of(dh, ds_, dr)
    g1, g2 = g1_ref[...], g2_ref[...]

    loads[0].wait()

    def norm_rows(i, _):
        dev, at = i // (rows // RB), pl.ds(lax.rem(i, rows // RB) * RB, RB)
        x = emb[dev, at, :].astype(F32)
        inv = lax.rsqrt(jnp.mean(x * x, axis=-1, keepdims=True) + NORM_EPS)
        a_all[dev, at, :] = (x * inv * g1).astype(BF16)
        return 0

    per_dev = rows // RB
    lax.fori_loop(me * per_dev, (me + 1) * per_dev, norm_rows, 0)

    for load in loads[1:4]:
        load.wait()
    acc[...] = jnp.zeros_like(acc)

    def forward(j, _):
        a = a_all[me]
        p = dot_nn(a, wg[j]).astype(BF16)
        q = dot_nn(a, wu[j]).astype(BF16)
        p_own[j], q_own[j] = p, q
        p, q = p.astype(F32), q.astype(F32)
        u = (p * jax.nn.sigmoid(p) * q).astype(BF16)
        acc[...] += dot_nn(u, wd[j])
        return 0

    lax.fori_loop(0, n, forward, 0)

    def hidden(i, _):
        at = pl.ds(i * RB, RB)
        h = (emb[me, at, :].astype(F32) + acc[at, :]).astype(BF16).astype(F32)
        h_wide[at, :] = h
        inv = lax.rsqrt(jnp.mean(h * h, axis=-1, keepdims=True) + NORM_EPS)
        hn[me, at, :] = (h * inv * g2).astype(BF16)
        return 0

    lax.fori_loop(0, per_dev, hidden, 0)
    hn_g.start()

    def logit(v, _):
        logits[v] = dot_nt(hn[me], emb[v])
        return 0

    lax.fori_loop(0, n, logit, 0)
    loads[4].wait()

    def softmax(i, _):
        at = pl.ds(i * RB, RB)

        def cnt_tile(v, k):
            return crow[pl.ds(i * (RB // 8), RB // 8), v * lt + k].reshape(RB, 128)

        def top(v, m):
            val = logits[v, at, :]
            for k in range(rows // 128):
                m = jnp.maximum(m, val[:, k * 128:(k + 1) * 128])
            return m

        m = jnp.max(lax.fori_loop(0, n, top, jnp.full((RB, 128), -jnp.inf, F32)), axis=-1, keepdims=True)

        def sums(v, carry):
            s, c, pick = carry
            for k in range(lt):
                cut = slice(k * 128, (k + 1) * 128)
                val, cnt = logits[v, at, cut], cnt_tile(v, k)
                ex = jnp.exp(val - m)
                logits[v, at, cut] = ex
                s, c, pick = s + ex, c + cnt, pick + cnt * val
            return s, c, pick

        zero = jnp.zeros((RB, 128), F32)
        s, c, pick = [jnp.sum(val, axis=-1, keepdims=True) for val in lax.fori_loop(0, n, sums, (zero, zero, zero))]
        lse = m + jnp.log(s)
        lane = lax.broadcasted_iota(I32, (RB, 128), 1)
        stat_col[at, :] = jnp.where(lane == 0, lse, jnp.where(lane == 1, c * coef, jnp.where(lane == 2, c * lse - pick, 0.0)))
        scale = c * coef / s

        def grad(v, _):
            for k in range(lt):
                cut = slice(k * 128, (k + 1) * 128)
                dlog[v, at, cut] = (logits[v, at, cut] * scale - cnt_tile(v, k) * coef).astype(BF16)
            return 0

        lax.fori_loop(0, n, grad, 0)
        return 0

    lax.fori_loop(0, per_dev, softmax, 0)
    stat[me] = jnp.transpose(stat_col[...])[0:8, :]

    acc[...] = jnp.zeros_like(acc)

    def dhn_step(v, _):
        acc[...] += dot_nn(dlog[v], emb[v])
        return 0

    lax.fori_loop(0, n, dhn_step, 0)
    stat_copies = [
        pltpu.make_async_remote_copy(
            src_ref=stat.at[me], dst_ref=stat.at[me], send_sem=st_s.at[k], recv_sem=st_r.at[k], device_id=(peer,), device_id_type=MESH
        )
        for k, peer in enumerate(peers)
    ]
    for copy in stat_copies:
        copy.start()

    def dhidden(i, _):
        at = pl.ds(i * RB, RB)
        h, scaled = h_wide[at, :], acc[at, :] * g2
        inv = lax.rsqrt(jnp.mean(h * h, axis=-1, keepdims=True) + NORM_EPS)
        grad = inv * (scaled - h * (inv * inv) * jnp.mean(scaled * h, axis=-1, keepdims=True))
        dh_wide[at, :] = grad
        dh[me, at, :] = grad.astype(BF16)
        return 0

    lax.fori_loop(0, per_dev, dhidden, 0)
    dh_g.start()
    hn_g.forward_near()

    lax.fori_loop(0, me * per_dev, norm_rows, 0)
    lax.fori_loop((me + 1) * per_dev, n * per_dev, norm_rows, 0)

    def slice_forward(s, _):
        p_all[s] = dot_nn(a_all[s], wg[me]).astype(BF16)
        q_all[s] = dot_nn(a_all[s], wu[me]).astype(BF16)
        return 0

    lax.fori_loop(0, n, slice_forward, 0)
    hn_g.forward_far()

    acc[...] = jnp.zeros_like(acc)

    def act_back(dact, p, q):
        sig = jax.nn.sigmoid(p)
        gated = p * sig
        dq = (dact * gated).astype(BF16)
        dp = (dact * q * sig * (1.0 + p * (1.0 - sig))).astype(BF16)
        return dp, dq, (gated * q).astype(BF16)

    def backward(j, _):
        dact = dot_nt(dh[me], wd[j])
        dp, dq, _u = act_back(dact, p_own[j].astype(F32), q_own[j].astype(F32))
        acc[...] += dot_nt(dp, wg[j]) + dot_nt(dq, wu[j])
        return 0

    lax.fori_loop(0, n, backward, 0)

    def dinput(i, _):
        at = pl.ds(i * RB, RB)
        x, scaled = emb[me, at, :].astype(F32), acc[at, :] * g1
        inv = lax.rsqrt(jnp.mean(x * x, axis=-1, keepdims=True) + NORM_EPS)
        de_o[at, :] = dh_wide[at, :] + inv * (scaled - x * (inv * inv) * jnp.mean(scaled * x, axis=-1, keepdims=True))
        return 0

    lax.fori_loop(0, per_dev, dinput, 0)
    dh_g.forward_near()
    for copy in stat_copies:
        copy.wait_recv()

    def head(dev, slot):
        col_load(dev, slot).wait()
        logits[0] = dot_nt(emb[me], hn[dev])
        lse, weight = stat[dev, 0:1, :], stat[dev, 1:2, :]

        def grad(i, _):
            at = pl.ds(i * RB, RB)
            for k in range(lt):
                cut = slice(k * 128, (k + 1) * 128)
                prob = jnp.exp(logits[0, at, cut] - lse[:, cut]) * weight[:, cut]
                cnt = ccol[slot, pl.ds(i * (RB // 8), RB // 8), k].reshape(RB, 128)
                dlog[0, at, cut] = (prob - cnt * coef).astype(BF16)
            return 0

        lax.fori_loop(0, per_dev, grad, 0)
        de_o[...] += dot_nn(dlog[0], hn[dev])

    dwg[...] = jnp.zeros_like(dwg)
    dwu[...] = jnp.zeros_like(dwu)
    dwd_o[...] = jnp.zeros_like(dwd_o)

    def weights(dev):
        dact = dot_nt(dh[dev], wd[me])
        dp, dq, u = act_back(dact, p_all[dev].astype(F32), q_all[dev].astype(F32))
        dwd_o[...] += dot_tn(u, dh[dev])
        dwg[...] += dot_tn(a_all[dev], dp)
        dwu[...] += dot_tn(a_all[dev], dq)

    pc, px, py, pd = hn_g.pc, hn_g.px, hn_g.py, hn_g.pd
    order = [(me, ()), (pc, (4,)), (px, ()), (py, ()), (flip(px, 1), (5,)), (flip(py, 1), (6,)), (pd, ()), (flip(pd, 1), (7, 8))]
    col_load(order[0][0], 0).start()
    for k, (dev, kinds) in enumerate(order):
        if k + 1 < n:
            col_load(order[k + 1][0], (k + 1) % 2).start()
        hn_g.wait_recv(*kinds)
        head(dev, k % 2)
        if k == 5:
            dh_g.forward_far()
    for dev, kinds in order:
        dh_g.wait_recv(*kinds)
        weights(dev)

    def exchange(k, peer, src, dst, row):
        return pltpu.make_async_remote_copy(
            src_ref=src.at[pl.ds(pl.multiple_of(peer * out_rows, out_rows), out_rows), :],
            dst_ref=dst.at[me],
            send_sem=ws.at[row, k], recv_sem=wr.at[row, k], device_id=(peer,), device_id_type=MESH,
        )

    swaps = [exchange(k, peer, src, dst, row) for k, peer in enumerate(peers) for row, (src, dst) in enumerate([(dwg, dwg_o), (dwu, dwu_o)])]
    for swap in swaps:
        swap.start()
    mine = pl.ds(pl.multiple_of(me * out_rows, out_rows), out_rows)
    dwg_o[me] = dwg[mine, :]
    dwu_o[me] = dwu[mine, :]
    total = jnp.zeros((1, rows), F32)
    for s in range(n):
        total = total + stat[s, 2:3, :]
    loss_o[...] = jnp.sum(total, axis=-1, keepdims=True) * coef + jnp.zeros((1, 128), F32)
    for copy in stat_copies:
        copy.wait_send()
    hn_g.wait_sends()
    dh_g.wait_sends()
    for swap in swaps:
        swap.wait()


def run_step(coef, emb, wg, wu, wd, crow, ccol, g1, g2):
    n, rows, width = emb.shape
    fs = wg.shape[2]
    out_rows = width // n
    any_spec = pl.BlockSpec(memory_space=pl.ANY)
    vmem = pl.BlockSpec(memory_space=pltpu.VMEM)
    dma = pltpu.SemaphoreType.DMA
    return pl.pallas_call(
        step_kernel,
        out_shape=(
            jax.ShapeDtypeStruct((1, 128), F32),
            jax.ShapeDtypeStruct((rows, width), F32),
            jax.ShapeDtypeStruct((n, out_rows, fs), F32),
            jax.ShapeDtypeStruct((n, out_rows, fs), F32),
            jax.ShapeDtypeStruct((fs, width), F32),
        ),
        in_specs=[pl.BlockSpec(memory_space=pltpu.SMEM)] + [any_spec] * 6 + [vmem] * 2,
        out_specs=(vmem,) * 5,
        scratch_shapes=[
            pltpu.VMEM((n, rows, width), BF16),
            pltpu.VMEM((n, width, fs), BF16),
            pltpu.VMEM((n, width, fs), BF16),
            pltpu.VMEM((n, fs, width), BF16),
            pltpu.VMEM((rows // 8, n * rows // 128, 8, 128), F32),
            pltpu.VMEM((2, rows // 8, rows // 128, 8, 128), F32),
            pltpu.VMEM((n, rows, width), BF16),
            pltpu.VMEM((n, rows, width), BF16),
            pltpu.VMEM((n, rows, width), BF16),
            pltpu.VMEM((n, rows, fs), BF16),
            pltpu.VMEM((n, rows, fs), BF16),
            pltpu.VMEM((n, rows, fs), BF16),
            pltpu.VMEM((n, rows, fs), BF16),
            pltpu.VMEM((n, rows, rows), F32),
            pltpu.VMEM((n, rows, rows), BF16),
            pltpu.VMEM((rows, width), F32),
            pltpu.VMEM((rows, width), F32),
            pltpu.VMEM((rows, width), F32),
            pltpu.VMEM((n, 8, rows), F32),
            pltpu.VMEM((rows, 128), F32),
            pltpu.VMEM((width, fs), F32),
            pltpu.VMEM((width, fs), F32),
            dma((5,)), dma((2,)), dma((9,)), dma((9,)), dma((9,)), dma((9,)), dma((n - 1,)), dma((n - 1,)), dma((2, n - 1)), dma((2, n - 1)),
        ],
        compiler_params=pltpu.CompilerParams(collective_id=1, has_side_effects=True, vmem_limit_bytes=VMEM_MAX),
        name="step",
    )(coef, emb, wg, wu, wd, crow, ccol, g1, g2)


def solution(mesh):
    def device_step(tok_ids, tok_labels, loss_mask, emb, g1, g2, w_gate, w_up, w_down):
        n = N_DEV
        rows, width = emb.shape
        vocab = rows * n
        n_tok = tok_ids.shape[0]
        fs = w_gate.shape[1] // n
        me = lax.axis_index("fsdp")

        live = loss_mask != 0
        by_id = lax.sort(jnp.where(live, tok_ids * 65536 + tok_labels, vocab * 65536))
        by_label = lax.sort(jnp.where(live, tok_labels * 65536 + tok_ids, vocab * 65536))
        tok = jnp.stack([by_id >> 16, by_id & 65535, by_label >> 16, by_label & 65535]).reshape(4, n_tok // 128, 128)

        def slices(w):
            return w.reshape(w.shape[0], n, fs).transpose(1, 0, 2)

        tok_all, wg_all, wu_all, wd_all, emb_all = gather_all(tok, slices(w_gate), slices(w_up), w_down, emb)
        tok_all = tok_all.reshape(n, 4, n_tok)

        def counts(major, minor):
            low = jnp.sum(major < me * rows, axis=1, dtype=I32)
            high = jnp.sum(major < (me + 1) * rows, axis=1, dtype=I32)
            bounds = jnp.concatenate([low, high, jnp.full((n,), me * rows, I32)])
            return count((major * vocab + minor).reshape(-1), bounds, rows, vocab)

        crow = counts(tok_all[:, 0], tok_all[:, 1])
        ccol = counts(tok_all[:, 2], tok_all[:, 3])
        n_live = jnp.sum(tok_all[:, 0] < vocab).astype(F32)
        coef = (1.0 / n_live).reshape(1, 1)
        loss, de, dwg, dwu, dwd = run_step(coef, emb_all, wg_all, wu_all, wd_all, crow, ccol, g1.reshape(1, width), g2.reshape(1, width))

        def whole(dw):
            return dw.transpose(1, 0, 2).reshape(w_gate.shape)

        return loss[0, 0], de, whole(dwg), whole(dwu), dwd

    row_spec = P("fsdp", None)
    tok_spec = P("fsdp")
    return jax.shard_map(device_step, mesh=mesh, in_specs=(tok_spec, tok_spec, tok_spec, row_spec, P(), P(), row_spec, row_spec, row_spec), out_specs=(P(), row_spec, row_spec, row_spec, row_spec), check_vma=False)
```

```python
import functools

import jax
import jax.numpy as jnp
from jax import lax
from jax.experimental import pallas as pl
from jax.experimental.pallas import tpu as pltpu
from jax.sharding import PartitionSpec as P


NORM_EPS = 1e-6
N_DEV = 8
F32, BF16, I32 = jnp.float32, jnp.bfloat16, jnp.int32
MESH = pl.DeviceIdType.MESH
VMEM_MAX = 66_000_000


def dot_nn(a, b):
    return jnp.dot(a, b, preferred_element_type=F32)


def dot_nt(a, b):
    return lax.dot_general(a, b, (((1,), (1,)), ((), ())), preferred_element_type=F32)


def dot_tn(a, b):
    return lax.dot_general(a, b, (((0,), (0,)), ((), ())), preferred_element_type=F32)


def flip(me, bit):
    return me + bit - 2 * bit * lax.rem(me // bit, 2)


def barrier_with(peers):
    sem = pltpu.get_barrier_semaphore()
    for peer in peers:
        pl.semaphore_signal(sem, inc=1, device_id=(peer,), device_id_type=MESH)
    pl.semaphore_wait(sem, len(peers))


class Gather:
    def __init__(self, slot, half, send_sem, recv_sem, me, own=None):
        self.slot, self.half, self.ss, self.rs, self.me = slot, half, send_sem, recv_sem, me
        self.own = slot(me) if own is None else own
        self.pc, self.px, self.py = flip(me, 1), flip(me, 2), flip(me, 4)
        self.pd = flip(self.px, 4)

    def copy(self, kind, src, dst, peer):
        return pltpu.make_async_remote_copy(
            src_ref=src, dst_ref=dst, send_sem=self.ss(kind), recv_sem=self.rs(kind), device_id=(peer,), device_id_type=MESH
        )

    def describe(self, kind):
        me, px, py, pd, pc = self.me, self.px, self.py, self.pd, self.pc
        if kind == 0:
            return self.copy(0, self.own, self.slot(me), px)
        if kind == 1:
            return self.copy(1, self.own, self.slot(me), py)
        if kind == 2:
            return self.copy(2, self.half(px, 0), self.half(px, 0), py)
        if kind == 3:
            return self.copy(3, self.half(py, 1), self.half(py, 1), px)
        if kind == 4:
            return self.copy(4, self.own, self.slot(me), pc)
        if kind == 5:
            return self.copy(5, self.slot(px), self.slot(px), pc)
        if kind == 6:
            return self.copy(6, self.slot(py), self.slot(py), pc)
        return self.copy(kind, self.half(pd, kind - 7), self.half(pd, kind - 7), pc)

    def start(self):
        for kind in (0, 1, 4):
            self.describe(kind).start()

    def forward_near(self):
        self.describe(0).wait_recv()
        self.describe(2).start()
        self.describe(5).start()
        self.describe(1).wait_recv()
        self.describe(3).start()
        self.describe(6).start()

    def forward_far(self):
        self.describe(2).wait_recv()
        self.describe(7).start()
        self.describe(3).wait_recv()
        self.describe(8).start()

    def wait_recv(self, *kinds):
        for kind in kinds:
            self.describe(kind).wait_recv()

    def wait_sends(self):
        for kind in range(9):
            self.describe(kind).wait_send()


def slice_kernel(gate, up, out):
    n, _, fs = out.shape
    rows = gate.shape[0]
    for k in range(n):
        out[k, 0:rows, :] = gate[:, k * fs:(k + 1) * fs]
        out[k, rows:2 * rows, :] = up[:, k * fs:(k + 1) * fs]


def slice_weights(gate, up):
    rows, width = gate.shape
    return pl.pallas_call(
        slice_kernel,
        out_shape=jax.ShapeDtypeStruct((N_DEV, 2 * rows, width // N_DEV), gate.dtype),
        cost_estimate=pl.CostEstimate(flops=1_000_000, bytes_accessed=1_000_000, transcendentals=0),
        name="slices",
    )(gate, up)


def token_kernel(tok, tok_o, send_sem, recv_sem, local_sem):
    me = lax.axis_index("fsdp")
    n = tok_o.shape[0]
    peers = [lax.rem(me + k, n) for k in range(1, n)]
    barrier_with(peers)
    copies = [
        pltpu.make_async_remote_copy(
            src_ref=tok, dst_ref=tok_o.at[me], send_sem=send_sem.at[k], recv_sem=recv_sem.at[k], device_id=(peer,), device_id_type=MESH
        )
        for k, peer in enumerate(peers)
    ]
    local = pltpu.make_async_copy(tok, tok_o.at[me], local_sem)
    for copy in copies:
        copy.start()
    local.start()
    for copy in copies:
        copy.wait()
    local.wait()


def gather_tokens(tok):
    dma = pltpu.SemaphoreType.DMA
    return pl.pallas_call(
        token_kernel,
        out_shape=jax.ShapeDtypeStruct((N_DEV,) + tok.shape, tok.dtype),
        in_specs=[pl.BlockSpec(memory_space=pltpu.VMEM)],
        out_specs=pl.BlockSpec(memory_space=pl.ANY),
        scratch_shapes=[dma((N_DEV - 1,)), dma((N_DEV - 1,)), dma],
        compiler_params=pltpu.CompilerParams(collective_id=0, has_side_effects=True),
        cost_estimate=pl.CostEstimate(flops=5_000_000_000, bytes_accessed=1_000_000, transcendentals=0),
        name="tokens",
    )(tok)


def count_kernel(bounds, keys, out):
    n_src = N_DEV
    per = keys.shape[0] // n_src
    size = out.shape[0]
    BLK = 256
    unroll = 8

    def clear(i, _):
        out[pl.ds(i * BLK, BLK), :] = jnp.zeros((BLK, 128), F32)
        return 0

    lax.fori_loop(0, size // BLK, clear, 0)
    lanes = lax.broadcasted_iota(I32, (1, 128), 1)

    def source(src, _):
        begin = bounds[src] + src * per
        end = bounds[n_src + src] + src * per

        def step(i, _):
            pos = begin + i * unroll
            places, marks = [], []
            for k in range(unroll):
                key = keys[jnp.minimum(pos + k, end - 1)]
                places.append(key >> 7)
                marks.append(jnp.where(pos + k < end, key & 127, -1))
            old = [out[pl.ds(place, 1), :] for place in places]
            delta = None
            for k in range(unroll):
                here = jnp.where(lanes == marks[k], 1.0, 0.0)
                delta = here if k == 0 else here + delta * jnp.where(places[k] == places[k - 1], 1.0, 0.0)
                old[k] = old[k] + delta
            for place, val in zip(places, old):
                out[pl.ds(place, 1), :] = val
            return 0

        lax.fori_loop(0, (end - begin + unroll - 1) // unroll, step, 0)
        return 0

    lax.fori_loop(0, n_src, source, 0)


def count(major, minor, first, rows, cols):
    low = jnp.sum(major < first, axis=(1, 2), dtype=I32)
    high = jnp.sum(major < first + rows, axis=(1, 2), dtype=I32)
    row, tiles = major - first, cols // 128
    keys = ((((row >> 3) * tiles + (minor >> 7)) * 8 + (row & 7)) * 128 + (minor & 127)).reshape(-1)
    smem = pl.BlockSpec(memory_space=pltpu.SMEM)
    return pl.pallas_call(
        count_kernel,
        out_shape=jax.ShapeDtypeStruct((rows * cols // 128, 128), F32),
        in_specs=[smem, smem],
        out_specs=pl.BlockSpec(memory_space=pltpu.VMEM),
        cost_estimate=pl.CostEstimate(flops=20_000_000_000, bytes_accessed=8_000_000, transcendentals=0),
        name="count",
    )(jnp.concatenate([low, high]), keys).reshape(rows // 8, tiles, 8, 128)


def step_kernel(
    coef_ref, emb_me, emb_x, emb_y, emb_d, gu_me, gu_x, gu_y, gu_d, wd_me, wd_x, wd_y, wd_d, crow_hbm, ccol_hbm, g1_ref, g2_ref,
    loss_o, de_o, dwg_o, dwu_o, dwd_o,
    emb, wg, wu, wd, crow, ccol, hn, dh, a_all, p_own, q_own, p_all, q_all, logits, dlog, h_wide, dh_wide, acc, stat, stat_col,
    dwg, dwu, got_g, got_u, load_sem, pair_s, pair_r, col_sem, hs, hr, ds_, dr, st_s, st_r, ws, wr,
):
    me = lax.axis_index("fsdp")
    n, rows, width = emb.shape
    fs = wg.shape[2]
    out_rows = dwg_o.shape[0]
    coef = coef_ref[0, 0]
    RB = 64
    lt = rows // 128
    peers = [lax.rem(me + k, n) for k in range(1, n)]

    pc, px, py = flip(me, 1), flip(me, 2), flip(me, 4)
    pd = flip(px, 4)
    devs = [me, px, py, pd]
    parts = []
    for dev, gu, down in zip(devs, [gu_me, gu_x, gu_y, gu_d], [wd_me, wd_x, wd_y, wd_d]):
        at = pl.ds(dev * out_rows, out_rows)
        parts.append((gu.at[:, 0:out_rows, :], wg.at[:, at, :]))
        parts.append((gu.at[:, out_rows:2 * out_rows, :], wu.at[:, at, :]))
        parts.append((down, wd.at[dev]))
    n_weight = len(parts)
    for dev, block in zip(devs, [emb_me, emb_x, emb_y, emb_d]):
        parts.append((block, emb.at[dev]))
    loads = [pltpu.make_async_copy(src, dst, load_sem.at[k]) for k, (src, dst) in enumerate(parts)]
    pairs = [
        pltpu.make_async_remote_copy(
            src_ref=src, dst_ref=dst, send_sem=pair_s.at[k], recv_sem=pair_r.at[k], device_id=(pc,), device_id_type=MESH
        )
        for k, (src, dst) in enumerate(parts)
    ]
    crow_load = pltpu.make_async_copy(crow_hbm, crow, load_sem.at[len(parts)])

    def col_load(dev, slot):
        return pltpu.make_async_copy(ccol_hbm.at[:, pl.ds(dev * lt, lt)], ccol.at[slot], col_sem.at[slot])

    loads[n_weight].start()
    for load in loads[:n_weight]:
        load.start()
    barrier_with(peers)
    for pair in pairs:
        pair.start()
    for load in loads[n_weight + 1:]:
        load.start()
    crow_load.start()

    def gather_of(buf, ss, rs):
        half = rows // 2
        return Gather(lambda d: buf.at[d], lambda d, i: buf.at[d, pl.ds(i * half, half)], lambda c: ss.at[c], lambda c: rs.at[c], me)

    hn_g, dh_g = gather_of(hn, hs, hr), gather_of(dh, ds_, dr)
    g1, g2 = g1_ref[...], g2_ref[...]

    loads[n_weight].wait()

    def norm_rows(i, _):
        dev, at = i // (rows // RB), pl.ds(lax.rem(i, rows // RB) * RB, RB)
        x = emb[dev, at, :].astype(F32)
        inv = lax.rsqrt(jnp.mean(x * x, axis=-1, keepdims=True) + NORM_EPS)
        a_all[dev, at, :] = (x * inv * g1).astype(BF16)
        return 0

    per_dev = rows // RB
    lax.fori_loop(me * per_dev, (me + 1) * per_dev, norm_rows, 0)

    for load, pair in zip(loads[:n_weight], pairs[:n_weight]):
        load.wait()
        pair.wait_recv()
    acc[...] = jnp.zeros_like(acc)

    def forward(j, _):
        a = a_all[me]
        p = dot_nn(a, wg[j]).astype(BF16)
        q = dot_nn(a, wu[j]).astype(BF16)
        p_own[j], q_own[j] = p, q
        p, q = p.astype(F32), q.astype(F32)
        u = (p * jax.nn.sigmoid(p) * q).astype(BF16)
        acc[...] += dot_nn(u, wd[j])
        return 0

    lax.fori_loop(0, n, forward, 0)

    def hidden(i, _):
        at = pl.ds(i * RB, RB)
        h = (emb[me, at, :].astype(F32) + acc[at, :]).astype(BF16).astype(F32)
        h_wide[at, :] = h
        inv = lax.rsqrt(jnp.mean(h * h, axis=-1, keepdims=True) + NORM_EPS)
        hn[me, at, :] = (h * inv * g2).astype(BF16)
        return 0

    lax.fori_loop(0, per_dev, hidden, 0)
    hn_g.start()
    for load in loads[n_weight + 1:]:
        load.wait()
    for pair in pairs[n_weight:]:
        pair.wait_recv()

    def logit(v, _):
        logits[v] = dot_nt(hn[me], emb[v])
        return 0

    lax.fori_loop(0, n, logit, 0)
    crow_load.wait()

    def softmax(i, _):
        at = pl.ds(i * RB, RB)

        def cnt_tile(v, k):
            return crow[pl.ds(i * (RB // 8), RB // 8), v * lt + k].reshape(RB, 128)

        def top(v, m):
            val = logits[v, at, :]
            for k in range(rows // 128):
                m = jnp.maximum(m, val[:, k * 128:(k + 1) * 128])
            return m

        m = jnp.max(lax.fori_loop(0, n, top, jnp.full((RB, 128), -jnp.inf, F32)), axis=-1, keepdims=True)

        def sums(v, carry):
            s, c, pick = carry
            for k in range(lt):
                cut = slice(k * 128, (k + 1) * 128)
                val, cnt = logits[v, at, cut], cnt_tile(v, k)
                ex = jnp.exp(val - m)
                logits[v, at, cut] = ex
                s, c, pick = s + ex, c + cnt, pick + cnt * val
            return s, c, pick

        zero = jnp.zeros((RB, 128), F32)
        s, c, pick = [jnp.sum(val, axis=-1, keepdims=True) for val in lax.fori_loop(0, n, sums, (zero, zero, zero))]
        lse = m + jnp.log(s)
        lane = lax.broadcasted_iota(I32, (RB, 128), 1)
        stat_col[at, :] = jnp.where(lane == 0, lse, jnp.where(lane == 1, c * coef, jnp.where(lane == 2, c * lse - pick, 0.0)))
        scale = c * coef / s

        def grad(v, _):
            for k in range(lt):
                cut = slice(k * 128, (k + 1) * 128)
                dlog[v, at, cut] = (logits[v, at, cut] * scale - cnt_tile(v, k) * coef).astype(BF16)
            return 0

        lax.fori_loop(0, n, grad, 0)
        return 0

    lax.fori_loop(0, per_dev, softmax, 0)
    stat[me] = jnp.transpose(stat_col[...])[0:8, :]

    acc[...] = jnp.zeros_like(acc)

    def dhn_step(v, _):
        acc[...] += dot_nn(dlog[v], emb[v])
        return 0

    lax.fori_loop(0, n, dhn_step, 0)
    stat_copies = [
        pltpu.make_async_remote_copy(
            src_ref=stat.at[me], dst_ref=stat.at[me], send_sem=st_s.at[k], recv_sem=st_r.at[k], device_id=(peer,), device_id_type=MESH
        )
        for k, peer in enumerate(peers)
    ]
    for copy in stat_copies:
        copy.start()

    def dhidden(i, _):
        at = pl.ds(i * RB, RB)
        h, scaled = h_wide[at, :], acc[at, :] * g2
        inv = lax.rsqrt(jnp.mean(h * h, axis=-1, keepdims=True) + NORM_EPS)
        grad = inv * (scaled - h * (inv * inv) * jnp.mean(scaled * h, axis=-1, keepdims=True))
        dh_wide[at, :] = grad
        dh[me, at, :] = grad.astype(BF16)
        return 0

    lax.fori_loop(0, per_dev, dhidden, 0)
    dh_g.start()
    hn_g.forward_near()

    lax.fori_loop(0, me * per_dev, norm_rows, 0)
    lax.fori_loop((me + 1) * per_dev, n * per_dev, norm_rows, 0)

    def slice_forward(s, _):
        p_all[s] = dot_nn(a_all[s], wg[me]).astype(BF16)
        q_all[s] = dot_nn(a_all[s], wu[me]).astype(BF16)
        return 0

    lax.fori_loop(0, n, slice_forward, 0)
    hn_g.forward_far()

    acc[...] = jnp.zeros_like(acc)

    def act_back(dact, p, q):
        sig = jax.nn.sigmoid(p)
        gated = p * sig
        dq = (dact * gated).astype(BF16)
        dp = (dact * q * sig * (1.0 + p * (1.0 - sig))).astype(BF16)
        return dp, dq, (gated * q).astype(BF16)

    def backward(j, _):
        dact = dot_nt(dh[me], wd[j])
        dp, dq, _u = act_back(dact, p_own[j].astype(F32), q_own[j].astype(F32))
        acc[...] += dot_nt(dp, wg[j]) + dot_nt(dq, wu[j])
        return 0

    lax.fori_loop(0, n, backward, 0)

    def dinput(i, _):
        at = pl.ds(i * RB, RB)
        x, scaled = emb[me, at, :].astype(F32), acc[at, :] * g1
        inv = lax.rsqrt(jnp.mean(x * x, axis=-1, keepdims=True) + NORM_EPS)
        de_o[at, :] = dh_wide[at, :] + inv * (scaled - x * (inv * inv) * jnp.mean(scaled * x, axis=-1, keepdims=True))
        return 0

    lax.fori_loop(0, per_dev, dinput, 0)
    dh_g.forward_near()
    for copy in stat_copies:
        copy.wait_recv()

    def head(dev, slot):
        col_load(dev, slot).wait()
        logits[0] = dot_nt(emb[me], hn[dev])
        lse, weight = stat[dev, 0:1, :], stat[dev, 1:2, :]

        def grad(i, _):
            at = pl.ds(i * RB, RB)
            for k in range(lt):
                cut = slice(k * 128, (k + 1) * 128)
                prob = jnp.exp(logits[0, at, cut] - lse[:, cut]) * weight[:, cut]
                cnt = ccol[slot, pl.ds(i * (RB // 8), RB // 8), k].reshape(RB, 128)
                dlog[0, at, cut] = (prob - cnt * coef).astype(BF16)
            return 0

        lax.fori_loop(0, per_dev, grad, 0)
        de_o[...] += dot_nn(dlog[0], hn[dev])

    dwg[...] = jnp.zeros_like(dwg)
    dwu[...] = jnp.zeros_like(dwu)
    dwd_o[...] = jnp.zeros_like(dwd_o)

    def weights(dev):
        dact = dot_nt(dh[dev], wd[me])
        dp, dq, u = act_back(dact, p_all[dev].astype(F32), q_all[dev].astype(F32))
        dwd_o[...] += dot_tn(u, dh[dev])
        dwg[...] += dot_tn(a_all[dev], dp)
        dwu[...] += dot_tn(a_all[dev], dq)

    order = [(me, ()), (pc, (4,)), (px, ()), (py, ()), (flip(px, 1), (5,)), (flip(py, 1), (6,)), (pd, ()), (flip(pd, 1), (7, 8))]
    col_load(order[0][0], 0).start()
    for k, (dev, kinds) in enumerate(order):
        if k + 1 < n:
            col_load(order[k + 1][0], (k + 1) % 2).start()
        hn_g.wait_recv(*kinds)
        head(dev, k % 2)
        if k == 5:
            dh_g.forward_far()
    for dev, kinds in order:
        dh_g.wait_recv(*kinds)
        weights(dev)

    def exchange(k, peer, src, dst, row):
        return pltpu.make_async_remote_copy(
            src_ref=src.at[pl.ds(pl.multiple_of(peer * out_rows, out_rows), out_rows), :],
            dst_ref=dst.at[me],
            send_sem=ws.at[row, k], recv_sem=wr.at[row, k], device_id=(peer,), device_id_type=MESH,
        )

    swaps = [exchange(k, peer, src, dst, row) for k, peer in enumerate(peers) for row, (src, dst) in enumerate([(dwg, got_g), (dwu, got_u)])]
    for swap in swaps:
        swap.start()
    mine = pl.ds(pl.multiple_of(me * out_rows, out_rows), out_rows)
    got_g[me] = dwg[mine, :]
    got_u[me] = dwu[mine, :]
    total = jnp.zeros((1, rows), F32)
    for s in range(n):
        total = total + stat[s, 2:3, :]
    loss_o[...] = jnp.sum(total, axis=-1, keepdims=True) * coef + jnp.zeros((1, 128), F32)
    for copy in stat_copies:
        copy.wait_send()
    hn_g.wait_sends()
    dh_g.wait_sends()
    for pair in pairs:
        pair.wait_send()
    for swap in swaps:
        swap.wait()
    for k in range(n):
        dwg_o[:, k * fs:(k + 1) * fs] = got_g[k]
        dwu_o[:, k * fs:(k + 1) * fs] = got_u[k]


def run_step(coef, embs, gus, downs, crow, ccol, g1, g2):
    n = N_DEV
    rows, width = embs[0].shape
    fs = gus[0].shape[2]
    out_rows = width // n
    any_spec = pl.BlockSpec(memory_space=pl.ANY)
    vmem = pl.BlockSpec(memory_space=pltpu.VMEM)
    dma = pltpu.SemaphoreType.DMA
    return pl.pallas_call(
        step_kernel,
        out_shape=(
            jax.ShapeDtypeStruct((1, 128), F32),
            jax.ShapeDtypeStruct((rows, width), F32),
            jax.ShapeDtypeStruct((out_rows, n * fs), F32),
            jax.ShapeDtypeStruct((out_rows, n * fs), F32),
            jax.ShapeDtypeStruct((fs, width), F32),
        ),
        in_specs=[pl.BlockSpec(memory_space=pltpu.SMEM)] + [any_spec] * 14 + [vmem] * 2,
        out_specs=(vmem,) * 5,
        scratch_shapes=[
            pltpu.VMEM((n, rows, width), BF16),
            pltpu.VMEM((n, width, fs), BF16),
            pltpu.VMEM((n, width, fs), BF16),
            pltpu.VMEM((n, fs, width), BF16),
            pltpu.VMEM((rows // 8, n * rows // 128, 8, 128), F32),
            pltpu.VMEM((2, rows // 8, rows // 128, 8, 128), F32),
            pltpu.VMEM((n, rows, width), BF16),
            pltpu.VMEM((n, rows, width), BF16),
            pltpu.VMEM((n, rows, width), BF16),
            pltpu.VMEM((n, rows, fs), BF16),
            pltpu.VMEM((n, rows, fs), BF16),
            pltpu.VMEM((n, rows, fs), BF16),
            pltpu.VMEM((n, rows, fs), BF16),
            pltpu.VMEM((n, rows, rows), F32),
            pltpu.VMEM((n, rows, rows), BF16),
            pltpu.VMEM((rows, width), F32),
            pltpu.VMEM((rows, width), F32),
            pltpu.VMEM((rows, width), F32),
            pltpu.VMEM((n, 8, rows), F32),
            pltpu.VMEM((rows, 128), F32),
            pltpu.VMEM((width, fs), F32),
            pltpu.VMEM((width, fs), F32),
            pltpu.VMEM((n, out_rows, fs), F32),
            pltpu.VMEM((n, out_rows, fs), F32),
            dma((17,)), dma((16,)), dma((16,)), dma((2,)), dma((9,)), dma((9,)), dma((9,)), dma((9,)), dma((n - 1,)), dma((n - 1,)), dma((2, n - 1)), dma((2, n - 1)),
        ],
        compiler_params=pltpu.CompilerParams(collective_id=1, has_side_effects=True, vmem_limit_bytes=VMEM_MAX),
        name="step",
    )(coef, *embs, *gus, *downs, crow, ccol, g1, g2)


def solution(mesh):
    def device_step(tok_ids, tok_labels, loss_mask, emb, g1, g2, w_gate, w_up, w_down):
        n = N_DEV
        rows, width = emb.shape
        vocab = rows * n
        n_tok = tok_ids.shape[0]
        me = lax.axis_index("fsdp")

        def send(bit):
            pairs = [(d, d ^ bit) for d in range(n)]
            return lambda val: lax.ppermute(val, "fsdp", pairs)

        along_x, along_y = send(2), send(4)
        gu = slice_weights(w_gate, w_up)
        gus, downs, embs = [[val, along_x(val), along_y(val)] for val in (gu, w_down, emb)]
        gus.append(along_x(gus[2]))
        downs.append(along_x(downs[2]))
        embs.append(along_y(embs[1]))

        live = loss_mask != 0
        by_id = lax.sort(jnp.where(live, tok_ids * 65536 + tok_labels, vocab * 65536))
        by_label = lax.sort(jnp.where(live, tok_labels * 65536 + tok_ids, vocab * 65536))
        tok = [part.reshape(n_tok // 128, 128) for part in (by_id >> 16, by_id & 65535, by_label >> 16, by_label & 65535)]
        tok = gather_tokens(jnp.concatenate(tok).astype(jnp.int16))
        ids, labels, labels2, ids2 = [tok[:, k * (n_tok // 128):(k + 1) * (n_tok // 128)].astype(I32) for k in range(4)]
        crow = count(ids, labels, me * rows, rows, vocab)
        ccol = count(labels2, ids2, me * rows, rows, vocab)
        n_live = jnp.sum(ids < vocab).astype(F32)
        coef = (1.0 / n_live).reshape(1, 1)
        loss, de, dwg, dwu, dwd = run_step(coef, embs, gus, downs, crow, ccol, g1.reshape(1, width), g2.reshape(1, width))
        return loss[0, 0], de, dwg, dwu, dwd

    row_spec = P("fsdp", None)
    tok_spec = P("fsdp")
    return jax.shard_map(device_step, mesh=mesh, in_specs=(tok_spec, tok_spec, tok_spec, row_spec, P(), P(), row_spec, row_spec, row_spec), out_specs=(P(), row_spec, row_spec, row_spec, row_spec), check_vma=False)
```

```python
import functools

import jax
import jax.numpy as jnp
from jax import lax
from jax.experimental import pallas as pl
from jax.experimental.pallas import tpu as pltpu
from jax.sharding import PartitionSpec as P


NORM_EPS = 1e-6
N_DEV = 8
F32, BF16, I32 = jnp.float32, jnp.bfloat16, jnp.int32
MESH = pl.DeviceIdType.MESH
VMEM_MAX = 66_000_000


def dot_nn(a, b):
    return jnp.dot(a, b, preferred_element_type=F32)


def dot_nt(a, b):
    return lax.dot_general(a, b, (((1,), (1,)), ((), ())), preferred_element_type=F32)


def dot_tn(a, b):
    return lax.dot_general(a, b, (((0,), (0,)), ((), ())), preferred_element_type=F32)


def flip(me, bit):
    return me + bit - 2 * bit * lax.rem(me // bit, 2)


def barrier_with(peers):
    sem = pltpu.get_barrier_semaphore()
    for peer in peers:
        pl.semaphore_signal(sem, inc=1, device_id=(peer,), device_id_type=MESH)
    pl.semaphore_wait(sem, len(peers))


class Gather:
    def __init__(self, slot, half, send_sem, recv_sem, me, own=None):
        self.slot, self.half, self.ss, self.rs, self.me = slot, half, send_sem, recv_sem, me
        self.own = slot(me) if own is None else own
        self.pc, self.px, self.py = flip(me, 1), flip(me, 2), flip(me, 4)
        self.pd = flip(self.px, 4)

    def copy(self, kind, src, dst, peer):
        return pltpu.make_async_remote_copy(
            src_ref=src, dst_ref=dst, send_sem=self.ss(kind), recv_sem=self.rs(kind), device_id=(peer,), device_id_type=MESH
        )

    def describe(self, kind):
        me, px, py, pd, pc = self.me, self.px, self.py, self.pd, self.pc
        if kind == 0:
            return self.copy(0, self.own, self.slot(me), px)
        if kind == 1:
            return self.copy(1, self.own, self.slot(me), py)
        if kind == 2:
            return self.copy(2, self.half(px, 0), self.half(px, 0), py)
        if kind == 3:
            return self.copy(3, self.half(py, 1), self.half(py, 1), px)
        if kind == 4:
            return self.copy(4, self.own, self.slot(me), pc)
        if kind == 5:
            return self.copy(5, self.slot(px), self.slot(px), pc)
        if kind == 6:
            return self.copy(6, self.slot(py), self.slot(py), pc)
        return self.copy(kind, self.half(pd, kind - 7), self.half(pd, kind - 7), pc)

    def start(self):
        for kind in (0, 1, 4):
            self.describe(kind).start()

    def forward_near(self):
        self.describe(0).wait_recv()
        self.describe(2).start()
        self.describe(5).start()
        self.describe(1).wait_recv()
        self.describe(3).start()
        self.describe(6).start()

    def forward_far(self):
        self.describe(2).wait_recv()
        self.describe(7).start()
        self.describe(3).wait_recv()
        self.describe(8).start()

    def wait_recv(self, *kinds):
        for kind in kinds:
            self.describe(kind).wait_recv()

    def wait_sends(self):
        for kind in range(9):
            self.describe(kind).wait_send()


def slice_kernel(gate, up, out):
    n, _, fs = out.shape
    rows = gate.shape[0]
    for k in range(n):
        out[k, 0:rows, :] = gate[:, k * fs:(k + 1) * fs]
        out[k, rows:2 * rows, :] = up[:, k * fs:(k + 1) * fs]


def slice_weights(gate, up):
    rows, width = gate.shape
    return pl.pallas_call(
        slice_kernel,
        out_shape=jax.ShapeDtypeStruct((N_DEV, 2 * rows, width // N_DEV), gate.dtype),
        cost_estimate=pl.CostEstimate(flops=1_000_000, bytes_accessed=1_000_000, transcendentals=0),
        name="slices",
    )(gate, up)


def token_kernel(tok, tok_o, send_sem, recv_sem, local_sem):
    me = lax.axis_index("fsdp")
    n = tok_o.shape[0]
    peers = [lax.rem(me + k, n) for k in range(1, n)]
    barrier_with(peers)
    copies = [
        pltpu.make_async_remote_copy(
            src_ref=tok, dst_ref=tok_o.at[me], send_sem=send_sem.at[k], recv_sem=recv_sem.at[k], device_id=(peer,), device_id_type=MESH
        )
        for k, peer in enumerate(peers)
    ]
    local = pltpu.make_async_copy(tok, tok_o.at[me], local_sem)
    for copy in copies:
        copy.start()
    local.start()
    for copy in copies:
        copy.wait()
    local.wait()


def gather_tokens(tok):
    dma = pltpu.SemaphoreType.DMA
    return pl.pallas_call(
        token_kernel,
        out_shape=jax.ShapeDtypeStruct((N_DEV,) + tok.shape, tok.dtype),
        in_specs=[pl.BlockSpec(memory_space=pltpu.VMEM)],
        out_specs=pl.BlockSpec(memory_space=pl.ANY),
        scratch_shapes=[dma((N_DEV - 1,)), dma((N_DEV - 1,)), dma],
        compiler_params=pltpu.CompilerParams(collective_id=0, has_side_effects=True),
        cost_estimate=pl.CostEstimate(flops=5_000_000_000, bytes_accessed=1_000_000, transcendentals=0),
        name="tokens",
    )(tok)


def count_kernel(bounds, keys_a, keys_b, out_a, out_b, list_a, list_b, acc_a, acc_b, in_sem, out_sem):
    n_src = N_DEV
    per = list_a.shape[0] // n_src
    size = acc_a.shape[0]
    BLK = 256
    unroll = 16
    jobs = [(keys_a, out_a, list_a, acc_a), (keys_b, out_b, list_b, acc_b)]
    loads = [pltpu.make_async_copy(keys, held, in_sem.at[k]) for k, (keys, _o, held, _a) in enumerate(jobs)]
    stores = [pltpu.make_async_copy(acc, out, out_sem.at[k]) for k, (_k, out, _h, acc) in enumerate(jobs)]
    loads[0].start()
    lanes = lax.broadcasted_iota(I32, (1, 128), 1)

    for which, (_keys, _out, held, acc) in enumerate(jobs):
        def clear(i, _):
            acc[pl.ds(i * BLK, BLK), :] = jnp.zeros((BLK, 128), F32)
            return 0

        lax.fori_loop(0, size // BLK, clear, 0)
        loads[which].wait()
        if which == 0:
            loads[1].start()

        def group(pos, end, whole):
            places, old, delta = [], [], None
            for k in range(unroll):
                key = held[pos + k] if whole else held[jnp.minimum(pos + k, end - 1)]
                places.append(key >> 7)
                mark = key & 127 if whole else jnp.where(pos + k < end, key & 127, -1)
                here = jnp.where(lanes == mark, 1.0, 0.0)
                delta = here if k == 0 else here + delta * jnp.where(places[k] == places[k - 1], 1.0, 0.0)
                old.append(acc[pl.ds(places[k], 1), :] + delta)
            for place, val in zip(places, old):
                acc[pl.ds(place, 1), :] = val

        def source(src, _):
            begin = bounds[which * 2 * n_src + src] + src * per
            end = bounds[which * 2 * n_src + n_src + src] + src * per
            n_whole = lax.shift_right_logical(end - begin, 4)

            def step(i, _):
                group(begin + i * unroll, end, True)
                return 0

            lax.fori_loop(0, n_whole, step, 0)

            @pl.when(begin + n_whole * unroll < end)
            def _():
                group(begin + n_whole * unroll, end, False)

            return 0

        lax.fori_loop(0, n_src, source, 0)
        stores[which].start()
    for store in stores:
        store.wait()


def count(pairs, first, rows, cols):
    bounds, keys, tiles = [], [], cols // 128
    for major, minor in pairs:
        bounds.append(jnp.sum(major < first, axis=(1, 2), dtype=I32))
        bounds.append(jnp.sum(major < first + rows, axis=(1, 2), dtype=I32))
        row = major - first
        keys.append(((((row >> 3) * tiles + (minor >> 7)) * 8 + (row & 7)) * 128 + (minor & 127)).reshape(-1))
    any_spec = pl.BlockSpec(memory_space=pl.ANY)
    tall = (rows * cols // 128, 128)
    outs = pl.pallas_call(
        count_kernel,
        out_shape=(jax.ShapeDtypeStruct(tall, F32),) * 2,
        in_specs=[pl.BlockSpec(memory_space=pltpu.SMEM), any_spec, any_spec],
        out_specs=(any_spec,) * 2,
        scratch_shapes=[pltpu.SMEM(keys[0].shape, I32)] * 2 + [pltpu.VMEM(tall, F32)] * 2 + [pltpu.SemaphoreType.DMA((2,))] * 2,
        cost_estimate=pl.CostEstimate(flops=30_000_000_000, bytes_accessed=16_000_000, transcendentals=0),
        name="count",
    )(jnp.concatenate(bounds), *keys)
    return [out.reshape(rows // 8, tiles, 8, 128) for out in outs]


def finish_kernel(de, got_g, got_u, dwd, de_o, dwg_o, dwu_o, dwd_o):
    n, _, fs = got_g.shape
    de_o[...] = de[...]
    dwd_o[...] = dwd[...]
    for k in range(n):
        dwg_o[:, k * fs:(k + 1) * fs] = got_g[k]
        dwu_o[:, k * fs:(k + 1) * fs] = got_u[k]


def finish(de, got_g, got_u, dwd):
    n, out_rows, fs = got_g.shape
    wide = jax.ShapeDtypeStruct((out_rows, n * fs), F32)
    return pl.pallas_call(finish_kernel, out_shape=(jax.ShapeDtypeStruct(de.shape, F32), wide, wide, jax.ShapeDtypeStruct(dwd.shape, F32)), name="finish")(
        de, got_g, got_u, dwd
    )


def step_kernel(
    coef_ref, emb_me, emb_x, emb_y, emb_d, gu_me, gu_x, gu_y, gu_d, wd_me, wd_x, wd_y, wd_d, crow_hbm, ccol_hbm, g1_ref, g2_ref,
    loss_o, de_o, got_g, got_u, dwd_o,
    emb, wg, wu, wd, crow, ccol, hn, dh, a_all, p_own, q_own, p_all, q_all, logits, dlog, h_wide, dh_wide, acc, stat, stat_col,
    dwg, dwu, u_late, load_sem, pair_s, pair_r, col_sem, hs, hr, ds_, dr, st_s, st_r, ws, wr,
):
    me = lax.axis_index("fsdp")
    n, rows, width = emb.shape
    fs = wg.shape[2]
    out_rows = got_g.shape[1]
    coef = coef_ref[0, 0]
    RB = 64
    lt = rows // 128
    peers = [lax.rem(me + k, n) for k in range(1, n)]

    pc, px, py = flip(me, 1), flip(me, 2), flip(me, 4)
    pd = flip(px, 4)
    devs = [me, px, py, pd]
    parts = []
    for dev, gu, down in zip(devs, [gu_me, gu_x, gu_y, gu_d], [wd_me, wd_x, wd_y, wd_d]):
        at = pl.ds(dev * out_rows, out_rows)
        parts.append((gu.at[:, 0:out_rows, :], wg.at[:, at, :]))
        parts.append((gu.at[:, out_rows:2 * out_rows, :], wu.at[:, at, :]))
        parts.append((down, wd.at[dev]))
    n_weight = len(parts)
    for dev, block in zip(devs, [emb_me, emb_x, emb_y, emb_d]):
        parts.append((block, emb.at[dev]))
    loads = [pltpu.make_async_copy(src, dst, load_sem.at[k]) for k, (src, dst) in enumerate(parts)]
    pairs = [
        pltpu.make_async_remote_copy(
            src_ref=src, dst_ref=dst, send_sem=pair_s.at[k], recv_sem=pair_r.at[k], device_id=(pc,), device_id_type=MESH
        )
        for k, (src, dst) in enumerate(parts)
    ]
    crow_load = pltpu.make_async_copy(crow_hbm, crow, load_sem.at[len(parts)])

    def col_load(dev, slot):
        return pltpu.make_async_copy(ccol_hbm.at[:, pl.ds(dev * lt, lt)], ccol.at[slot], col_sem.at[slot])

    loads[n_weight].start()
    for load in loads[:n_weight]:
        load.start()
    barrier_with(peers)
    for pair in pairs:
        pair.start()
    for load in loads[n_weight + 1:]:
        load.start()
    crow_load.start()

    def gather_of(buf, ss, rs):
        half = rows // 2
        return Gather(lambda d: buf.at[d], lambda d, i: buf.at[d, pl.ds(i * half, half)], lambda c: ss.at[c], lambda c: rs.at[c], me)

    hn_g, dh_g = gather_of(hn, hs, hr), gather_of(dh, ds_, dr)
    g1, g2 = g1_ref[...], g2_ref[...]

    loads[n_weight].wait()

    def norm_rows(i, _):
        dev, at = i // (rows // RB), pl.ds(lax.rem(i, rows // RB) * RB, RB)
        x = emb[dev, at, :].astype(F32)
        inv = lax.rsqrt(jnp.mean(x * x, axis=-1, keepdims=True) + NORM_EPS)
        a_all[dev, at, :] = (x * inv * g1).astype(BF16)
        return 0

    per_dev = rows // RB
    lax.fori_loop(me * per_dev, (me + 1) * per_dev, norm_rows, 0)

    for load, pair in zip(loads[:n_weight], pairs[:n_weight]):
        load.wait()
        pair.wait_recv()
    acc[...] = jnp.zeros_like(acc)

    def forward(j, _):
        a = a_all[me]
        p = dot_nn(a, wg[j]).astype(BF16)
        q = dot_nn(a, wu[j]).astype(BF16)
        p_own[j], q_own[j] = p, q
        p, q = p.astype(F32), q.astype(F32)
        u = (p * jax.nn.sigmoid(p) * q).astype(BF16)
        acc[...] += dot_nn(u, wd[j])
        return 0

    lax.fori_loop(0, n, forward, 0)

    def hidden(i, _):
        at = pl.ds(i * RB, RB)
        h = (emb[me, at, :].astype(F32) + acc[at, :]).astype(BF16).astype(F32)
        h_wide[at, :] = h
        inv = lax.rsqrt(jnp.mean(h * h, axis=-1, keepdims=True) + NORM_EPS)
        hn[me, at, :] = (h * inv * g2).astype(BF16)
        return 0

    lax.fori_loop(0, per_dev, hidden, 0)
    hn_g.start()
    for load in loads[n_weight + 1:]:
        load.wait()
    for pair in pairs[n_weight:]:
        pair.wait_recv()

    def logit(v, _):
        logits[v] = dot_nt(hn[me], emb[v])
        return 0

    lax.fori_loop(0, n, logit, 0)
    crow_load.wait()

    def softmax(i, _):
        at = pl.ds(i * RB, RB)

        def cnt_tile(v, k):
            return crow[pl.ds(i * (RB // 8), RB // 8), v * lt + k].reshape(RB, 128)

        def top(v, m):
            val = logits[v, at, :]
            for k in range(rows // 128):
                m = jnp.maximum(m, val[:, k * 128:(k + 1) * 128])
            return m

        m = jnp.max(lax.fori_loop(0, n, top, jnp.full((RB, 128), -jnp.inf, F32)), axis=-1, keepdims=True)

        def sums(v, carry):
            s, c, pick = carry
            for k in range(lt):
                cut = slice(k * 128, (k + 1) * 128)
                val, cnt = logits[v, at, cut], cnt_tile(v, k)
                ex = jnp.exp(val - m)
                logits[v, at, cut] = ex
                s, c, pick = s + ex, c + cnt, pick + cnt * val
            return s, c, pick

        zero = jnp.zeros((RB, 128), F32)
        s, c, pick = [jnp.sum(val, axis=-1, keepdims=True) for val in lax.fori_loop(0, n, sums, (zero, zero, zero))]
        lse = m + jnp.log(s)
        lane = lax.broadcasted_iota(I32, (RB, 128), 1)
        stat_col[at, :] = jnp.where(lane == 0, lse, jnp.where(lane == 1, c * coef, jnp.where(lane == 2, c * lse - pick, 0.0)))
        scale = c * coef / s

        def grad(v, _):
            for k in range(lt):
                cut = slice(k * 128, (k + 1) * 128)
                dlog[v, at, cut] = (logits[v, at, cut] * scale - cnt_tile(v, k) * coef).astype(BF16)
            return 0

        lax.fori_loop(0, n, grad, 0)
        return 0

    lax.fori_loop(0, per_dev, softmax, 0)
    stat[me] = jnp.transpose(stat_col[...])[0:8, :]

    acc[...] = jnp.zeros_like(acc)

    def dhn_step(v, _):
        acc[...] += dot_nn(dlog[v], emb[v])
        return 0

    lax.fori_loop(0, n, dhn_step, 0)
    stat_copies = [
        pltpu.make_async_remote_copy(
            src_ref=stat.at[me], dst_ref=stat.at[me], send_sem=st_s.at[k], recv_sem=st_r.at[k], device_id=(peer,), device_id_type=MESH
        )
        for k, peer in enumerate(peers)
    ]
    for copy in stat_copies:
        copy.start()

    def dhidden(i, _):
        at = pl.ds(i * RB, RB)
        h, scaled = h_wide[at, :], acc[at, :] * g2
        inv = lax.rsqrt(jnp.mean(h * h, axis=-1, keepdims=True) + NORM_EPS)
        grad = inv * (scaled - h * (inv * inv) * jnp.mean(scaled * h, axis=-1, keepdims=True))
        dh_wide[at, :] = grad
        dh[me, at, :] = grad.astype(BF16)
        return 0

    lax.fori_loop(0, per_dev, dhidden, 0)
    dh_g.start()
    hn_g.forward_near()

    lax.fori_loop(0, me * per_dev, norm_rows, 0)
    lax.fori_loop((me + 1) * per_dev, n * per_dev, norm_rows, 0)

    def slice_forward(s, _):
        p_all[s] = dot_nn(a_all[s], wg[me]).astype(BF16)
        q_all[s] = dot_nn(a_all[s], wu[me]).astype(BF16)
        return 0

    lax.fori_loop(0, n, slice_forward, 0)

    acc[...] = jnp.zeros_like(acc)

    def act_back(dact, p, q):
        sig = jax.nn.sigmoid(p)
        gated = p * sig
        dq = (dact * gated).astype(BF16)
        dp = (dact * q * sig * (1.0 + p * (1.0 - sig))).astype(BF16)
        return dp, dq, (gated * q).astype(BF16)

    def backward(j, _):
        dact = dot_nt(dh[me], wd[j])
        dp, dq, _u = act_back(dact, p_own[j].astype(F32), q_own[j].astype(F32))
        acc[...] += dot_nt(dp, wg[j]) + dot_nt(dq, wu[j])
        return 0

    lax.fori_loop(0, n, backward, 0)

    def dinput(i, _):
        at = pl.ds(i * RB, RB)
        x, scaled = emb[me, at, :].astype(F32), acc[at, :] * g1
        inv = lax.rsqrt(jnp.mean(x * x, axis=-1, keepdims=True) + NORM_EPS)
        de_o[at, :] = dh_wide[at, :] + inv * (scaled - x * (inv * inv) * jnp.mean(scaled * x, axis=-1, keepdims=True))
        return 0

    lax.fori_loop(0, per_dev, dinput, 0)
    for copy in stat_copies:
        copy.wait_recv()

    def head(dev, slot):
        col_load(dev, slot).wait()
        logits[0] = dot_nt(emb[me], hn[dev])
        lse, weight = stat[dev, 0:1, :], stat[dev, 1:2, :]

        def grad(i, _):
            at = pl.ds(i * RB, RB)
            for k in range(lt):
                cut = slice(k * 128, (k + 1) * 128)
                prob = jnp.exp(logits[0, at, cut] - lse[:, cut]) * weight[:, cut]
                cnt = ccol[slot, pl.ds(i * (RB // 8), RB // 8), k].reshape(RB, 128)
                dlog[0, at, cut] = (prob - cnt * coef).astype(BF16)
            return 0

        lax.fori_loop(0, per_dev, grad, 0)
        de_o[...] += dot_nn(dlog[0], hn[dev])

    dwg[...] = jnp.zeros_like(dwg)
    dwu[...] = jnp.zeros_like(dwu)
    dwd_o[...] = jnp.zeros_like(dwd_o)

    def act_grads(dev):
        dact = dot_nt(dh[dev], wd[me])
        return act_back(dact, p_all[dev].astype(F32), q_all[dev].astype(F32))

    def weights(dev):
        dp, dq, u = act_grads(dev)
        dwd_o[...] += dot_tn(u, dh[dev])
        dwg[...] += dot_tn(a_all[dev], dp)
        dwu[...] += dot_tn(a_all[dev], dq)

    def exchange(k, peer, src, dst, row):
        return pltpu.make_async_remote_copy(
            src_ref=src.at[pl.ds(pl.multiple_of(peer * out_rows, out_rows), out_rows), :],
            dst_ref=dst.at[me],
            send_sem=ws.at[row, k], recv_sem=wr.at[row, k], device_id=(peer,), device_id_type=MESH,
        )

    swaps_g = [exchange(k, peer, dwg, got_g, 0) for k, peer in enumerate(peers)]
    swaps_u = [exchange(k, peer, dwu, got_u, 1) for k, peer in enumerate(peers)]

    order = [me, pc, px, py, flip(px, 1), flip(py, 1), pd, flip(pd, 1)]
    col_load(order[0], 0).start()

    def heads(*places):
        for k in places:
            if k + 1 < n:
                col_load(order[k + 1], (k + 1) % 2).start()
            head(order[k], k % 2)

    hn_g.wait_recv(4)
    heads(0, 1)
    dh_g.forward_near()
    heads(2, 3)
    hn_g.wait_recv(5, 6)
    heads(4, 5)
    weights(order[0])
    dh_g.wait_recv(4)
    weights(order[1])
    weights(order[2])
    weights(order[3])
    hn_g.forward_far()
    dh_g.wait_recv(5, 6)
    weights(order[4])
    weights(order[5])
    heads(6)
    hn_g.wait_recv(7, 8)
    heads(7)
    dh_g.forward_far()
    for k, kinds in ((0, ()), (1, (7, 8))):
        dh_g.wait_recv(*kinds)
        dev = order[6 + k]
        p_all[dev], q_all[dev], u_late[k] = act_grads(dev)
        dwg[...] += dot_tn(a_all[dev], p_all[dev])
    for swap in swaps_g:
        swap.start()
    for dev in order[6:]:
        dwu[...] += dot_tn(a_all[dev], q_all[dev])
    for swap in swaps_u:
        swap.start()
    for k, dev in enumerate(order[6:]):
        dwd_o[...] += dot_tn(u_late[k], dh[dev])
    swaps = swaps_g + swaps_u
    mine = pl.ds(pl.multiple_of(me * out_rows, out_rows), out_rows)
    got_g[me] = dwg[mine, :]
    got_u[me] = dwu[mine, :]
    total = jnp.zeros((1, rows), F32)
    for s in range(n):
        total = total + stat[s, 2:3, :]
    loss_o[...] = jnp.sum(total, axis=-1, keepdims=True) * coef + jnp.zeros((1, 128), F32)
    for copy in stat_copies:
        copy.wait_send()
    hn_g.wait_sends()
    dh_g.wait_sends()
    for pair in pairs:
        pair.wait_send()
    for swap in swaps:
        swap.wait()


def run_step(coef, embs, gus, downs, crow, ccol, g1, g2):
    n = N_DEV
    rows, width = embs[0].shape
    fs = gus[0].shape[2]
    out_rows = width // n
    any_spec = pl.BlockSpec(memory_space=pl.ANY)
    vmem = pl.BlockSpec(memory_space=pltpu.VMEM)
    dma = pltpu.SemaphoreType.DMA
    return pl.pallas_call(
        step_kernel,
        out_shape=(
            jax.ShapeDtypeStruct((1, 128), F32),
            jax.ShapeDtypeStruct((rows, width), F32),
            jax.ShapeDtypeStruct((n, out_rows, fs), F32),
            jax.ShapeDtypeStruct((n, out_rows, fs), F32),
            jax.ShapeDtypeStruct((fs, width), F32),
        ),
        in_specs=[pl.BlockSpec(memory_space=pltpu.SMEM)] + [any_spec] * 14 + [vmem] * 2,
        out_specs=(vmem,) * 5,
        scratch_shapes=[
            pltpu.VMEM((n, rows, width), BF16),
            pltpu.VMEM((n, width, fs), BF16),
            pltpu.VMEM((n, width, fs), BF16),
            pltpu.VMEM((n, fs, width), BF16),
            pltpu.VMEM((rows // 8, n * rows // 128, 8, 128), F32),
            pltpu.VMEM((2, rows // 8, rows // 128, 8, 128), F32),
            pltpu.VMEM((n, rows, width), BF16),
            pltpu.VMEM((n, rows, width), BF16),
            pltpu.VMEM((n, rows, width), BF16),
            pltpu.VMEM((n, rows, fs), BF16),
            pltpu.VMEM((n, rows, fs), BF16),
            pltpu.VMEM((n, rows, fs), BF16),
            pltpu.VMEM((n, rows, fs), BF16),
            pltpu.VMEM((n, rows, rows), F32),
            pltpu.VMEM((n, rows, rows), BF16),
            pltpu.VMEM((rows, width), F32),
            pltpu.VMEM((rows, width), F32),
            pltpu.VMEM((rows, width), F32),
            pltpu.VMEM((n, 8, rows), F32),
            pltpu.VMEM((rows, 128), F32),
            pltpu.VMEM((width, fs), F32),
            pltpu.VMEM((width, fs), F32),
            pltpu.VMEM((2, rows, fs), BF16),
            dma((17,)), dma((16,)), dma((16,)), dma((2,)), dma((9,)), dma((9,)), dma((9,)), dma((9,)), dma((n - 1,)), dma((n - 1,)), dma((2, n - 1)), dma((2, n - 1)),
        ],
        compiler_params=pltpu.CompilerParams(collective_id=1, has_side_effects=True, vmem_limit_bytes=VMEM_MAX),
        name="step",
    )(coef, *embs, *gus, *downs, crow, ccol, g1, g2)


def solution(mesh):
    def device_step(tok_ids, tok_labels, loss_mask, emb, g1, g2, w_gate, w_up, w_down):
        n = N_DEV
        rows, width = emb.shape
        vocab = rows * n
        n_tok = tok_ids.shape[0]
        me = lax.axis_index("fsdp")

        def send(bit):
            pairs = [(d, d ^ bit) for d in range(n)]
            return lambda val: lax.ppermute(val, "fsdp", pairs)

        along_x, along_y = send(2), send(4)
        gu = slice_weights(w_gate, w_up)
        gus, downs, embs = [[val, along_x(val), along_y(val)] for val in (gu, w_down, emb)]

        live = loss_mask != 0
        by_id = lax.sort(jnp.where(live, tok_ids * 65536 + tok_labels, vocab * 65536))
        by_label = lax.sort(jnp.where(live, tok_labels * 65536 + tok_ids, vocab * 65536))
        tok = [part.reshape(n_tok // 128, 128) for part in (by_id >> 16, by_id & 65535, by_label >> 16, by_label & 65535)]
        tok = gather_tokens(jnp.concatenate(tok).astype(jnp.int16))
        tok, gus[2], downs[2], embs[1] = lax.optimization_barrier((tok, gus[2], downs[2], embs[1]))
        gus.append(along_x(gus[2]))
        downs.append(along_x(downs[2]))
        embs.append(along_y(embs[1]))
        ids, labels, labels2, ids2 = [tok[:, k * (n_tok // 128):(k + 1) * (n_tok // 128)].astype(I32) for k in range(4)]
        crow, ccol = count([(ids, labels), (labels2, ids2)], me * rows, rows, vocab)
        n_live = jnp.sum(ids < vocab).astype(F32)
        coef = (1.0 / n_live).reshape(1, 1)
        loss, *grads = run_step(coef, embs, gus, downs, crow, ccol, g1.reshape(1, width), g2.reshape(1, width))
        return (loss[0, 0], *finish(*grads))

    row_spec = P("fsdp", None)
    tok_spec = P("fsdp")
    return jax.shard_map(device_step, mesh=mesh, in_specs=(tok_spec, tok_spec, tok_spec, row_spec, P(), P(), row_spec, row_spec, row_spec), out_specs=(P(), row_spec, row_spec, row_spec, row_spec), check_vma=False)
```

```python
import functools

import jax
import jax.numpy as jnp
from jax import lax
from jax.experimental import pallas as pl
from jax.experimental.pallas import tpu as pltpu
from jax.sharding import PartitionSpec as P


NORM_EPS = 1e-6
N_DEV = 8
F32, BF16, I32 = jnp.float32, jnp.bfloat16, jnp.int32
MESH = pl.DeviceIdType.MESH
VMEM_MAX = 66_000_000


class Phases:
    def __init__(self):
        self.now = None

    def __call__(self, name=None):
        if self.now is not None:
            self.now.__exit__(None, None, None)
        self.now = jax.named_scope(name) if name else None
        if self.now is not None:
            self.now.__enter__()


def dot_nn(a, b):
    return jnp.dot(a, b, preferred_element_type=F32)


def dot_nt(a, b):
    return lax.dot_general(a, b, (((1,), (1,)), ((), ())), preferred_element_type=F32)


def dot_tn(a, b):
    return lax.dot_general(a, b, (((0,), (0,)), ((), ())), preferred_element_type=F32)


def flip(me, bit):
    return me + bit - 2 * bit * lax.rem(me // bit, 2)


def barrier_with(peers):
    sem = pltpu.get_barrier_semaphore()
    for peer in peers:
        pl.semaphore_signal(sem, inc=1, device_id=(peer,), device_id_type=MESH)
    pl.semaphore_wait(sem, len(peers))


class Gather:
    def __init__(self, slot, half, send_sem, recv_sem, me, own=None):
        self.slot, self.half, self.ss, self.rs, self.me = slot, half, send_sem, recv_sem, me
        self.own = slot(me) if own is None else own
        self.pc, self.px, self.py = flip(me, 1), flip(me, 2), flip(me, 4)
        self.pd = flip(self.px, 4)

    def copy(self, kind, src, dst, peer):
        return pltpu.make_async_remote_copy(
            src_ref=src, dst_ref=dst, send_sem=self.ss(kind), recv_sem=self.rs(kind), device_id=(peer,), device_id_type=MESH
        )

    def describe(self, kind):
        me, px, py, pd, pc = self.me, self.px, self.py, self.pd, self.pc
        if kind == 0:
            return self.copy(0, self.own, self.slot(me), px)
        if kind == 1:
            return self.copy(1, self.own, self.slot(me), py)
        if kind == 2:
            return self.copy(2, self.half(px, 0), self.half(px, 0), py)
        if kind == 3:
            return self.copy(3, self.half(py, 1), self.half(py, 1), px)
        if kind == 4:
            return self.copy(4, self.own, self.slot(me), pc)
        if kind == 5:
            return self.copy(5, self.slot(px), self.slot(px), pc)
        if kind == 6:
            return self.copy(6, self.slot(py), self.slot(py), pc)
        return self.copy(kind, self.half(pd, kind - 7), self.half(pd, kind - 7), pc)

    def start(self):
        for kind in (0, 1, 4):
            self.describe(kind).start()

    def forward_pair(self):
        for kind in (0, 1):
            self.describe(kind).wait_recv()
            self.describe(5 + kind).start()

    def forward_cross(self):
        self.describe(2).start()
        self.describe(3).start()

    def forward_far(self):
        self.describe(2).wait_recv()
        self.describe(7).start()
        self.describe(3).wait_recv()
        self.describe(8).start()

    def wait_recv(self, *kinds):
        for kind in kinds:
            self.describe(kind).wait_recv()

    def wait_sends(self):
        for kind in range(9):
            self.describe(kind).wait_send()


def slice_kernel(gate, up, out):
    n, _, fs = out.shape
    rows = gate.shape[0]
    for k in range(n):
        out[k, 0:rows, :] = gate[:, k * fs:(k + 1) * fs]
        out[k, rows:2 * rows, :] = up[:, k * fs:(k + 1) * fs]


def slice_weights(gate, up):
    rows, width = gate.shape
    return pl.pallas_call(
        slice_kernel,
        out_shape=jax.ShapeDtypeStruct((N_DEV, 2 * rows, width // N_DEV), gate.dtype),
        cost_estimate=pl.CostEstimate(flops=1_000_000, bytes_accessed=1_000_000, transcendentals=0),
        name="slices",
    )(gate, up)


def token_kernel(tok, tok_o, send_sem, recv_sem, local_sem):
    me = lax.axis_index("fsdp")
    n = tok_o.shape[0]
    peers = [lax.rem(me + k, n) for k in range(1, n)]
    barrier_with(peers)
    copies = [
        pltpu.make_async_remote_copy(
            src_ref=tok, dst_ref=tok_o.at[me], send_sem=send_sem.at[k], recv_sem=recv_sem.at[k], device_id=(peer,), device_id_type=MESH
        )
        for k, peer in enumerate(peers)
    ]
    local = pltpu.make_async_copy(tok, tok_o.at[me], local_sem)
    for copy in copies:
        copy.start()
    local.start()
    for copy in copies:
        copy.wait()
    local.wait()


def gather_tokens(tok):
    dma = pltpu.SemaphoreType.DMA
    return pl.pallas_call(
        token_kernel,
        out_shape=jax.ShapeDtypeStruct((N_DEV,) + tok.shape, tok.dtype),
        in_specs=[pl.BlockSpec(memory_space=pltpu.VMEM)],
        out_specs=pl.BlockSpec(memory_space=pl.ANY),
        scratch_shapes=[dma((N_DEV - 1,)), dma((N_DEV - 1,)), dma],
        compiler_params=pltpu.CompilerParams(collective_id=0, has_side_effects=True),
        cost_estimate=pl.CostEstimate(flops=5_000_000_000, bytes_accessed=1_000_000, transcendentals=0),
        name="tokens",
    )(tok)


def count_kernel(bounds, keys_a, keys_b, out_a, out_b, list_a, list_b, acc_a, acc_b, in_sem, out_sem):
    n_src = N_DEV
    per = list_a.shape[0] // n_src
    size = acc_a.shape[0]
    BLK = 256
    unroll = 16
    jobs = [(keys_a, out_a, list_a, acc_a), (keys_b, out_b, list_b, acc_b)]
    loads = [pltpu.make_async_copy(keys, held, in_sem.at[k]) for k, (keys, _o, held, _a) in enumerate(jobs)]
    stores = [pltpu.make_async_copy(acc, out, out_sem.at[k]) for k, (_k, out, _h, acc) in enumerate(jobs)]
    loads[0].start()
    lanes = lax.broadcasted_iota(I32, (1, 128), 1)

    for which, (_keys, _out, held, acc) in enumerate(jobs):
        def clear(i, _):
            acc[pl.ds(i * BLK, BLK), :] = jnp.zeros((BLK, 128), F32)
            return 0

        lax.fori_loop(0, size // BLK, clear, 0)
        loads[which].wait()
        if which == 0:
            loads[1].start()

        def group(pos, end, whole):
            places, old, delta = [], [], None
            for k in range(unroll):
                key = held[pos + k] if whole else held[jnp.minimum(pos + k, end - 1)]
                places.append(key >> 7)
                mark = key & 127 if whole else jnp.where(pos + k < end, key & 127, -1)
                here = jnp.where(lanes == mark, 1.0, 0.0)
                delta = here if k == 0 else here + delta * jnp.where(places[k] == places[k - 1], 1.0, 0.0)
                old.append(acc[pl.ds(places[k], 1), :] + delta)
            for place, val in zip(places, old):
                acc[pl.ds(place, 1), :] = val

        def source(src, _):
            begin = bounds[which * 2 * n_src + src] + src * per
            end = bounds[which * 2 * n_src + n_src + src] + src * per
            n_whole = lax.shift_right_logical(end - begin, 4)

            def step(i, _):
                group(begin + i * unroll, end, True)
                return 0

            lax.fori_loop(0, n_whole, step, 0)

            @pl.when(begin + n_whole * unroll < end)
            def _():
                group(begin + n_whole * unroll, end, False)

            return 0

        lax.fori_loop(0, n_src, source, 0)
        stores[which].start()
    for store in stores:
        store.wait()


def count(pairs, first, rows, cols):
    bounds, keys, tiles = [], [], cols // 128
    for major, minor in pairs:
        bounds.append(jnp.sum(major < first, axis=(1, 2), dtype=I32))
        bounds.append(jnp.sum(major < first + rows, axis=(1, 2), dtype=I32))
        row = major - first
        keys.append(((((row >> 3) * tiles + (minor >> 7)) * 8 + (row & 7)) * 128 + (minor & 127)).reshape(-1))
    any_spec = pl.BlockSpec(memory_space=pl.ANY)
    tall = (rows * cols // 128, 128)
    outs = pl.pallas_call(
        count_kernel,
        out_shape=(jax.ShapeDtypeStruct(tall, F32),) * 2,
        in_specs=[pl.BlockSpec(memory_space=pltpu.SMEM), any_spec, any_spec],
        out_specs=(any_spec,) * 2,
        scratch_shapes=[pltpu.SMEM(keys[0].shape, I32)] * 2 + [pltpu.VMEM(tall, F32)] * 2 + [pltpu.SemaphoreType.DMA((2,))] * 2,
        cost_estimate=pl.CostEstimate(flops=30_000_000_000, bytes_accessed=16_000_000, transcendentals=0),
        name="count",
    )(jnp.concatenate(bounds), *keys)
    return [out.reshape(rows // 8, tiles, 8, 128) for out in outs]


def finish_kernel(de, got_g, got_u, dwd, de_o, dwg_o, dwu_o, dwd_o):
    n, _, fs = got_g.shape
    de_o[...] = de[...]
    dwd_o[...] = dwd[...]
    for k in range(n):
        dwg_o[:, k * fs:(k + 1) * fs] = got_g[k]
        dwu_o[:, k * fs:(k + 1) * fs] = got_u[k]


def finish(de, got_g, got_u, dwd):
    n, out_rows, fs = got_g.shape
    wide = jax.ShapeDtypeStruct((out_rows, n * fs), F32)
    return pl.pallas_call(finish_kernel, out_shape=(jax.ShapeDtypeStruct(de.shape, F32), wide, wide, jax.ShapeDtypeStruct(dwd.shape, F32)), name="finish")(
        de, got_g, got_u, dwd
    )


def step_kernel(
    coef_ref, emb_me, emb_x, emb_y, emb_d, gu_me, gu_x, gu_y, gu_d, wd_me, wd_x, wd_y, wd_d, crow_hbm, ccol_hbm, g1_ref, g2_ref,
    loss_o, de_o, got_g, got_u, dwd_o,
    emb, wg, wu, wd, cnt, hn, dh, a_all, p_own, q_own, q_all, logits, dlog, h_wide, acc, stat, stat_col, top, sums,
    dwg, dwu, load_sem, pair_s, pair_r, hs, hr, ds_, dr, st_s, st_r, ws, wr,
):
    me = lax.axis_index("fsdp")
    n = wg.shape[0]
    rows, width = h_wide.shape
    fs = wg.shape[2]
    out_rows = got_g.shape[1]
    coef = coef_ref[0, 0]
    ph = Phases()
    ph("a_start")
    NB = 128
    RB = 64
    wide = logits.shape[2]
    tiles = wide // 128
    peers = [lax.rem(me + k, n) for k in range(1, n)]

    def block(dev):
        return pl.ds(pl.multiple_of(dev * rows, rows), rows)

    def p_at(s):
        return (slice(None), pl.ds(pl.multiple_of(2 * rows + s * 256, 256), fs))

    mine = block(me)
    pc, px, py = flip(me, 1), flip(me, 2), flip(me, 4)
    pd = flip(px, 4)
    devs = [me, px, py, pd]
    parts = []
    for dev, gu, down in zip(devs, [gu_me, gu_x, gu_y, gu_d], [wd_me, wd_x, wd_y, wd_d]):
        at = pl.ds(dev * out_rows, out_rows)
        parts.append((gu.at[:, 0:out_rows, :], wg.at[:, at, :]))
        parts.append((gu.at[:, out_rows:2 * out_rows, :], wu.at[:, at, :]))
        parts.append((down, wd.at[dev]))
    n_weight = len(parts)
    for dev, part in zip(devs, [emb_me, emb_x, emb_y, emb_d]):
        parts.append((part, emb.at[block(dev), :]))
    loads = [pltpu.make_async_copy(src, dst, load_sem.at[k]) for k, (src, dst) in enumerate(parts)]
    pairs = [
        pltpu.make_async_remote_copy(
            src_ref=src, dst_ref=dst, send_sem=pair_s.at[k], recv_sem=pair_r.at[k], device_id=(pc,), device_id_type=MESH
        )
        for k, (src, dst) in enumerate(parts)
    ]
    row_counts = pltpu.make_async_copy(crow_hbm, cnt, load_sem.at[len(parts)])
    col_counts = pltpu.make_async_copy(ccol_hbm, cnt, load_sem.at[len(parts) + 1])

    for load in loads[n_weight:] + loads[:n_weight]:
        load.start()
    ph("b_barrier")
    barrier_with(peers)
    for pair in pairs:
        pair.start()
    row_counts.start()

    def gather_of(buf, ss, rs):
        half = rows // 2
        return Gather(
            lambda d: buf.at[block(d), :],
            lambda d, i: buf.at[pl.ds(pl.multiple_of(d * rows + i * half, half), half), :],
            lambda c: ss.at[c], lambda c: rs.at[c], me,
        )

    hn_g, dh_g = gather_of(hn, hs, hr), gather_of(dh, ds_, dr)
    g1, g2 = g1_ref[...], g2_ref[...]

    ph("d_norm")

    def norm_rows(dev):
        def norm(i, _):
            at = pl.ds(pl.multiple_of(dev * rows + i * NB, NB), NB)
            x = emb[at, :].astype(F32)
            inv = lax.rsqrt(jnp.mean(x * x, axis=-1, keepdims=True) + NORM_EPS)
            a_all[at, :] = (x * inv * g1).astype(BF16)
            return 0

        lax.fori_loop(0, rows // NB, norm, 0, unroll=2)

    for k, dev in enumerate(devs):
        loads[n_weight + k].wait()
        norm_rows(dev)

    ph("e_waitW")
    for load, pair in zip(loads[:n_weight], pairs[:n_weight]):
        load.wait()
        pair.wait_recv()
    ph("f_fwd")
    acc[...] = jnp.zeros_like(acc)

    def forward(j, _):
        a = a_all[mine, :]
        p = dot_nn(a, wg[j]).astype(BF16)
        q = dot_nn(a, wu[j]).astype(BF16)
        p_own[j], q_own[j] = p, q
        p, q = p.astype(F32), q.astype(F32)
        u = (p * jax.nn.sigmoid(p) * q).astype(BF16)
        acc[...] += dot_nn(u, wd[j])
        return 0

    lax.fori_loop(0, n, forward, 0, unroll=2)
    ph("g_hidden")

    def hidden(i, _):
        at = pl.ds(pl.multiple_of(i * NB, NB), NB)
        row = pl.ds(pl.multiple_of(me * rows + i * NB, NB), NB)
        h = (emb[row, :].astype(F32) + acc[at, :]).astype(BF16).astype(F32)
        h_wide[at, :] = h
        inv = lax.rsqrt(jnp.mean(h * h, axis=-1, keepdims=True) + NORM_EPS)
        hn[row, :] = (h * inv * g2).astype(BF16)
        return 0

    lax.fori_loop(0, rows // NB, hidden, 0, unroll=2)
    hn_g.start()
    ph("h_waitE")
    for pair in pairs[n_weight:]:
        pair.wait_recv()

    ph("i_logit")
    top[...] = jnp.full_like(top, -jnp.inf)

    def logit(v, _):
        val = dot_nt(hn[mine, :], emb[pl.ds(pl.multiple_of(v * wide, wide), wide), :])
        logits[v] = val
        m = top[...]
        for k in range(tiles):
            m = jnp.maximum(m, val[:, k * 128:(k + 1) * 128])
        top[...] = m
        return 0

    lax.fori_loop(0, n * rows // wide, logit, 0)
    row_counts.wait()
    ph("j_softmax")
    top[...] = jnp.max(top[...], axis=-1, keepdims=True) + jnp.zeros((rows, 128), F32)

    def counts(i, v, k):
        return cnt[pl.ds(i * (RB // 8), RB // 8), v * tiles + k].reshape(RB, 128)

    def total(i, _):
        at = pl.ds(pl.multiple_of(i * RB, RB), RB)
        m = top[at, :]

        def part(v, carry):
            s, c, pick = carry
            for k in range(tiles):
                cut = slice(k * 128, (k + 1) * 128)
                val, num = logits[v, at, cut], counts(i, v, k)
                ex = jnp.exp(val - m)
                logits[v, at, cut] = ex
                s, c, pick = s + ex, c + num, pick + num * val
            return s, c, pick

        zero = jnp.zeros((RB, 128), F32)
        sums[0, at, :], sums[1, at, :], sums[2, at, :] = lax.fori_loop(0, n * rows // wide, part, (zero, zero, zero))
        return 0

    lax.fori_loop(0, rows // RB, total, 0)
    s, c, pick = [jnp.sum(sums[k], axis=-1, keepdims=True) for k in range(3)]
    lse = top[:, 0:1] + jnp.log(s)
    lane = lax.broadcasted_iota(I32, (rows, 128), 1)
    stat_col[...] = jnp.where(lane == 0, lse, jnp.where(lane == 1, c * coef, jnp.where(lane == 2, c * lse - pick, 0.0)))
    sums[0] = c * coef / s + jnp.zeros((rows, 128), F32)

    def grad(i, _):
        at = pl.ds(pl.multiple_of(i * RB, RB), RB)
        scale = sums[0, at, :]

        def part(v, _):
            for k in range(tiles):
                cut = slice(k * 128, (k + 1) * 128)
                here = pl.ds(pl.multiple_of(v * wide + k * 128, 128), 128)
                dlog[at, here] = (logits[v, at, cut] * scale - counts(i, v, k) * coef).astype(BF16)
            return 0

        lax.fori_loop(0, n * rows // wide, part, 0)
        return 0

    lax.fori_loop(0, rows // RB, grad, 0)
    col_counts.start()
    stat[me] = jnp.transpose(stat_col[...])[0:8, :]
    ph("k_dhn")
    acc[...] = dot_nn(dlog[...], emb[...])
    stat_copies = [
        pltpu.make_async_remote_copy(
            src_ref=stat.at[me], dst_ref=stat.at[me], send_sem=st_s.at[k], recv_sem=st_r.at[k], device_id=(peer,), device_id_type=MESH
        )
        for k, peer in enumerate(peers)
    ]
    for copy in stat_copies:
        copy.start()
    ph("l_dhidden")

    def dhidden(i, _):
        at = pl.ds(pl.multiple_of(i * NB, NB), NB)
        h, scaled = h_wide[at, :], acc[at, :] * g2
        inv = lax.rsqrt(jnp.mean(h * h, axis=-1, keepdims=True) + NORM_EPS)
        grad = inv * (scaled - h * (inv * inv) * jnp.mean(scaled * h, axis=-1, keepdims=True))
        de_o[at, :] = grad
        dh[pl.ds(pl.multiple_of(me * rows + i * NB, NB), NB), :] = grad.astype(BF16)
        return 0

    lax.fori_loop(0, rows // NB, dhidden, 0, unroll=2)
    dh_g.start()
    ph("m_hnnear")
    hn_g.forward_pair()

    ph("n_norm")
    for dev in devs:
        norm_rows(flip(dev, 1))
    ph("o_slice")

    def slice_forward(s, _):
        a = a_all[block(s), :]
        dlog[p_at(s)] = dot_nn(a, wg[me]).astype(BF16)
        q_all[s] = dot_nn(a, wu[me]).astype(BF16)
        return 0

    lax.fori_loop(0, n, slice_forward, 0, unroll=2)

    ph("p_back")
    acc[...] = jnp.zeros_like(acc)

    def act_back(dact, p, q):
        sig = jax.nn.sigmoid(p)
        gated = p * sig
        dq = (dact * gated).astype(BF16)
        dp = (dact * q * sig * (1.0 + p * (1.0 - sig))).astype(BF16)
        return dp, dq, (gated * q).astype(BF16)

    def backward(j, _):
        dact = dot_nt(dh[mine, :], wd[j])
        dp, dq, _u = act_back(dact, p_own[j].astype(F32), q_own[j].astype(F32))
        acc[...] += dot_nt(dp, wg[j]) + dot_nt(dq, wu[j])
        return 0

    lax.fori_loop(0, n, backward, 0, unroll=2)
    ph("q_dinput")

    def dinput(i, _):
        at = pl.ds(pl.multiple_of(i * NB, NB), NB)
        x, scaled = emb[pl.ds(pl.multiple_of(me * rows + i * NB, NB), NB), :].astype(F32), acc[at, :] * g1
        inv = lax.rsqrt(jnp.mean(x * x, axis=-1, keepdims=True) + NORM_EPS)
        de_o[at, :] += inv * (scaled - x * (inv * inv) * jnp.mean(scaled * x, axis=-1, keepdims=True))
        return 0

    lax.fori_loop(0, rows // NB, dinput, 0, unroll=2)
    ph("r_stat")
    for copy in stat_copies:
        copy.wait_recv()
    col_counts.wait()

    def head(dev):
        low = dev - lax.rem(dev, 2)
        pair = pl.ds(pl.multiple_of(low * rows, 2 * rows), 2 * rows)
        for k in range(2 * rows // 256):
            source, cut = low + k * 256 // rows, slice(k * 256 % rows, k * 256 % rows + 256)
            lt = dot_nt(emb[mine, :], hn[pl.ds(pl.multiple_of(low * rows + k * 256, 256), 256), :])
            tile = low * (rows // 128) + 2 * k
            num = jnp.concatenate([cnt[:, tile].reshape(rows, 128), cnt[:, tile + 1].reshape(rows, 128)], axis=1)
            prob = jnp.exp(lt - stat[source, 0:1, cut]) * stat[source, 1:2, cut]
            dlog[:, k * 256:(k + 1) * 256] = (prob - num * coef).astype(BF16)
        de_o[...] += dot_nn(dlog[:, 0:2 * rows], hn[pair, :])

    dwg[...] = jnp.zeros_like(dwg)
    dwu[...] = jnp.zeros_like(dwu)
    dwd_o[...] = jnp.zeros_like(dwd_o)

    def act_grads(dev):
        dact = dot_nt(dh[block(dev), :], wd[me])
        return act_back(dact, dlog[p_at(dev)].astype(F32), q_all[dev].astype(F32))

    def weights(dev):
        dp, dq, u = act_grads(dev)
        dwd_o[...] += dot_tn(u, dh[block(dev), :])
        dwg[...] += dot_tn(a_all[block(dev), :], dp)
        dwu[...] += dot_tn(a_all[block(dev), :], dq)

    def exchange(k, peer, src, dst, row):
        return pltpu.make_async_remote_copy(
            src_ref=src.at[pl.ds(pl.multiple_of(peer * out_rows, out_rows), out_rows), :],
            dst_ref=dst.at[me],
            send_sem=ws.at[row, k], recv_sem=wr.at[row, k], device_id=(peer,), device_id_type=MESH,
        )

    swaps_g = [exchange(k, peer, dwg, got_g, 0) for k, peer in enumerate(peers)]
    swaps_u = [exchange(k, peer, dwu, got_u, 1) for k, peer in enumerate(peers)]

    ph("s_w01")
    dh_g.wait_recv(4)
    weights(me)
    weights(pc)
    ph("t_dhnear")
    dh_g.forward_pair()
    dh_g.forward_cross()
    hn_g.forward_cross()
    ph("u_w23")
    weights(px)
    weights(py)
    ph("v_w45")
    dh_g.wait_recv(5, 6)
    weights(flip(px, 1))
    weights(flip(py, 1))
    ph("w_head0")
    hn_g.wait_recv(4)
    head(me)
    ph("x_dhfar")
    dh_g.forward_far()
    ph("y_late")
    late = [pd, flip(pd, 1)]
    for k, kinds in ((0, ()), (1, (7, 8))):
        dh_g.wait_recv(*kinds)
        dev = late[k]
        dlog[p_at(dev)], q_all[dev], dlog[p_at(n + k)] = act_grads(dev)
        dwg[...] += dot_tn(a_all[block(dev), :], dlog[p_at(dev)])
    for swap in swaps_g:
        swap.start()
    for dev in late:
        dwu[...] += dot_tn(a_all[block(dev), :], q_all[dev])
    for swap in swaps_u:
        swap.start()
    ph("z_hnfar")
    hn_g.forward_far()
    ph("za_head")
    for k, dev in enumerate(late):
        dwd_o[...] += dot_tn(dlog[p_at(n + k)], dh[block(dev), :])
    hn_g.wait_recv(5, 6)
    head(px)
    head(py)
    hn_g.wait_recv(7, 8)
    head(pd)
    ph("zc_tail")
    keep = pl.ds(pl.multiple_of(me * out_rows, out_rows), out_rows)
    got_g[me] = dwg[keep, :]
    got_u[me] = dwu[keep, :]
    total_loss = jnp.zeros((1, rows), F32)
    for s in range(n):
        total_loss = total_loss + stat[s, 2:3, :]
    loss_o[...] = jnp.sum(total_loss, axis=-1, keepdims=True) * coef + jnp.zeros((1, 128), F32)
    ph("zd_waits")
    for copy in stat_copies:
        copy.wait_send()
    hn_g.wait_sends()
    dh_g.wait_sends()
    for pair in pairs:
        pair.wait_send()
    for swap in swaps_g + swaps_u:
        swap.wait()
    ph()


def run_step(coef, embs, gus, downs, crow, ccol, g1, g2):
    n = N_DEV
    rows, width = embs[0].shape
    fs = gus[0].shape[2]
    out_rows = width // n
    any_spec = pl.BlockSpec(memory_space=pl.ANY)
    vmem = pl.BlockSpec(memory_space=pltpu.VMEM)
    dma = pltpu.SemaphoreType.DMA
    return pl.pallas_call(
        step_kernel,
        out_shape=(
            jax.ShapeDtypeStruct((1, 128), F32),
            jax.ShapeDtypeStruct((rows, width), F32),
            jax.ShapeDtypeStruct((n, out_rows, fs), F32),
            jax.ShapeDtypeStruct((n, out_rows, fs), F32),
            jax.ShapeDtypeStruct((fs, width), F32),
        ),
        in_specs=[pl.BlockSpec(memory_space=pltpu.SMEM)] + [any_spec] * 14 + [vmem] * 2,
        out_specs=(vmem,) * 5,
        scratch_shapes=[
            pltpu.VMEM((n * rows, width), BF16),
            pltpu.VMEM((n, width, fs), BF16),
            pltpu.VMEM((n, width, fs), BF16),
            pltpu.VMEM((n, fs, width), BF16),
            pltpu.VMEM((rows // 8, n * rows // 128, 8, 128), F32),
            pltpu.VMEM((n * rows, width), BF16),
            pltpu.VMEM((n * rows, width), BF16),
            pltpu.VMEM((n * rows, width), BF16),
            pltpu.VMEM((n, rows, fs), BF16),
            pltpu.VMEM((n, rows, fs), BF16),
            pltpu.VMEM((n, rows, fs), BF16),
            pltpu.VMEM((n // 2, rows, 2 * rows), F32),
            pltpu.VMEM((rows, n * rows), BF16),
            pltpu.VMEM((rows, width), F32),
            pltpu.VMEM((rows, width), F32),
            pltpu.VMEM((n, 8, rows), F32),
            pltpu.VMEM((rows, 128), F32),
            pltpu.VMEM((rows, 128), F32),
            pltpu.VMEM((3, rows, 128), F32),
            pltpu.VMEM((width, fs), F32),
            pltpu.VMEM((width, fs), F32),
            dma((18,)), dma((16,)), dma((16,)), dma((9,)), dma((9,)), dma((9,)), dma((9,)), dma((n - 1,)), dma((n - 1,)), dma((2, n - 1)), dma((2, n - 1)),
        ],
        compiler_params=pltpu.CompilerParams(collective_id=1, has_side_effects=True, vmem_limit_bytes=VMEM_MAX),
        name="step",
    )(coef, *embs, *gus, *downs, crow, ccol, g1, g2)


def solution(mesh):
    def device_step(tok_ids, tok_labels, loss_mask, emb, g1, g2, w_gate, w_up, w_down):
        n = N_DEV
        rows, width = emb.shape
        vocab = rows * n
        n_tok = tok_ids.shape[0]
        me = lax.axis_index("fsdp")

        def send(bit):
            pairs = [(d, d ^ bit) for d in range(n)]
            return lambda val: lax.ppermute(val, "fsdp", pairs)

        along_x, along_y = send(2), send(4)
        gu = slice_weights(w_gate, w_up)
        gus, downs, embs = [[val, along_x(val), along_y(val)] for val in (gu, w_down, emb)]

        live = loss_mask != 0
        by_id = lax.sort(jnp.where(live, tok_ids * 65536 + tok_labels, vocab * 65536))
        by_label = lax.sort(jnp.where(live, tok_labels * 65536 + tok_ids, vocab * 65536))
        tok = [part.reshape(n_tok // 128, 128) for part in (by_id >> 16, by_id & 65535, by_label >> 16, by_label & 65535)]
        tok = gather_tokens(jnp.concatenate(tok).astype(jnp.int16))
        tok, gus[2], downs[2], embs[1] = lax.optimization_barrier((tok, gus[2], downs[2], embs[1]))
        gus.append(along_x(gus[2]))
        downs.append(along_x(downs[2]))
        embs.append(along_y(embs[1]))
        ids, labels, labels2, ids2 = [tok[:, k * (n_tok // 128):(k + 1) * (n_tok // 128)].astype(I32) for k in range(4)]
        crow, ccol = count([(ids, labels), (labels2, ids2)], me * rows, rows, vocab)
        n_live = jnp.sum(ids < vocab).astype(F32)
        coef = (1.0 / n_live).reshape(1, 1)
        loss, *grads = run_step(coef, embs, gus, downs, crow, ccol, g1.reshape(1, width), g2.reshape(1, width))
        return (loss[0, 0], *finish(*grads))

    row_spec = P("fsdp", None)
    tok_spec = P("fsdp")
    return jax.shard_map(device_step, mesh=mesh, in_specs=(tok_spec, tok_spec, tok_spec, row_spec, P(), P(), row_spec, row_spec, row_spec), out_specs=(P(), row_spec, row_spec, row_spec, row_spec), check_vma=False)
```

```python
import functools

import jax
import jax.numpy as jnp
from jax import lax
from jax.experimental import pallas as pl
from jax.experimental.pallas import tpu as pltpu
from jax.sharding import PartitionSpec as P


NORM_EPS = 1e-6
N_DEV = 8
F32, BF16, I32 = jnp.float32, jnp.bfloat16, jnp.int32
MESH = pl.DeviceIdType.MESH
VMEM_MAX = 66_000_000


class Phases:
    def __init__(self):
        self.now = None

    def __call__(self, name=None):
        if self.now is not None:
            self.now.__exit__(None, None, None)
        self.now = jax.named_scope(name) if name else None
        if self.now is not None:
            self.now.__enter__()


def dot_nn(a, b):
    return jnp.dot(a, b, preferred_element_type=F32)


def dot_nt(a, b):
    return lax.dot_general(a, b, (((1,), (1,)), ((), ())), preferred_element_type=F32)


def dot_tn(a, b):
    return lax.dot_general(a, b, (((0,), (0,)), ((), ())), preferred_element_type=F32)


def flip(me, bit):
    return me + bit - 2 * bit * lax.rem(me // bit, 2)


def barrier_with(peers):
    sem = pltpu.get_barrier_semaphore()
    for peer in peers:
        pl.semaphore_signal(sem, inc=1, device_id=(peer,), device_id_type=MESH)
    pl.semaphore_wait(sem, len(peers))


class Gather:
    def __init__(self, slot, half, send_sem, recv_sem, me, own=None):
        self.slot, self.half, self.ss, self.rs, self.me = slot, half, send_sem, recv_sem, me
        self.own = slot(me) if own is None else own
        self.pc, self.px, self.py = flip(me, 1), flip(me, 2), flip(me, 4)
        self.pd = flip(self.px, 4)

    def copy(self, kind, src, dst, peer):
        return pltpu.make_async_remote_copy(
            src_ref=src, dst_ref=dst, send_sem=self.ss(kind), recv_sem=self.rs(kind), device_id=(peer,), device_id_type=MESH
        )

    def describe(self, kind):
        me, px, py, pd, pc = self.me, self.px, self.py, self.pd, self.pc
        if kind == 0:
            return self.copy(0, self.own, self.slot(me), px)
        if kind == 1:
            return self.copy(1, self.own, self.slot(me), py)
        if kind == 2:
            return self.copy(2, self.half(px, 0), self.half(px, 0), py)
        if kind == 3:
            return self.copy(3, self.half(py, 1), self.half(py, 1), px)
        if kind == 4:
            return self.copy(4, self.own, self.slot(me), pc)
        if kind == 5:
            return self.copy(5, self.slot(px), self.slot(px), pc)
        if kind == 6:
            return self.copy(6, self.slot(py), self.slot(py), pc)
        return self.copy(kind, self.half(pd, kind - 7), self.half(pd, kind - 7), pc)

    def start(self):
        for kind in (0, 1, 4):
            self.describe(kind).start()

    def forward_pair(self):
        for kind in (0, 1):
            self.describe(kind).wait_recv()
            self.describe(5 + kind).start()

    def forward_cross(self):
        self.describe(2).start()
        self.describe(3).start()

    def forward_far(self):
        self.describe(2).wait_recv()
        self.describe(7).start()
        self.describe(3).wait_recv()
        self.describe(8).start()

    def wait_recv(self, *kinds):
        for kind in kinds:
            self.describe(kind).wait_recv()

    def wait_sends(self, *kinds):
        for kind in kinds or range(9):
            self.describe(kind).wait_send()


def slice_kernel(gate, up, out):
    n, _, fs = out.shape
    rows = gate.shape[0]
    for k in range(n):
        out[k, 0:rows, :] = gate[:, k * fs:(k + 1) * fs]
        out[k, rows:2 * rows, :] = up[:, k * fs:(k + 1) * fs]


def slice_weights(gate, up):
    rows, width = gate.shape
    return pl.pallas_call(
        slice_kernel,
        out_shape=jax.ShapeDtypeStruct((N_DEV, 2 * rows, width // N_DEV), gate.dtype),
        cost_estimate=pl.CostEstimate(flops=1_000_000, bytes_accessed=1_000_000, transcendentals=0),
        name="slices",
    )(gate, up)


def token_kernel(tok, tok_o, send_sem, recv_sem, local_sem):
    me = lax.axis_index("fsdp")
    n = tok_o.shape[0]
    peers = [lax.rem(me + k, n) for k in range(1, n)]
    barrier_with(peers)
    copies = [
        pltpu.make_async_remote_copy(
            src_ref=tok, dst_ref=tok_o.at[me], send_sem=send_sem.at[k], recv_sem=recv_sem.at[k], device_id=(peer,), device_id_type=MESH
        )
        for k, peer in enumerate(peers)
    ]
    local = pltpu.make_async_copy(tok, tok_o.at[me], local_sem)
    for copy in copies:
        copy.start()
    local.start()
    for copy in copies:
        copy.wait()
    local.wait()


def gather_tokens(tok):
    dma = pltpu.SemaphoreType.DMA
    return pl.pallas_call(
        token_kernel,
        out_shape=jax.ShapeDtypeStruct((N_DEV,) + tok.shape, tok.dtype),
        in_specs=[pl.BlockSpec(memory_space=pltpu.VMEM)],
        out_specs=pl.BlockSpec(memory_space=pl.ANY),
        scratch_shapes=[dma((N_DEV - 1,)), dma((N_DEV - 1,)), dma],
        compiler_params=pltpu.CompilerParams(collective_id=0, has_side_effects=True),
        cost_estimate=pl.CostEstimate(flops=5_000_000_000, bytes_accessed=1_000_000, transcendentals=0),
        name="tokens",
    )(tok)


def count_kernel(bounds, keys_a, keys_b, out_a, out_b, list_a, list_b, acc_a, acc_b, in_sem, out_sem):
    n_src = N_DEV
    per = list_a.shape[0] // n_src
    size = acc_a.shape[0]
    BLK = 256
    unroll = 8
    jobs = [(keys_a, out_a, list_a, acc_a), (keys_b, out_b, list_b, acc_b)]
    loads = [pltpu.make_async_copy(keys, held, in_sem.at[k]) for k, (keys, _o, held, _a) in enumerate(jobs)]
    stores = [pltpu.make_async_copy(acc, out, out_sem.at[k]) for k, (_k, out, _h, acc) in enumerate(jobs)]
    for load in loads:
        load.start()
    lanes = lax.broadcasted_iota(I32, (1, 128), 1)

    def clear(i, _):
        acc_a[pl.ds(i * BLK, BLK), :] = jnp.zeros((BLK, 128), F32)
        acc_b[pl.ds(i * BLK, BLK), :] = jnp.zeros((BLK, 128), F32)
        return 0

    lax.fori_loop(0, size // BLK, clear, 0)
    for load in loads:
        load.wait()

    def group(streams, whole):
        done = []
        for held, acc, pos, end in streams:
            places, vals, delta = [], [], None
            for k in range(unroll):
                key = held[pos + k] if whole else held[jnp.minimum(pos + k, end - 1)]
                places.append(key >> 7)
                spread = jnp.full((1, 128), key, I32)
                here = jnp.where(lanes == (spread & 127), 1.0 if whole else jnp.where(pos + k < end, 1.0, 0.0), 0.0)
                delta = here if k == 0 else here + jnp.where((spread ^ before) < 128, delta, 0.0)
                before = spread
                vals.append(acc[pl.ds(places[k], 1), :] + delta)
            done.append((acc, places, vals))
        for acc, places, vals in done:
            for place, val in zip(places, vals):
                acc[pl.ds(place, 1), :] = val

    def source(src, _):
        ranges = []
        for which, (_k, _o, held, acc) in enumerate(jobs):
            begin = bounds[which * 2 * n_src + src] + src * per
            end = bounds[which * 2 * n_src + n_src + src] + src * per
            ranges.append((held, acc, begin, end, lax.shift_right_logical(end - begin, 3)))
        both = jnp.minimum(ranges[0][4], ranges[1][4])

        def step(i, _):
            group([(held, acc, begin + i * unroll, end) for held, acc, begin, end, _n in ranges], True)
            return 0

        lax.fori_loop(0, both, step, 0)
        for held, acc, begin, end, n_whole in ranges:
            def rest(i, _):
                group([(held, acc, begin + i * unroll, end)], True)
                return 0

            lax.fori_loop(both, n_whole, rest, 0)

            @pl.when(begin + n_whole * unroll < end)
            def _():
                group([(held, acc, begin + n_whole * unroll, end)], False)

        return 0

    lax.fori_loop(0, n_src, source, 0)
    for store in stores:
        store.start()
    for store in stores:
        store.wait()


def count(pairs, first, rows, cols):
    bounds, keys, tiles = [], [], cols // 128
    for major, minor in pairs:
        bounds.append(jnp.sum(major < first, axis=(1, 2), dtype=I32))
        bounds.append(jnp.sum(major < first + rows, axis=(1, 2), dtype=I32))
        row = major - first
        keys.append(((((row >> 3) * tiles + (minor >> 7)) * 8 + (row & 7)) * 128 + (minor & 127)).reshape(-1))
    any_spec = pl.BlockSpec(memory_space=pl.ANY)
    tall = (rows * cols // 128, 128)
    outs = pl.pallas_call(
        count_kernel,
        out_shape=(jax.ShapeDtypeStruct(tall, F32),) * 2,
        in_specs=[pl.BlockSpec(memory_space=pltpu.SMEM), any_spec, any_spec],
        out_specs=(any_spec,) * 2,
        scratch_shapes=[pltpu.SMEM(keys[0].shape, I32)] * 2 + [pltpu.VMEM(tall, F32)] * 2 + [pltpu.SemaphoreType.DMA((2,))] * 2,
        cost_estimate=pl.CostEstimate(flops=30_000_000_000, bytes_accessed=16_000_000, transcendentals=0),
        name="count",
    )(jnp.concatenate(bounds), *keys)
    return [out.reshape(rows // 8, tiles, 8, 128) for out in outs]


def finish_kernel(de, got_g, got_u, dwd, de_o, dwg_o, dwu_o, dwd_o):
    n, _, fs = got_g.shape
    de_o[...] = de[...]
    dwd_o[...] = dwd[...]
    for k in range(n):
        dwg_o[:, k * fs:(k + 1) * fs] = got_g[k]
        dwu_o[:, k * fs:(k + 1) * fs] = got_u[k]


def finish(de, got_g, got_u, dwd):
    n, out_rows, fs = got_g.shape
    wide = jax.ShapeDtypeStruct((out_rows, n * fs), F32)
    return pl.pallas_call(finish_kernel, out_shape=(jax.ShapeDtypeStruct(de.shape, F32), wide, wide, jax.ShapeDtypeStruct(dwd.shape, F32)), name="finish")(
        de, got_g, got_u, dwd
    )


def step_kernel(
    coef_ref, emb_me, emb_x, emb_y, gu_me, gu_x, gu_y, gu_d, wd_me, wd_x, wd_y, wd_d, crow_hbm, ccol_hbm, g1_ref, g2_ref,
    loss_o, de_o, got_g, got_u, dwd_o,
    emb, wg, wu, wd, cnt, hn, dh, a_all, p_own, q_own, q_all, logits, dlog, h_wide, acc, stat, stat_col, top, sums,
    dwg, dwu, load_sem, pair_s, pair_r, es, er, hs, hr, ds_, dr, st_s, st_r, ws, wr,
):
    me = lax.axis_index("fsdp")
    n = wg.shape[0]
    rows, width = h_wide.shape
    fs = wg.shape[2]
    out_rows = got_g.shape[1]
    coef = coef_ref[0, 0]
    ph = Phases()
    ph("a_start")
    NB = 128
    RB = 64
    wide = logits.shape[2]
    tiles = wide // 128
    peers = [lax.rem(me + k, n) for k in range(1, n)]

    def block(dev):
        return pl.ds(pl.multiple_of(dev * rows, rows), rows)

    def p_at(s):
        return (slice(None), pl.ds(pl.multiple_of(2 * rows + s * 256, 256), fs))

    mine = block(me)
    pc, px, py = flip(me, 1), flip(me, 2), flip(me, 4)
    pd = flip(px, 4)
    devs = [me, px, py, pd]
    parts = []
    for dev, gu, down in zip(devs, [gu_me, gu_x, gu_y, gu_d], [wd_me, wd_x, wd_y, wd_d]):
        at = pl.ds(dev * out_rows, out_rows)
        parts.append((gu.at[:, 0:out_rows, :], wg.at[:, at, :]))
        parts.append((gu.at[:, out_rows:2 * out_rows, :], wu.at[:, at, :]))
        parts.append((down, wd.at[dev]))
    n_weight = len(parts)
    for dev, part in zip(devs, [emb_me, emb_x, emb_y]):
        parts.append((part, emb.at[block(dev), :]))
    loads = [pltpu.make_async_copy(src, dst, load_sem.at[k]) for k, (src, dst) in enumerate(parts)]
    pairs = [
        pltpu.make_async_remote_copy(
            src_ref=src, dst_ref=dst, send_sem=pair_s.at[k], recv_sem=pair_r.at[k], device_id=(pc,), device_id_type=MESH
        )
        for k, (src, dst) in enumerate(parts)
    ]
    row_counts = pltpu.make_async_copy(crow_hbm, cnt, load_sem.at[len(parts)])
    col_counts = pltpu.make_async_copy(ccol_hbm, cnt, load_sem.at[len(parts) + 1])

    for load in loads[n_weight:] + loads[:n_weight]:
        load.start()
    ph("b_barrier")
    barrier_with(peers)
    for pair in pairs:
        pair.start()
    row_counts.start()

    def gather_of(buf, ss, rs):
        half = rows // 2
        return Gather(
            lambda d: buf.at[block(d), :],
            lambda d, i: buf.at[pl.ds(pl.multiple_of(d * rows + i * half, half), half), :],
            lambda c: ss.at[c], lambda c: rs.at[c], me,
        )

    emb_g, hn_g, dh_g = gather_of(emb, es, er), gather_of(hn, hs, hr), gather_of(dh, ds_, dr)
    g1, g2 = g1_ref[...], g2_ref[...]

    ph("d_norm")

    def norm_rows(dev):
        def norm(i, _):
            at = pl.ds(pl.multiple_of(dev * rows + i * NB, NB), NB)
            x = emb[at, :].astype(F32)
            inv = lax.rsqrt(jnp.mean(x * x, axis=-1, keepdims=True) + NORM_EPS)
            a_all[at, :] = (x * inv * g1).astype(BF16)
            return 0

        lax.fori_loop(0, rows // NB, norm, 0, unroll=2)

    for load in loads[n_weight:]:
        load.wait()
    emb_g.forward_cross()
    for dev in devs[:3]:
        norm_rows(dev)

    ph("e_waitW")
    for load, pair in zip(loads[:n_weight], pairs[:n_weight]):
        load.wait()
        pair.wait_recv()
    ph("f_fwd")
    acc[...] = jnp.zeros_like(acc)

    def forward(j, _):
        a = a_all[mine, :]
        p = dot_nn(a, wg[j]).astype(BF16)
        q = dot_nn(a, wu[j]).astype(BF16)
        p_own[j], q_own[j] = p, q
        p, q = p.astype(F32), q.astype(F32)
        u = (p * jax.nn.sigmoid(p) * q).astype(BF16)
        acc[...] += dot_nn(u, wd[j])
        return 0

    lax.fori_loop(0, n // 2, forward, 0, unroll=2)
    emb_g.forward_far()
    lax.fori_loop(n // 2, n, forward, 0, unroll=2)
    ph("g_hidden")

    def hidden(i, _):
        at = pl.ds(pl.multiple_of(i * NB, NB), NB)
        row = pl.ds(pl.multiple_of(me * rows + i * NB, NB), NB)
        h = (emb[row, :].astype(F32) + acc[at, :]).astype(BF16).astype(F32)
        h_wide[at, :] = h
        inv = lax.rsqrt(jnp.mean(h * h, axis=-1, keepdims=True) + NORM_EPS)
        hn[row, :] = (h * inv * g2).astype(BF16)
        return 0

    lax.fori_loop(0, rows // NB, hidden, 0, unroll=2)
    hn_g.start()
    ph("h_waitE")
    for pair in pairs[n_weight:]:
        pair.wait_recv()
    emb_g.wait_recv(7, 8)

    ph("i_logit")
    top[...] = jnp.full_like(top, -jnp.inf)

    def logit(v, _):
        val = dot_nt(hn[mine, :], emb[pl.ds(pl.multiple_of(v * wide, wide), wide), :])
        logits[v] = val
        m = top[...]
        for k in range(tiles):
            m = jnp.maximum(m, val[:, k * 128:(k + 1) * 128])
        top[...] = m
        return 0

    lax.fori_loop(0, n * rows // wide, logit, 0)
    row_counts.wait()
    ph("j_softmax")
    top[...] = jnp.max(top[...], axis=-1, keepdims=True) + jnp.zeros((rows, 128), F32)

    def counts(i, v, k):
        return cnt[pl.ds(i * (RB // 8), RB // 8), v * tiles + k].reshape(RB, 128)

    def total(i, _):
        at = pl.ds(pl.multiple_of(i * RB, RB), RB)
        m = top[at, :]

        def part(v, carry):
            s, c, pick = carry
            for k in range(tiles):
                cut = slice(k * 128, (k + 1) * 128)
                val, num = logits[v, at, cut], counts(i, v, k)
                ex = jnp.exp(val - m)
                logits[v, at, cut] = ex
                s, c, pick = s + ex, c + num, pick + num * val
            return s, c, pick

        zero = jnp.zeros((RB, 128), F32)
        sums[0, at, :], sums[1, at, :], sums[2, at, :] = lax.fori_loop(0, n * rows // wide, part, (zero, zero, zero))
        return 0

    lax.fori_loop(0, rows // RB, total, 0)
    s, c, pick = [jnp.sum(sums[k], axis=-1, keepdims=True) for k in range(3)]
    lse = top[:, 0:1] + jnp.log(s)
    lane = lax.broadcasted_iota(I32, (rows, 128), 1)
    stat_col[...] = jnp.where(lane == 0, lse, jnp.where(lane == 1, c * coef, jnp.where(lane == 2, c * lse - pick, 0.0)))
    sums[0] = c * coef / s + jnp.zeros((rows, 128), F32)

    def grad(i, _):
        at = pl.ds(pl.multiple_of(i * RB, RB), RB)
        scale = sums[0, at, :]

        def part(v, _):
            for k in range(tiles):
                cut = slice(k * 128, (k + 1) * 128)
                here = pl.ds(pl.multiple_of(v * wide + k * 128, 128), 128)
                dlog[at, here] = (logits[v, at, cut] * scale - counts(i, v, k) * coef).astype(BF16)
            return 0

        lax.fori_loop(0, n * rows // wide, part, 0)
        return 0

    lax.fori_loop(0, rows // RB, grad, 0)
    col_counts.start()
    stat[me] = jnp.transpose(stat_col[...])[0:8, :]
    ph("k_dhn")
    acc[...] = dot_nn(dlog[...], emb[...])
    stat_copies = [
        pltpu.make_async_remote_copy(
            src_ref=stat.at[me], dst_ref=stat.at[me], send_sem=st_s.at[k], recv_sem=st_r.at[k], device_id=(peer,), device_id_type=MESH
        )
        for k, peer in enumerate(peers)
    ]
    for copy in stat_copies:
        copy.start()
    ph("l_dhidden")

    def dhidden(i, _):
        at = pl.ds(pl.multiple_of(i * NB, NB), NB)
        h, scaled = h_wide[at, :], acc[at, :] * g2
        inv = lax.rsqrt(jnp.mean(h * h, axis=-1, keepdims=True) + NORM_EPS)
        grad = inv * (scaled - h * (inv * inv) * jnp.mean(scaled * h, axis=-1, keepdims=True))
        de_o[at, :] = grad
        dh[pl.ds(pl.multiple_of(me * rows + i * NB, NB), NB), :] = grad.astype(BF16)
        return 0

    lax.fori_loop(0, rows // NB, dhidden, 0, unroll=2)
    dh_g.start()
    ph("m_hnnear")
    hn_g.forward_pair()

    ph("n_norm")
    for dev in [pd] + [flip(dev, 1) for dev in devs]:
        norm_rows(dev)
    ph("o_slice")

    def slice_forward(s, _):
        a = a_all[block(s), :]
        dlog[p_at(s)] = dot_nn(a, wg[me]).astype(BF16)
        q_all[s] = dot_nn(a, wu[me]).astype(BF16)
        return 0

    lax.fori_loop(0, n, slice_forward, 0, unroll=2)

    ph("p_back")
    acc[...] = jnp.zeros_like(acc)

    def act_back(dact, p, q):
        sig = jax.nn.sigmoid(p)
        gated = p * sig
        dq = (dact * gated).astype(BF16)
        dp = (dact * q * sig * (1.0 + p * (1.0 - sig))).astype(BF16)
        return dp, dq, (gated * q).astype(BF16)

    def backward(j, _):
        dact = dot_nt(dh[mine, :], wd[j])
        dp, dq, _u = act_back(dact, p_own[j].astype(F32), q_own[j].astype(F32))
        acc[...] += dot_nt(dp, wg[j]) + dot_nt(dq, wu[j])
        return 0

    lax.fori_loop(0, n, backward, 0, unroll=2)
    ph("q_dinput")

    def dinput(i, _):
        at = pl.ds(pl.multiple_of(i * NB, NB), NB)
        x, scaled = emb[pl.ds(pl.multiple_of(me * rows + i * NB, NB), NB), :].astype(F32), acc[at, :] * g1
        inv = lax.rsqrt(jnp.mean(x * x, axis=-1, keepdims=True) + NORM_EPS)
        de_o[at, :] += inv * (scaled - x * (inv * inv) * jnp.mean(scaled * x, axis=-1, keepdims=True))
        return 0

    lax.fori_loop(0, rows // NB, dinput, 0, unroll=2)
    ph("r_stat")
    for copy in stat_copies:
        copy.wait_recv()
    col_counts.wait()

    def head(dev):
        low = dev - lax.rem(dev, 2)
        pair = pl.ds(pl.multiple_of(low * rows, 2 * rows), 2 * rows)
        for k in range(2 * rows // 256):
            source, cut = low + k * 256 // rows, slice(k * 256 % rows, k * 256 % rows + 256)
            lt = dot_nt(emb[mine, :], hn[pl.ds(pl.multiple_of(low * rows + k * 256, 256), 256), :])
            tile = low * (rows // 128) + 2 * k
            num = jnp.concatenate([cnt[:, tile].reshape(rows, 128), cnt[:, tile + 1].reshape(rows, 128)], axis=1)
            prob = jnp.exp(lt - stat[source, 0:1, cut]) * stat[source, 1:2, cut]
            dlog[:, k * 256:(k + 1) * 256] = (prob - num * coef).astype(BF16)
        de_o[...] += dot_nn(dlog[:, 0:2 * rows], hn[pair, :])

    dwg[...] = jnp.zeros_like(dwg)
    dwu[...] = jnp.zeros_like(dwu)
    dwd_o[...] = jnp.zeros_like(dwd_o)

    def act_grads(dev):
        dact = dot_nt(dh[block(dev), :], wd[me])
        return act_back(dact, dlog[p_at(dev)].astype(F32), q_all[dev].astype(F32))

    def weights(dev):
        dp, dq, u = act_grads(dev)
        dwd_o[...] += dot_tn(u, dh[block(dev), :])
        dwg[...] += dot_tn(a_all[block(dev), :], dp)
        dwu[...] += dot_tn(a_all[block(dev), :], dq)

    def exchange(k, peer, src, dst, row):
        return pltpu.make_async_remote_copy(
            src_ref=src.at[pl.ds(pl.multiple_of(peer * out_rows, out_rows), out_rows), :],
            dst_ref=dst.at[me],
            send_sem=ws.at[row, k], recv_sem=wr.at[row, k], device_id=(peer,), device_id_type=MESH,
        )

    swaps_g = [exchange(k, peer, dwg, got_g, 0) for k, peer in enumerate(peers)]
    swaps_u = [exchange(k, peer, dwu, got_u, 1) for k, peer in enumerate(peers)]

    ph("s_w01")
    dh_g.wait_recv(4)
    weights(me)
    weights(pc)
    ph("t_dhnear")
    dh_g.forward_pair()
    dh_g.forward_cross()
    hn_g.forward_cross()
    ph("u_w23")
    weights(px)
    weights(py)
    ph("v_w45")
    dh_g.wait_recv(5, 6)
    weights(flip(px, 1))
    weights(flip(py, 1))
    ph("w_head0")
    hn_g.wait_recv(4)
    head(me)
    ph("x_dhfar")
    dh_g.forward_far()
    ph("y_late")
    late = [pd, flip(pd, 1)]
    for k, kinds in ((0, ()), (1, (7, 8))):
        dh_g.wait_recv(*kinds)
        dev = late[k]
        dlog[p_at(dev)], q_all[dev], dlog[p_at(n + k)] = act_grads(dev)
        dwg[...] += dot_tn(a_all[block(dev), :], dlog[p_at(dev)])
    for swap in swaps_g:
        swap.start()
    for dev in late:
        dwu[...] += dot_tn(a_all[block(dev), :], q_all[dev])
    for swap in swaps_u:
        swap.start()
    ph("z_hnfar")
    hn_g.forward_far()
    ph("za_head")
    for k, dev in enumerate(late):
        dwd_o[...] += dot_tn(dlog[p_at(n + k)], dh[block(dev), :])
    hn_g.wait_recv(5, 6)
    head(px)
    head(py)
    hn_g.wait_recv(7, 8)
    head(pd)
    ph("zc_tail")
    keep = pl.ds(pl.multiple_of(me * out_rows, out_rows), out_rows)
    got_g[me] = dwg[keep, :]
    got_u[me] = dwu[keep, :]
    total_loss = jnp.zeros((1, rows), F32)
    for s in range(n):
        total_loss = total_loss + stat[s, 2:3, :]
    loss_o[...] = jnp.sum(total_loss, axis=-1, keepdims=True) * coef + jnp.zeros((1, 128), F32)
    ph("zd_waits")
    for copy in stat_copies:
        copy.wait_send()
    emb_g.wait_sends(2, 3, 7, 8)
    hn_g.wait_sends()
    dh_g.wait_sends()
    for pair in pairs:
        pair.wait_send()
    for swap in swaps_g + swaps_u:
        swap.wait()
    ph()


def run_step(coef, embs, gus, downs, crow, ccol, g1, g2):
    n = N_DEV
    rows, width = embs[0].shape
    fs = gus[0].shape[2]
    out_rows = width // n
    any_spec = pl.BlockSpec(memory_space=pl.ANY)
    vmem = pl.BlockSpec(memory_space=pltpu.VMEM)
    dma = pltpu.SemaphoreType.DMA
    return pl.pallas_call(
        step_kernel,
        out_shape=(
            jax.ShapeDtypeStruct((1, 128), F32),
            jax.ShapeDtypeStruct((rows, width), F32),
            jax.ShapeDtypeStruct((n, out_rows, fs), F32),
            jax.ShapeDtypeStruct((n, out_rows, fs), F32),
            jax.ShapeDtypeStruct((fs, width), F32),
        ),
        in_specs=[pl.BlockSpec(memory_space=pltpu.SMEM)] + [any_spec] * 13 + [vmem] * 2,
        out_specs=(vmem,) * 5,
        scratch_shapes=[
            pltpu.VMEM((n * rows, width), BF16),
            pltpu.VMEM((n, width, fs), BF16),
            pltpu.VMEM((n, width, fs), BF16),
            pltpu.VMEM((n, fs, width), BF16),
            pltpu.VMEM((rows // 8, n * rows // 128, 8, 128), F32),
            pltpu.VMEM((n * rows, width), BF16),
            pltpu.VMEM((n * rows, width), BF16),
            pltpu.VMEM((n * rows, width), BF16),
            pltpu.VMEM((n, rows, fs), BF16),
            pltpu.VMEM((n, rows, fs), BF16),
            pltpu.VMEM((n, rows, fs), BF16),
            pltpu.VMEM((n // 2, rows, 2 * rows), F32),
            pltpu.VMEM((rows, n * rows), BF16),
            pltpu.VMEM((rows, width), F32),
            pltpu.VMEM((rows, width), F32),
            pltpu.VMEM((n, 8, rows), F32),
            pltpu.VMEM((rows, 128), F32),
            pltpu.VMEM((rows, 128), F32),
            pltpu.VMEM((3, rows, 128), F32),
            pltpu.VMEM((width, fs), F32),
            pltpu.VMEM((width, fs), F32),
            dma((17,)), dma((15,)), dma((15,)), dma((9,)), dma((9,)), dma((9,)), dma((9,)), dma((9,)), dma((9,)), dma((n - 1,)), dma((n - 1,)), dma((2, n - 1)), dma((2, n - 1)),
        ],
        compiler_params=pltpu.CompilerParams(collective_id=1, has_side_effects=True, vmem_limit_bytes=VMEM_MAX),
        name="step",
    )(coef, *embs, *gus, *downs, crow, ccol, g1, g2)


def solution(mesh):
    def device_step(tok_ids, tok_labels, loss_mask, emb, g1, g2, w_gate, w_up, w_down):
        n = N_DEV
        rows, width = emb.shape
        vocab = rows * n
        n_tok = tok_ids.shape[0]
        me = lax.axis_index("fsdp")

        def send(bit):
            pairs = [(d, d ^ bit) for d in range(n)]
            return lambda val: lax.ppermute(val, "fsdp", pairs)

        along_x, along_y = send(2), send(4)
        gu = slice_weights(w_gate, w_up)
        gus, downs = [[val, along_x(val), along_y(val)] for val in (gu, w_down)]

        live = loss_mask != 0
        by_id = lax.sort(jnp.where(live, tok_ids * 65536 + tok_labels, vocab * 65536))
        by_label = lax.sort(jnp.where(live, tok_labels * 65536 + tok_ids, vocab * 65536))
        tok = [part.reshape(n_tok // 128, 128) for part in (by_id >> 16, by_id & 65535, by_label >> 16, by_label & 65535)]
        tok = gather_tokens(jnp.concatenate(tok).astype(jnp.int16))
        tok, gus[2], downs[1], emb_later = lax.optimization_barrier((tok, gus[2], downs[1], emb))
        embs = [emb, along_x(emb_later), along_y(emb_later)]
        gus.append(along_x(gus[2]))
        downs.append(along_y(downs[1]))
        ids, labels, labels2, ids2 = [tok[:, k * (n_tok // 128):(k + 1) * (n_tok // 128)].astype(I32) for k in range(4)]
        crow, ccol = count([(ids, labels), (labels2, ids2)], me * rows, rows, vocab)
        n_live = jnp.sum(ids < vocab).astype(F32)
        coef = (1.0 / n_live).reshape(1, 1)
        loss, *grads = run_step(coef, embs, gus, downs, crow, ccol, g1.reshape(1, width), g2.reshape(1, width))
        return (loss[0, 0], *finish(*grads))

    row_spec = P("fsdp", None)
    tok_spec = P("fsdp")
    return jax.shard_map(device_step, mesh=mesh, in_specs=(tok_spec, tok_spec, tok_spec, row_spec, P(), P(), row_spec, row_spec, row_spec), out_specs=(P(), row_spec, row_spec, row_spec, row_spec), check_vma=False)
```

```python
import functools

import jax
import jax.numpy as jnp
from jax import lax
from jax.experimental import pallas as pl
from jax.experimental.pallas import tpu as pltpu
from jax.sharding import PartitionSpec as P


NORM_EPS = 1e-6
N_DEV = 8
F32, BF16, I32 = jnp.float32, jnp.bfloat16, jnp.int32
MESH = pl.DeviceIdType.MESH
VMEM_MAX = 66_000_000


class Phases:
    def __init__(self):
        self.now = None

    def __call__(self, name=None):
        if self.now is not None:
            self.now.__exit__(None, None, None)
        self.now = jax.named_scope(name) if name else None
        if self.now is not None:
            self.now.__enter__()


def dot_nn(a, b):
    return jnp.dot(a, b, preferred_element_type=F32)


def dot_nt(a, b):
    return lax.dot_general(a, b, (((1,), (1,)), ((), ())), preferred_element_type=F32)


def dot_tn(a, b):
    return lax.dot_general(a, b, (((0,), (0,)), ((), ())), preferred_element_type=F32)


def flip(me, bit):
    return me + bit - 2 * bit * lax.rem(me // bit, 2)


def barrier_with(peers):
    sem = pltpu.get_barrier_semaphore()
    for peer in peers:
        pl.semaphore_signal(sem, inc=1, device_id=(peer,), device_id_type=MESH)
    pl.semaphore_wait(sem, len(peers))


class Gather:
    def __init__(self, slot, half, send_sem, recv_sem, me, own=None):
        self.slot, self.half, self.ss, self.rs, self.me = slot, half, send_sem, recv_sem, me
        self.own = slot(me) if own is None else own
        self.pc, self.px, self.py = flip(me, 1), flip(me, 2), flip(me, 4)
        self.pd = flip(self.px, 4)

    def copy(self, kind, src, dst, peer):
        return pltpu.make_async_remote_copy(
            src_ref=src, dst_ref=dst, send_sem=self.ss(kind), recv_sem=self.rs(kind), device_id=(peer,), device_id_type=MESH
        )

    def describe(self, kind):
        me, px, py, pd, pc = self.me, self.px, self.py, self.pd, self.pc
        if kind == 0:
            return self.copy(0, self.own, self.slot(me), px)
        if kind == 1:
            return self.copy(1, self.own, self.slot(me), py)
        if kind == 2:
            return self.copy(2, self.half(px, 0), self.half(px, 0), py)
        if kind == 3:
            return self.copy(3, self.half(py, 1), self.half(py, 1), px)
        if kind == 4:
            return self.copy(4, self.own, self.slot(me), pc)
        if kind == 5:
            return self.copy(5, self.slot(px), self.slot(px), pc)
        if kind == 6:
            return self.copy(6, self.slot(py), self.slot(py), pc)
        return self.copy(kind, self.half(pd, kind - 7), self.half(pd, kind - 7), pc)

    def start(self):
        for kind in (0, 1, 4):
            self.describe(kind).start()

    def forward_pair(self):
        for kind in (0, 1):
            self.describe(kind).wait_recv()
            self.describe(5 + kind).start()

    def forward_cross(self):
        self.describe(2).start()
        self.describe(3).start()

    def forward_far(self):
        self.describe(2).wait_recv()
        self.describe(7).start()
        self.describe(3).wait_recv()
        self.describe(8).start()

    def wait_recv(self, *kinds):
        for kind in kinds:
            self.describe(kind).wait_recv()

    def wait_sends(self, *kinds):
        for kind in kinds or range(9):
            self.describe(kind).wait_send()


def slice_kernel(gate, up, out):
    n, _, fs = out.shape
    rows = gate.shape[0]
    for k in range(n):
        out[k, 0:rows, :] = gate[:, k * fs:(k + 1) * fs]
        out[k, rows:2 * rows, :] = up[:, k * fs:(k + 1) * fs]


def slice_weights(gate, up):
    rows, width = gate.shape
    return pl.pallas_call(
        slice_kernel,
        out_shape=jax.ShapeDtypeStruct((N_DEV, 2 * rows, width // N_DEV), gate.dtype),
        cost_estimate=pl.CostEstimate(flops=1_000_000, bytes_accessed=1_000_000, transcendentals=0),
        name="slices",
    )(gate, up)


def token_kernel(tok, tok_o, send_sem, recv_sem, local_sem):
    me = lax.axis_index("fsdp")
    n = tok_o.shape[0]
    peers = [lax.rem(me + k, n) for k in range(1, n)]
    barrier_with(peers)
    copies = [
        pltpu.make_async_remote_copy(
            src_ref=tok, dst_ref=tok_o.at[me], send_sem=send_sem.at[k], recv_sem=recv_sem.at[k], device_id=(peer,), device_id_type=MESH
        )
        for k, peer in enumerate(peers)
    ]
    local = pltpu.make_async_copy(tok, tok_o.at[me], local_sem)
    for copy in copies:
        copy.start()
    local.start()
    for copy in copies:
        copy.wait()
    local.wait()


def gather_tokens(tok):
    dma = pltpu.SemaphoreType.DMA
    return pl.pallas_call(
        token_kernel,
        out_shape=jax.ShapeDtypeStruct((N_DEV,) + tok.shape, tok.dtype),
        in_specs=[pl.BlockSpec(memory_space=pltpu.VMEM)],
        out_specs=pl.BlockSpec(memory_space=pl.ANY),
        scratch_shapes=[dma((N_DEV - 1,)), dma((N_DEV - 1,)), dma],
        compiler_params=pltpu.CompilerParams(collective_id=0, has_side_effects=True),
        cost_estimate=pl.CostEstimate(flops=5_000_000_000, bytes_accessed=1_000_000, transcendentals=0),
        name="tokens",
    )(tok)


def count_kernel(bounds, keys_a, keys_b, out_a, out_b, list_a, list_b, acc_a, acc_b, in_sem, out_sem):
    n_src = N_DEV
    per = list_a.shape[0] // n_src
    size = acc_a.shape[0]
    BLK = 256
    unroll = 8
    jobs = [(keys_a, out_a, list_a, acc_a), (keys_b, out_b, list_b, acc_b)]
    stores = [pltpu.make_async_copy(acc, out, out_sem.at[k]) for k, (_k, out, _h, acc) in enumerate(jobs)]
    PART = 1024

    def segment(which, src):
        begin = bounds[which * 2 * n_src + src] + src * per
        return begin, bounds[which * 2 * n_src + n_src + src] + src * per

    def fetch(src, run):
        for which, (keys, _o, held, _a) in enumerate(jobs):
            begin, end = segment(which, src)

            def one(t, _):
                at = pl.ds(pl.multiple_of(t * PART, PART), PART)
                run(pltpu.make_async_copy(keys.at[at], held.at[at], in_sem.at[which]))
                return 0

            lax.fori_loop(lax.shift_right_logical(begin, 10), jnp.where(begin < end, lax.shift_right_logical(end + PART - 1, 10), 0), one, 0)

    lax.fori_loop(0, n_src, lambda src, _: (fetch(src, lambda copy: copy.start()), 0)[1], 0)
    lanes = lax.broadcasted_iota(I32, (1, 128), 1)

    def clear(i, _):
        acc_a[pl.ds(i * BLK, BLK), :] = jnp.zeros((BLK, 128), F32)
        acc_b[pl.ds(i * BLK, BLK), :] = jnp.zeros((BLK, 128), F32)
        return 0

    lax.fori_loop(0, size // BLK, clear, 0)
    lax.fori_loop(0, n_src, lambda src, _: (fetch(src, lambda copy: copy.wait()), 0)[1], 0)

    def group(streams, whole):
        done = []
        for held, acc, pos, end in streams:
            places, vals, delta = [], [], None
            for k in range(unroll):
                key = held[pos + k] if whole else held[jnp.minimum(pos + k, end - 1)]
                places.append(key >> 7)
                spread = jnp.full((1, 128), key, I32)
                here = jnp.where(lanes == (spread & 127), 1.0 if whole else jnp.where(pos + k < end, 1.0, 0.0), 0.0)
                delta = here if k == 0 else here + jnp.where((spread ^ before) < 128, delta, 0.0)
                before = spread
                vals.append(acc[pl.ds(places[k], 1), :] + delta)
            done.append((acc, places, vals))
        for acc, places, vals in done:
            for place, val in zip(places, vals):
                acc[pl.ds(place, 1), :] = val

    def source(src, _):
        ranges = []
        for which, (_k, _o, held, acc) in enumerate(jobs):
            begin, end = segment(which, src)
            ranges.append((held, acc, begin, end, lax.shift_right_logical(end - begin, 3)))
        both = jnp.minimum(ranges[0][4], ranges[1][4])

        def step(i, _):
            group([(held, acc, begin + i * unroll, end) for held, acc, begin, end, _n in ranges], True)
            return 0

        lax.fori_loop(0, both, step, 0)
        for held, acc, begin, end, n_whole in ranges:
            def rest(i, _):
                group([(held, acc, begin + i * unroll, end)], True)
                return 0

            lax.fori_loop(both, n_whole, rest, 0)

            @pl.when(begin + n_whole * unroll < end)
            def _():
                group([(held, acc, begin + n_whole * unroll, end)], False)

        return 0

    lax.fori_loop(0, n_src, source, 0)
    for store in stores:
        store.start()
    for store in stores:
        store.wait()


def count(pairs, first, rows, cols):
    bounds, keys, tiles = [], [], cols // 128
    for major, minor in pairs:
        bounds.append(jnp.sum(major < first, axis=(1, 2), dtype=I32))
        bounds.append(jnp.sum(major < first + rows, axis=(1, 2), dtype=I32))
        row = major - first
        keys.append(((((row >> 3) * tiles + (minor >> 7)) * 8 + (row & 7)) * 128 + (minor & 127)).reshape(-1))
    any_spec = pl.BlockSpec(memory_space=pl.ANY)
    tall = (rows * cols // 128, 128)
    outs = pl.pallas_call(
        count_kernel,
        out_shape=(jax.ShapeDtypeStruct(tall, F32),) * 2,
        in_specs=[pl.BlockSpec(memory_space=pltpu.SMEM), any_spec, any_spec],
        out_specs=(any_spec,) * 2,
        scratch_shapes=[pltpu.SMEM(keys[0].shape, I32)] * 2 + [pltpu.VMEM(tall, F32)] * 2 + [pltpu.SemaphoreType.DMA((2,))] * 2,
        cost_estimate=pl.CostEstimate(flops=30_000_000_000, bytes_accessed=16_000_000, transcendentals=0),
        name="count",
    )(jnp.concatenate(bounds), *keys)
    return [out.reshape(rows // 8, tiles, 8, 128) for out in outs]


def finish_kernel(de, got_g, got_u, dwd, de_o, dwg_o, dwu_o, dwd_o):
    n, _, fs = got_g.shape
    de_o[...] = de[...]
    dwd_o[...] = dwd[...]
    for k in range(n):
        dwg_o[:, k * fs:(k + 1) * fs] = got_g[k]
        dwu_o[:, k * fs:(k + 1) * fs] = got_u[k]


def finish(de, got_g, got_u, dwd):
    n, out_rows, fs = got_g.shape
    wide = jax.ShapeDtypeStruct((out_rows, n * fs), F32)
    return pl.pallas_call(finish_kernel, out_shape=(jax.ShapeDtypeStruct(de.shape, F32), wide, wide, jax.ShapeDtypeStruct(dwd.shape, F32)), name="finish")(
        de, got_g, got_u, dwd
    )


def step_kernel(
    coef_ref, emb_me, emb_x, emb_y, gu_me, gu_x, gu_y, gu_d, wd_me, wd_x, wd_y, wd_d, crow_hbm, ccol_hbm, g1_ref, g2_ref,
    loss_o, de_out, got_g, got_u, dwd_out,
    de_o, dwd_o, emb, wg, wu, wd, cnt, hn, dh, a_all, p_own, q_own, q_all, logits, dlog, h_wide, acc, stat, stat_col, top, sums,
    dwg, dwu, load_sem, pair_s, pair_r, es, er, hs, hr, ds_, dr, st_s, st_r, ws, wr, out_sem,
):
    me = lax.axis_index("fsdp")
    n = wg.shape[0]
    rows, width = h_wide.shape
    fs = wg.shape[2]
    out_rows = got_g.shape[1]
    coef = coef_ref[0, 0]
    ph = Phases()
    ph("a_start")
    NB = 128
    RB = 64
    wide = logits.shape[2]
    tiles = wide // 128
    peers = [lax.rem(me + k, n) for k in range(1, n)]

    def block(dev):
        return pl.ds(pl.multiple_of(dev * rows, rows), rows)

    def p_at(s):
        return (slice(None), pl.ds(pl.multiple_of(2 * rows + s * 256, 256), fs))

    mine = block(me)
    pc, px, py = flip(me, 1), flip(me, 2), flip(me, 4)
    pd = flip(px, 4)
    devs = [me, px, py, pd]
    parts = []
    for dev, down in zip(devs, [wd_me, wd_x, wd_y, wd_d]):
        parts.append((down, wd.at[dev]))
    for wave in range(2):
        part = pl.ds(wave * (n // 2), n // 2)
        for dev, gu in zip(devs, [gu_me, gu_x, gu_y, gu_d]):
            at = pl.ds(dev * out_rows, out_rows)
            parts.append((gu.at[part, 0:out_rows, :], wg.at[part, at, :]))
            parts.append((gu.at[part, out_rows:2 * out_rows, :], wu.at[part, at, :]))
    n_first = len(parts) - 2 * len(devs)
    n_weight = len(parts)
    for dev, part in zip(devs, [emb_me, emb_x, emb_y]):
        parts.append((part, emb.at[block(dev), :]))
    loads = [pltpu.make_async_copy(src, dst, load_sem.at[k]) for k, (src, dst) in enumerate(parts)]
    pairs = [
        pltpu.make_async_remote_copy(
            src_ref=src, dst_ref=dst, send_sem=pair_s.at[k], recv_sem=pair_r.at[k], device_id=(pc,), device_id_type=MESH
        )
        for k, (src, dst) in enumerate(parts)
    ]
    row_counts = pltpu.make_async_copy(crow_hbm, cnt, load_sem.at[len(parts)])
    col_counts = pltpu.make_async_copy(ccol_hbm, cnt, load_sem.at[len(parts) + 1])

    barrier = pltpu.get_barrier_semaphore()
    for peer in peers:
        pl.semaphore_signal(barrier, inc=1, device_id=(peer,), device_id_type=MESH)
    for load in loads[n_weight:] + loads[:n_weight]:
        load.start()
    def gather_of(buf, ss, rs):
        half = rows // 2
        return Gather(
            lambda d: buf.at[block(d), :],
            lambda d, i: buf.at[pl.ds(pl.multiple_of(d * rows + i * half, half), half), :],
            lambda c: ss.at[c], lambda c: rs.at[c], me,
        )

    emb_g, hn_g, dh_g = gather_of(emb, es, er), gather_of(hn, hs, hr), gather_of(dh, ds_, dr)
    g1, g2 = g1_ref[...], g2_ref[...]

    ph("d_norm")

    def norm_rows(dev):
        def norm(i, _):
            at = pl.ds(pl.multiple_of(dev * rows + i * NB, NB), NB)
            x = emb[at, :].astype(F32)
            inv = lax.rsqrt(jnp.mean(x * x, axis=-1, keepdims=True) + NORM_EPS)
            a_all[at, :] = (x * inv * g1).astype(BF16)
            return 0

        lax.fori_loop(0, rows // NB, norm, 0, unroll=2)

    for load in loads[n_weight:]:
        load.wait()
    norm_rows(me)
    ph("b_barrier")
    pl.semaphore_wait(barrier, len(peers))
    for pair in pairs:
        pair.start()
    emb_g.forward_cross()
    row_counts.start()
    norm_rows(px)
    norm_rows(py)

    ph("e_waitW")
    def weights_here(low, high):
        for load, pair in zip(loads[low:high], pairs[low:high]):
            load.wait()
            pair.wait_recv()

    weights_here(0, n_first)
    ph("f_fwd")
    acc[...] = jnp.zeros_like(acc)

    def forward(j, _):
        a = a_all[mine, :]
        p = dot_nn(a, wg[j]).astype(BF16)
        q = dot_nn(a, wu[j]).astype(BF16)
        p_own[j], q_own[j] = p, q
        p, q = p.astype(F32), q.astype(F32)
        u = (p * jax.nn.sigmoid(p) * q).astype(BF16)
        acc[...] += dot_nn(u, wd[j])
        return 0

    lax.fori_loop(0, n // 2, forward, 0, unroll=2)
    emb_g.forward_far()
    weights_here(n_first, n_weight)
    lax.fori_loop(n // 2, n, forward, 0, unroll=2)
    ph("g_hidden")

    def hidden(i, _):
        at = pl.ds(pl.multiple_of(i * NB, NB), NB)
        row = pl.ds(pl.multiple_of(me * rows + i * NB, NB), NB)
        h = (emb[row, :].astype(F32) + acc[at, :]).astype(BF16).astype(F32)
        h_wide[at, :] = h
        inv = lax.rsqrt(jnp.mean(h * h, axis=-1, keepdims=True) + NORM_EPS)
        hn[row, :] = (h * inv * g2).astype(BF16)
        return 0

    lax.fori_loop(0, rows // NB, hidden, 0, unroll=2)
    hn_g.start()
    ph("h_waitE")
    for pair in pairs[n_weight:]:
        pair.wait_recv()
    emb_g.wait_recv(7, 8)

    ph("i_logit")
    top[...] = jnp.full_like(top, -jnp.inf)

    def logit(v, _):
        val = dot_nt(hn[mine, :], emb[pl.ds(pl.multiple_of(v * wide, wide), wide), :])
        logits[v] = val
        m = top[...]
        for k in range(tiles):
            m = jnp.maximum(m, val[:, k * 128:(k + 1) * 128])
        top[...] = m
        return 0

    lax.fori_loop(0, n * rows // wide, logit, 0)
    row_counts.wait()
    ph("j_softmax")
    top[...] = jnp.max(top[...], axis=-1, keepdims=True) + jnp.zeros((rows, 128), F32)

    def counts(i, v, k):
        return cnt[pl.ds(i * (RB // 8), RB // 8), v * tiles + k].reshape(RB, 128)

    def total(i, _):
        at = pl.ds(pl.multiple_of(i * RB, RB), RB)
        m = top[at, :]

        def part(v, carry):
            s, c, pick = carry
            for k in range(tiles):
                cut = slice(k * 128, (k + 1) * 128)
                val, num = logits[v, at, cut], counts(i, v, k)
                ex = jnp.exp(val - m)
                logits[v, at, cut] = ex
                s, c, pick = s + ex, c + num, pick + num * val
            return s, c, pick

        zero = jnp.zeros((RB, 128), F32)
        sums[0, at, :], sums[1, at, :], sums[2, at, :] = lax.fori_loop(0, n * rows // wide, part, (zero, zero, zero))
        return 0

    lax.fori_loop(0, rows // RB, total, 0)
    s, c, pick = [jnp.sum(sums[k], axis=-1, keepdims=True) for k in range(3)]
    lse = top[:, 0:1] + jnp.log(s)
    lane = lax.broadcasted_iota(I32, (rows, 128), 1)
    stat_col[...] = jnp.where(lane == 0, lse, jnp.where(lane == 1, c * coef, jnp.where(lane == 2, c * lse - pick, 0.0)))
    sums[0] = c * coef / s + jnp.zeros((rows, 128), F32)

    def grad(i, _):
        at = pl.ds(pl.multiple_of(i * RB, RB), RB)
        scale = sums[0, at, :]

        def part(v, _):
            for k in range(tiles):
                cut = slice(k * 128, (k + 1) * 128)
                here = pl.ds(pl.multiple_of(v * wide + k * 128, 128), 128)
                dlog[at, here] = (logits[v, at, cut] * scale - counts(i, v, k) * coef).astype(BF16)
            return 0

        lax.fori_loop(0, n * rows // wide, part, 0)
        return 0

    lax.fori_loop(0, rows // RB, grad, 0)
    col_counts.start()
    stat[me] = jnp.transpose(stat_col[...])[0:8, :]
    ph("k_dhn")
    acc[...] = dot_nn(dlog[...], emb[...])
    stat_copies = [
        pltpu.make_async_remote_copy(
            src_ref=stat.at[me], dst_ref=stat.at[me], send_sem=st_s.at[k], recv_sem=st_r.at[k], device_id=(peer,), device_id_type=MESH
        )
        for k, peer in enumerate(peers)
    ]
    for copy in stat_copies:
        copy.start()
    ph("l_dhidden")

    def dhidden(i, _):
        at = pl.ds(pl.multiple_of(i * NB, NB), NB)
        h, scaled = h_wide[at, :], acc[at, :] * g2
        inv = lax.rsqrt(jnp.mean(h * h, axis=-1, keepdims=True) + NORM_EPS)
        grad = inv * (scaled - h * (inv * inv) * jnp.mean(scaled * h, axis=-1, keepdims=True))
        de_o[at, :] = grad
        dh[pl.ds(pl.multiple_of(me * rows + i * NB, NB), NB), :] = grad.astype(BF16)
        return 0

    lax.fori_loop(0, rows // NB, dhidden, 0, unroll=2)
    dh_g.start()

    ph("n_norm")
    for dev in [pd] + [flip(dev, 1) for dev in devs]:
        norm_rows(dev)
    ph("o_slice")

    def slice_forward(s, _):
        a = a_all[block(s), :]
        dlog[p_at(s)] = dot_nn(a, wg[me]).astype(BF16)
        q_all[s] = dot_nn(a, wu[me]).astype(BF16)
        return 0

    lax.fori_loop(0, n, slice_forward, 0, unroll=2)

    ph("m_hnnear")
    hn_g.forward_pair()

    ph("p_back")
    acc[...] = jnp.zeros_like(acc)

    def act_back(dact, p, q):
        sig = jax.nn.sigmoid(p)
        gated = p * sig
        dq = (dact * gated).astype(BF16)
        dp = (dact * q * sig * (1.0 + p * (1.0 - sig))).astype(BF16)
        return dp, dq, (gated * q).astype(BF16)

    def backward(j, _):
        dact = dot_nt(dh[mine, :], wd[j])
        dp, dq, _u = act_back(dact, p_own[j].astype(F32), q_own[j].astype(F32))
        acc[...] += dot_nt(dp, wg[j]) + dot_nt(dq, wu[j])
        return 0

    lax.fori_loop(0, n, backward, 0, unroll=2)
    ph("q_dinput")

    def dinput(i, _):
        at = pl.ds(pl.multiple_of(i * NB, NB), NB)
        x, scaled = emb[pl.ds(pl.multiple_of(me * rows + i * NB, NB), NB), :].astype(F32), acc[at, :] * g1
        inv = lax.rsqrt(jnp.mean(x * x, axis=-1, keepdims=True) + NORM_EPS)
        de_o[at, :] += inv * (scaled - x * (inv * inv) * jnp.mean(scaled * x, axis=-1, keepdims=True))
        return 0

    lax.fori_loop(0, rows // NB, dinput, 0, unroll=2)
    ph("r_stat")
    for copy in stat_copies:
        copy.wait_recv()
    col_counts.wait()

    def head(dev):
        low = dev - lax.rem(dev, 2)
        pair = pl.ds(pl.multiple_of(low * rows, 2 * rows), 2 * rows)
        for k in range(2 * rows // 256):
            source, cut = low + k * 256 // rows, slice(k * 256 % rows, k * 256 % rows + 256)
            lt = dot_nt(emb[mine, :], hn[pl.ds(pl.multiple_of(low * rows + k * 256, 256), 256), :])
            tile = low * (rows // 128) + 2 * k
            num = jnp.concatenate([cnt[:, tile].reshape(rows, 128), cnt[:, tile + 1].reshape(rows, 128)], axis=1)
            prob = jnp.exp(lt - stat[source, 0:1, cut]) * stat[source, 1:2, cut]
            dlog[:, k * 256:(k + 1) * 256] = (prob - num * coef).astype(BF16)
        de_o[...] += dot_nn(dlog[:, 0:2 * rows], hn[pair, :])

    dwg[...] = jnp.zeros_like(dwg)
    dwu[...] = jnp.zeros_like(dwu)
    dwd_o[...] = jnp.zeros_like(dwd_o)

    def act_grads(dev):
        dact = dot_nt(dh[block(dev), :], wd[me])
        return act_back(dact, dlog[p_at(dev)].astype(F32), q_all[dev].astype(F32))

    def weights(dev):
        dp, dq, u = act_grads(dev)
        dwd_o[...] += dot_tn(u, dh[block(dev), :])
        dwg[...] += dot_tn(a_all[block(dev), :], dp)
        dwu[...] += dot_tn(a_all[block(dev), :], dq)

    def exchange(k, peer, src, dst, row):
        return pltpu.make_async_remote_copy(
            src_ref=src.at[pl.ds(pl.multiple_of(peer * out_rows, out_rows), out_rows), :],
            dst_ref=dst.at[me],
            send_sem=ws.at[row, k], recv_sem=wr.at[row, k], device_id=(peer,), device_id_type=MESH,
        )

    swaps_g = [exchange(k, peer, dwg, got_g, 0) for k, peer in enumerate(peers)]
    swaps_u = [exchange(k, peer, dwu, got_u, 1) for k, peer in enumerate(peers)]

    ph("s_w01")
    dh_g.wait_recv(4)
    weights(me)
    weights(pc)
    ph("t_dhnear")
    dh_g.forward_pair()
    dh_g.forward_cross()
    hn_g.forward_cross()
    ph("u_w23")
    weights(px)
    weights(py)
    ph("v_w45")
    dh_g.wait_recv(5, 6)
    weights(flip(px, 1))
    weights(flip(py, 1))
    ph("w_heads")
    hn_g.wait_recv(4, 5, 6)
    head(me)
    head(px)
    head(py)
    ph("x_dhfar")
    dh_g.forward_far()
    ph("y_late")
    late = [pd, flip(pd, 1)]
    for k, kinds in ((0, ()), (1, (7, 8))):
        dh_g.wait_recv(*kinds)
        dev = late[k]
        dlog[p_at(dev)], q_all[dev], dlog[p_at(n + k)] = act_grads(dev)
        dwg[...] += dot_tn(a_all[block(dev), :], dlog[p_at(dev)])
    for swap in swaps_g:
        swap.start()
    for dev in late:
        dwu[...] += dot_tn(a_all[block(dev), :], q_all[dev])
    for swap in swaps_u:
        swap.start()
    keep = pl.ds(pl.multiple_of(me * out_rows, out_rows), out_rows)
    outs = [pltpu.make_async_copy(dwg.at[keep, :], got_g.at[me], out_sem.at[0]), pltpu.make_async_copy(dwu.at[keep, :], got_u.at[me], out_sem.at[1])]
    for out in outs:
        out.start()
    for k, dev in enumerate(late):
        dwd_o[...] += dot_tn(dlog[p_at(n + k)], dh[block(dev), :])
    ph("z_hnfar")
    hn_g.forward_far()
    outs.append(pltpu.make_async_copy(dwd_o, dwd_out, out_sem.at[2]))
    outs[-1].start()
    hn_g.wait_recv(7, 8)
    ph("za_head")
    head(pd)
    outs.append(pltpu.make_async_copy(de_o, de_out, out_sem.at[3]))
    outs[-1].start()
    total_loss = jnp.zeros((1, rows), F32)
    for s in range(n):
        total_loss = total_loss + stat[s, 2:3, :]
    loss_o[...] = jnp.sum(total_loss, axis=-1, keepdims=True) * coef + jnp.zeros((1, 128), F32)
    ph("zd_waits")
    for copy in stat_copies:
        copy.wait_send()
    emb_g.wait_sends(2, 3, 7, 8)
    hn_g.wait_sends()
    dh_g.wait_sends()
    for pair in pairs:
        pair.wait_send()
    for out in outs:
        out.wait()
    for swap in swaps_g + swaps_u:
        swap.wait()
    ph()


def run_step(coef, embs, gus, downs, crow, ccol, g1, g2):
    n = N_DEV
    rows, width = embs[0].shape
    fs = gus[0].shape[2]
    out_rows = width // n
    any_spec = pl.BlockSpec(memory_space=pl.ANY)
    vmem = pl.BlockSpec(memory_space=pltpu.VMEM)
    dma = pltpu.SemaphoreType.DMA
    return pl.pallas_call(
        step_kernel,
        out_shape=(
            jax.ShapeDtypeStruct((1, 128), F32),
            jax.ShapeDtypeStruct((rows, width), F32),
            jax.ShapeDtypeStruct((n, out_rows, fs), F32),
            jax.ShapeDtypeStruct((n, out_rows, fs), F32),
            jax.ShapeDtypeStruct((fs, width), F32),
        ),
        in_specs=[pl.BlockSpec(memory_space=pltpu.SMEM)] + [any_spec] * 13 + [vmem] * 2,
        out_specs=(vmem,) + (any_spec,) * 4,
        scratch_shapes=[
            pltpu.VMEM((rows, width), F32),
            pltpu.VMEM((fs, width), F32),
            pltpu.VMEM((n * rows, width), BF16),
            pltpu.VMEM((n, width, fs), BF16),
            pltpu.VMEM((n, width, fs), BF16),
            pltpu.VMEM((n, fs, width), BF16),
            pltpu.VMEM((rows // 8, n * rows // 128, 8, 128), F32),
            pltpu.VMEM((n * rows, width), BF16),
            pltpu.VMEM((n * rows, width), BF16),
            pltpu.VMEM((n * rows, width), BF16),
            pltpu.VMEM((n, rows, fs), BF16),
            pltpu.VMEM((n, rows, fs), BF16),
            pltpu.VMEM((n, rows, fs), BF16),
            pltpu.VMEM((n // 2, rows, 2 * rows), F32),
            pltpu.VMEM((rows, n * rows), BF16),
            pltpu.VMEM((rows, width), F32),
            pltpu.VMEM((rows, width), F32),
            pltpu.VMEM((n, 8, rows), F32),
            pltpu.VMEM((rows, 128), F32),
            pltpu.VMEM((rows, 128), F32),
            pltpu.VMEM((3, rows, 128), F32),
            pltpu.VMEM((width, fs), F32),
            pltpu.VMEM((width, fs), F32),
            dma((25,)), dma((23,)), dma((23,)), dma((9,)), dma((9,)), dma((9,)), dma((9,)), dma((9,)), dma((9,)), dma((n - 1,)), dma((n - 1,)), dma((2, n - 1)), dma((2, n - 1)), dma((4,)),
        ],
        compiler_params=pltpu.CompilerParams(collective_id=1, has_side_effects=True, vmem_limit_bytes=VMEM_MAX),
        name="step",
    )(coef, *embs, *gus, *downs, crow, ccol, g1, g2)


def solution(mesh):
    def device_step(tok_ids, tok_labels, loss_mask, emb, g1, g2, w_gate, w_up, w_down):
        n = N_DEV
        rows, width = emb.shape
        vocab = rows * n
        n_tok = tok_ids.shape[0]
        me = lax.axis_index("fsdp")

        def send(bit):
            pairs = [(d, d ^ bit) for d in range(n)]
            return lambda val: lax.ppermute(val, "fsdp", pairs)

        along_x, along_y = send(2), send(4)
        gu = slice_weights(w_gate, w_up)
        gus, downs = [[val, along_x(val), along_y(val)] for val in (gu, w_down)]

        live = loss_mask != 0
        by_id = lax.sort(jnp.where(live, tok_ids * 65536 + tok_labels, vocab * 65536), is_stable=False)
        by_label = lax.sort(jnp.where(live, tok_labels * 65536 + tok_ids, vocab * 65536), is_stable=False)
        tok = [part.reshape(n_tok // 128, 128) for part in (by_id >> 16, by_id & 65535, by_label >> 16, by_label & 65535)]
        tok = gather_tokens(jnp.concatenate(tok).astype(jnp.int16))
        tok, gus[2], downs[1], emb_later = lax.optimization_barrier((tok, gus[2], downs[1], emb))
        embs = [emb, along_x(emb_later), along_y(emb_later)]
        gus.append(along_x(gus[2]))
        downs.append(along_y(downs[1]))
        ids, labels, labels2, ids2 = [tok[:, k * (n_tok // 128):(k + 1) * (n_tok // 128)].astype(I32) for k in range(4)]
        crow, ccol = count([(ids, labels), (labels2, ids2)], me * rows, rows, vocab)
        n_live = jnp.sum(ids < vocab).astype(F32)
        coef = (1.0 / n_live).reshape(1, 1)
        loss, *grads = run_step(coef, embs, gus, downs, crow, ccol, g1.reshape(1, width), g2.reshape(1, width))
        return (loss[0, 0], *finish(*grads))

    row_spec = P("fsdp", None)
    tok_spec = P("fsdp")
    return jax.shard_map(device_step, mesh=mesh, in_specs=(tok_spec, tok_spec, tok_spec, row_spec, P(), P(), row_spec, row_spec, row_spec), out_specs=(P(), row_spec, row_spec, row_spec, row_spec), check_vma=False)
```

```python
import functools

import jax
import jax.numpy as jnp
from jax import lax
from jax.experimental import pallas as pl
from jax.experimental.pallas import tpu as pltpu
from jax.sharding import PartitionSpec as P


NORM_EPS = 1e-6
N_DEV = 8
F32, BF16, I32 = jnp.float32, jnp.bfloat16, jnp.int32
MESH = pl.DeviceIdType.MESH
VMEM_MAX = 66_000_000
VMEM_ALL = 67_000_000


class Phases:
    def __init__(self):
        self.now = None

    def __call__(self, name=None):
        if self.now is not None:
            self.now.__exit__(None, None, None)
        self.now = jax.named_scope(name) if name else None
        if self.now is not None:
            self.now.__enter__()


def dot_nn(a, b):
    return jnp.dot(a, b, preferred_element_type=F32)


def dot_nt(a, b):
    return lax.dot_general(a, b, (((1,), (1,)), ((), ())), preferred_element_type=F32)


def dot_tn(a, b):
    return lax.dot_general(a, b, (((0,), (0,)), ((), ())), preferred_element_type=F32)


def flip(me, bit):
    return me + bit - 2 * bit * lax.rem(me // bit, 2)


def barrier_with(peers):
    sem = pltpu.get_barrier_semaphore()
    for peer in peers:
        pl.semaphore_signal(sem, inc=1, device_id=(peer,), device_id_type=MESH)
    pl.semaphore_wait(sem, len(peers))


class Gather:
    def __init__(self, slot, half, send_sem, recv_sem, me):
        self.slot, self.half, self.ss, self.rs, self.me = slot, half, send_sem, recv_sem, me
        self.pc, self.px, self.py = flip(me, 1), flip(me, 2), flip(me, 4)
        self.pd = flip(self.px, 4)

    def copy(self, kind, src, dst, peer):
        return pltpu.make_async_remote_copy(
            src_ref=src, dst_ref=dst, send_sem=self.ss(kind), recv_sem=self.rs(kind), device_id=(peer,), device_id_type=MESH
        )

    def describe(self, kind):
        me, px, py, pd, pc = self.me, self.px, self.py, self.pd, self.pc
        if kind in (0, 9):
            return self.copy(kind, self.half(me, kind // 9), self.half(me, kind // 9), px)
        if kind in (1, 10):
            return self.copy(kind, self.half(me, 1 - kind // 10), self.half(me, 1 - kind // 10), py)
        if kind == 2:
            return self.copy(2, self.half(px, 0), self.half(px, 0), py)
        if kind == 3:
            return self.copy(3, self.half(py, 1), self.half(py, 1), px)
        if kind == 4:
            return self.copy(4, self.slot(me), self.slot(me), pc)
        if kind == 5:
            return self.copy(5, self.slot(px), self.slot(px), pc)
        if kind == 6:
            return self.copy(6, self.slot(py), self.slot(py), pc)
        return self.copy(kind, self.half(pd, kind - 7), self.half(pd, kind - 7), pc)

    def start(self):
        for kind in (0, 1, 9, 10, 4):
            self.describe(kind).start()

    def forward_pair(self):
        for kind in (0, 1):
            self.describe(9 + kind).wait_recv()
            self.describe(5 + kind).start()

    def forward_cross(self, wait=True):
        for kind in (0, 1):
            if wait:
                self.describe(kind).wait_recv()
            self.describe(2 + kind).start()

    def forward_far(self):
        self.describe(2).wait_recv()
        self.describe(7).start()
        self.describe(3).wait_recv()
        self.describe(8).start()

    def wait_recv(self, *kinds):
        for kind in kinds:
            self.describe(kind).wait_recv()

    def wait_sends(self, *kinds):
        for kind in kinds or range(11):
            self.describe(kind).wait_send()


def slice_kernel(gate, up, out):
    n, _, fs = out.shape
    rows = gate.shape[0]
    for k in range(n):
        out[k, 0:rows, :] = gate[:, k * fs:(k + 1) * fs]
        out[k, rows:2 * rows, :] = up[:, k * fs:(k + 1) * fs]


def slice_weights(gate, up):
    rows, width = gate.shape
    return pl.pallas_call(
        slice_kernel,
        out_shape=jax.ShapeDtypeStruct((N_DEV, 2 * rows, width // N_DEV), gate.dtype),
        cost_estimate=pl.CostEstimate(flops=1_000_000, bytes_accessed=1_000_000, transcendentals=0),
        name="slices",
    )(gate, up)


def token_kernel(tok, tok_o, send_sem, recv_sem, local_sem):
    me = lax.axis_index("fsdp")
    n = tok_o.shape[0]
    peers = [lax.rem(me + k, n) for k in range(1, n)]
    barrier_with(peers)
    copies = [
        pltpu.make_async_remote_copy(
            src_ref=tok, dst_ref=tok_o.at[me], send_sem=send_sem.at[k], recv_sem=recv_sem.at[k], device_id=(peer,), device_id_type=MESH
        )
        for k, peer in enumerate(peers)
    ]
    local = pltpu.make_async_copy(tok, tok_o.at[me], local_sem)
    for copy in copies:
        copy.start()
    local.start()
    for copy in copies:
        copy.wait()
    local.wait()


def gather_tokens(tok):
    dma = pltpu.SemaphoreType.DMA
    return pl.pallas_call(
        token_kernel,
        out_shape=jax.ShapeDtypeStruct((N_DEV,) + tok.shape, tok.dtype),
        in_specs=[pl.BlockSpec(memory_space=pltpu.VMEM)],
        out_specs=pl.BlockSpec(memory_space=pl.ANY),
        scratch_shapes=[dma((N_DEV - 1,)), dma((N_DEV - 1,)), dma],
        compiler_params=pltpu.CompilerParams(collective_id=0, has_side_effects=True, vmem_limit_bytes=VMEM_ALL),
        cost_estimate=pl.CostEstimate(flops=5_000_000_000, bytes_accessed=1_000_000, transcendentals=0),
        name="tokens",
    )(tok)


def count_kernel(bounds, keys_a, keys_b, out_a, out_b, list_a, list_b, acc_a, acc_b, in_sem, out_sem):
    n_src = N_DEV
    per = list_a.shape[0] // n_src
    size = acc_a.shape[0]
    BLK = 256
    unroll = 8
    jobs = [(keys_a, out_a, list_a, acc_a), (keys_b, out_b, list_b, acc_b)]
    stores = [pltpu.make_async_copy(acc, out, out_sem.at[k]) for k, (_k, out, _h, acc) in enumerate(jobs)]
    PART = 1024

    def segment(which, src):
        begin = bounds[which * 2 * n_src + src] + src * per
        return begin, bounds[which * 2 * n_src + n_src + src] + src * per

    def fetch(src, run):
        for which, (keys, _o, held, _a) in enumerate(jobs):
            begin, end = segment(which, src)

            def one(t, _):
                at = pl.ds(pl.multiple_of(t * PART, PART), PART)
                run(pltpu.make_async_copy(keys.at[at], held.at[at], in_sem.at[which]))
                return 0

            lax.fori_loop(lax.shift_right_logical(begin, 10), jnp.where(begin < end, lax.shift_right_logical(end + PART - 1, 10), 0), one, 0)

    lax.fori_loop(0, n_src, lambda src, _: (fetch(src, lambda copy: copy.start()), 0)[1], 0)
    lanes = lax.broadcasted_iota(I32, (1, 128), 1)

    def clear(i, _):
        acc_a[pl.ds(i * BLK, BLK), :] = jnp.zeros((BLK, 128), F32)
        acc_b[pl.ds(i * BLK, BLK), :] = jnp.zeros((BLK, 128), F32)
        return 0

    lax.fori_loop(0, size // BLK, clear, 0)
    lax.fori_loop(0, n_src, lambda src, _: (fetch(src, lambda copy: copy.wait()), 0)[1], 0)

    def group(streams, whole):
        done = []
        for held, acc, pos, end in streams:
            places, vals, delta = [], [], None
            for k in range(unroll):
                key = held[pos + k] if whole else held[jnp.minimum(pos + k, end - 1)]
                places.append(key >> 7)
                spread = jnp.full((1, 128), key, I32)
                here = jnp.where(lanes == (spread & 127), 1.0 if whole else jnp.where(pos + k < end, 1.0, 0.0), 0.0)
                delta = here if k == 0 else here + jnp.where((spread ^ before) < 128, delta, 0.0)
                before = spread
                vals.append(acc[pl.ds(places[k], 1), :] + delta)
            done.append((acc, places, vals))
        for acc, places, vals in done:
            for place, val in zip(places, vals):
                acc[pl.ds(place, 1), :] = val

    def source(src, _):
        ranges = []
        for which, (_k, _o, held, acc) in enumerate(jobs):
            begin, end = segment(which, src)
            ranges.append((held, acc, begin, end, lax.shift_right_logical(end - begin, 3)))
        both = jnp.minimum(ranges[0][4], ranges[1][4])

        def step(i, _):
            group([(held, acc, begin + i * unroll, end) for held, acc, begin, end, _n in ranges], True)
            return 0

        lax.fori_loop(0, both, step, 0)
        for held, acc, begin, end, n_whole in ranges:
            def rest(i, _):
                group([(held, acc, begin + i * unroll, end)], True)
                return 0

            lax.fori_loop(both, n_whole, rest, 0)

            @pl.when(begin + n_whole * unroll < end)
            def _():
                group([(held, acc, begin + n_whole * unroll, end)], False)

        return 0

    lax.fori_loop(0, n_src, source, 0)
    for store in stores:
        store.start()
    for store in stores:
        store.wait()


def count(pairs, first, rows, cols):
    bounds, keys, tiles = [], [], cols // 128
    for major, minor in pairs:
        bounds.append(jnp.sum(major < first, axis=(1, 2), dtype=I32))
        bounds.append(jnp.sum(major < first + rows, axis=(1, 2), dtype=I32))
        row = major - first
        keys.append(((((row >> 3) * tiles + (minor >> 7)) * 8 + (row & 7)) * 128 + (minor & 127)).reshape(-1))
    any_spec = pl.BlockSpec(memory_space=pl.ANY)
    tall = (rows * cols // 128, 128)
    outs = pl.pallas_call(
        count_kernel,
        out_shape=(jax.ShapeDtypeStruct(tall, F32),) * 2,
        in_specs=[pl.BlockSpec(memory_space=pltpu.SMEM), any_spec, any_spec],
        out_specs=(any_spec,) * 2,
        scratch_shapes=[pltpu.SMEM(keys[0].shape, I32)] * 2 + [pltpu.VMEM(tall, F32)] * 2 + [pltpu.SemaphoreType.DMA((2,))] * 2,
        compiler_params=pltpu.CompilerParams(vmem_limit_bytes=VMEM_ALL),
        cost_estimate=pl.CostEstimate(flops=30_000_000_000, bytes_accessed=16_000_000, transcendentals=0),
        name="count",
    )(jnp.concatenate(bounds), *keys)
    return [out.reshape(rows // 8, tiles, 8, 128) for out in outs]


def finish_kernel(de, got_g, got_u, dwd, de_o, dwg_o, dwu_o, dwd_o, de_v, g_v, u_v, dwd_v, wg_v, wu_v, in_sem, out_sem):
    n, _, fs = g_v.shape
    ins = [pltpu.make_async_copy(src, dst, in_sem.at[k]) for k, (src, dst) in enumerate([(got_g, g_v), (got_u, u_v), (de, de_v), (dwd, dwd_v)])]
    outs = [pltpu.make_async_copy(src, dst, out_sem.at[k]) for k, (src, dst) in enumerate([(wg_v, dwg_o), (wu_v, dwu_o), (de_v, de_o), (dwd_v, dwd_o)])]
    for copy in ins:
        copy.start()
    for which, (src, dst) in enumerate([(g_v, wg_v), (u_v, wu_v)]):
        ins[which].wait()
        for k in range(n):
            dst[:, k * fs:(k + 1) * fs] = src[k]
        if which == 1:
            outs[0].start()
    for which in (2, 3):
        ins[which].wait()
        outs[which].start()
    outs[1].start()
    for copy in outs:
        copy.wait()


def finish(de, got_g, got_u, dwd):
    n, out_rows, fs = got_g.shape
    wide = jax.ShapeDtypeStruct((out_rows, n * fs), F32)
    any_spec = pl.BlockSpec(memory_space=pl.ANY)
    held = [pltpu.VMEM(val.shape, F32) for val in (de, got_g, got_u, dwd, wide, wide)]
    return pl.pallas_call(
        finish_kernel,
        out_shape=(jax.ShapeDtypeStruct(de.shape, F32), wide, wide, jax.ShapeDtypeStruct(dwd.shape, F32)),
        in_specs=[any_spec] * 4,
        out_specs=(any_spec,) * 4,
        scratch_shapes=held + [pltpu.SemaphoreType.DMA((4,)), pltpu.SemaphoreType.DMA((4,))],
        compiler_params=pltpu.CompilerParams(vmem_limit_bytes=VMEM_ALL),
        name="finish",
    )(de, got_g, got_u, dwd)


def step_kernel(
    coef_ref, emb_me, emb_x, emb_y, gu_me, gu_x, gu_y, gu_d, wd_me, wd_x, wd_y, wd_d, crow_hbm, ccol_hbm, g1_ref, g2_ref,
    loss_o, de_out, got_g, got_u, dwd_out,
    de_o, dwd_o, emb, wg, wu, wd, cnt, hn, dh, a_all, p_own, q_own, q_all, logits, dlog, h_wide, acc, stat, stat_col, top, sums,
    dwg, dwu, load_sem, pair_s, pair_r, es, er, hs, hr, ds_, dr, st_s, st_r, ws, wr, out_sem,
):
    me = lax.axis_index("fsdp")
    n = wg.shape[0]
    rows, width = h_wide.shape
    fs = wg.shape[2]
    out_rows = got_g.shape[1]
    coef = coef_ref[0, 0]
    ph = Phases()
    ph("a_start")
    NB = 128
    RB = 64
    wide = logits.shape[2]
    tiles = wide // 128
    peers = [lax.rem(me + k, n) for k in range(1, n)]

    def block(dev):
        return pl.ds(pl.multiple_of(dev * rows, rows), rows)

    def p_at(s):
        return (slice(None), pl.ds(pl.multiple_of(2 * rows + s * 256, 256), fs))

    mine = block(me)
    pc, px, py = flip(me, 1), flip(me, 2), flip(me, 4)
    pd = flip(px, 4)
    devs = [me, px, py, pd]
    parts = []
    for dev, down in zip(devs, [wd_me, wd_x, wd_y, wd_d]):
        parts.append((down, wd.at[dev]))
    for wave in range(2):
        part = pl.ds(wave * (n // 2), n // 2)
        for dev, gu in zip(devs, [gu_me, gu_x, gu_y, gu_d]):
            at = pl.ds(dev * out_rows, out_rows)
            parts.append((gu.at[part, 0:out_rows, :], wg.at[part, at, :]))
            parts.append((gu.at[part, out_rows:2 * out_rows, :], wu.at[part, at, :]))
    n_first = len(parts) - 2 * len(devs)
    n_weight = len(parts)
    for dev, part in zip(devs, [emb_me, emb_x, emb_y]):
        parts.append((part, emb.at[block(dev), :]))
    loads = [pltpu.make_async_copy(src, dst, load_sem.at[k]) for k, (src, dst) in enumerate(parts)]
    pairs = [
        pltpu.make_async_remote_copy(
            src_ref=src, dst_ref=dst, send_sem=pair_s.at[k], recv_sem=pair_r.at[k], device_id=(pc,), device_id_type=MESH
        )
        for k, (src, dst) in enumerate(parts)
    ]
    row_counts = pltpu.make_async_copy(crow_hbm, cnt, load_sem.at[len(parts)])
    col_counts = pltpu.make_async_copy(ccol_hbm, cnt, load_sem.at[len(parts) + 1])

    barrier = pltpu.get_barrier_semaphore()
    for peer in peers:
        pl.semaphore_signal(barrier, inc=1, device_id=(peer,), device_id_type=MESH)
    for load in loads[n_weight:] + loads[:n_weight]:
        load.start()
    def gather_of(buf, ss, rs):
        half = rows // 2
        return Gather(
            lambda d: buf.at[block(d), :],
            lambda d, i: buf.at[pl.ds(pl.multiple_of(d * rows + i * half, half), half), :],
            lambda c: ss.at[c], lambda c: rs.at[c], me,
        )

    emb_g, hn_g, dh_g = gather_of(emb, es, er), gather_of(hn, hs, hr), gather_of(dh, ds_, dr)
    g1, g2 = g1_ref[...], g2_ref[...]

    ph("d_norm")

    def norm_rows(dev):
        def norm(i, _):
            at = pl.ds(pl.multiple_of(dev * rows + i * NB, NB), NB)
            x = emb[at, :].astype(F32)
            inv = lax.rsqrt(jnp.mean(x * x, axis=-1, keepdims=True) + NORM_EPS)
            a_all[at, :] = (x * inv * g1).astype(BF16)
            return 0

        lax.fori_loop(0, rows // NB, norm, 0, unroll=2)

    for load in loads[n_weight:]:
        load.wait()
    norm_rows(me)
    ph("b_barrier")
    pl.semaphore_wait(barrier, len(peers))
    for pair in pairs:
        pair.start()
    emb_g.forward_cross(wait=False)
    row_counts.start()
    norm_rows(px)
    norm_rows(py)

    ph("e_waitW")
    def weights_here(low, high):
        for load, pair in zip(loads[low:high], pairs[low:high]):
            load.wait()
            pair.wait_recv()

    weights_here(0, n_first)
    ph("f_fwd")
    acc[...] = jnp.zeros_like(acc)

    def forward(j, _):
        a = a_all[mine, :]
        p = dot_nn(a, wg[j]).astype(BF16)
        q = dot_nn(a, wu[j]).astype(BF16)
        p_own[j], q_own[j] = p, q
        p, q = p.astype(F32), q.astype(F32)
        u = (p * jax.nn.sigmoid(p) * q).astype(BF16)
        acc[...] += dot_nn(u, wd[j])
        return 0

    lax.fori_loop(0, n // 2, forward, 0, unroll=2)
    emb_g.forward_far()
    weights_here(n_first, n_weight)
    lax.fori_loop(n // 2, n, forward, 0, unroll=2)
    ph("g_hidden")

    def hidden(i, _):
        at = pl.ds(pl.multiple_of(i * NB, NB), NB)
        row = pl.ds(pl.multiple_of(me * rows + i * NB, NB), NB)
        h = (emb[row, :].astype(F32) + acc[at, :]).astype(BF16).astype(F32)
        h_wide[at, :] = h
        inv = lax.rsqrt(jnp.mean(h * h, axis=-1, keepdims=True) + NORM_EPS)
        hn[row, :] = (h * inv * g2).astype(BF16)
        return 0

    lax.fori_loop(0, rows // NB, hidden, 0, unroll=2)
    hn_g.start()
    ph("h_waitE")
    for pair in pairs[n_weight:]:
        pair.wait_recv()
    emb_g.wait_recv(7, 8)

    ph("i_logit")
    top[...] = jnp.full_like(top, -jnp.inf)

    def logit(v, _):
        val = dot_nt(hn[mine, :], emb[pl.ds(pl.multiple_of(v * wide, wide), wide), :])
        logits[v] = val
        m = top[...]
        for k in range(tiles):
            m = jnp.maximum(m, val[:, k * 128:(k + 1) * 128])
        top[...] = m
        return 0

    lax.fori_loop(0, n * rows // wide, logit, 0)
    row_counts.wait()
    ph("j_softmax")
    top[...] = jnp.max(top[...], axis=-1, keepdims=True) + jnp.zeros((rows, 128), F32)

    def counts(i, v, k):
        return cnt[pl.ds(i * (RB // 8), RB // 8), v * tiles + k].reshape(RB, 128)

    def total(i, _):
        at = pl.ds(pl.multiple_of(i * RB, RB), RB)
        m = top[at, :]

        def part(v, carry):
            s, c, pick = carry
            for k in range(tiles):
                cut = slice(k * 128, (k + 1) * 128)
                val, num = logits[v, at, cut], counts(i, v, k)
                ex = jnp.exp(val - m)
                logits[v, at, cut] = ex
                s, c, pick = s + ex, c + num, pick + num * val
            return s, c, pick

        zero = jnp.zeros((RB, 128), F32)
        sums[0, at, :], sums[1, at, :], sums[2, at, :] = lax.fori_loop(0, n * rows // wide, part, (zero, zero, zero))
        return 0

    lax.fori_loop(0, rows // RB, total, 0)
    s, c, pick = [jnp.sum(sums[k], axis=-1, keepdims=True) for k in range(3)]
    lse = top[:, 0:1] + jnp.log(s)
    lane = lax.broadcasted_iota(I32, (rows, 128), 1)
    stat_col[...] = jnp.where(lane == 0, lse, jnp.where(lane == 1, c * coef, jnp.where(lane == 2, c * lse - pick, 0.0)))
    sums[0] = c * coef / s + jnp.zeros((rows, 128), F32)

    def grad(i, _):
        at = pl.ds(pl.multiple_of(i * RB, RB), RB)
        scale = sums[0, at, :]

        def part(v, _):
            for k in range(tiles):
                cut = slice(k * 128, (k + 1) * 128)
                here = pl.ds(pl.multiple_of(v * wide + k * 128, 128), 128)
                dlog[at, here] = (logits[v, at, cut] * scale - counts(i, v, k) * coef).astype(BF16)
            return 0

        lax.fori_loop(0, n * rows // wide, part, 0)
        return 0

    lax.fori_loop(0, rows // RB, grad, 0)
    col_counts.start()
    stat[me] = jnp.transpose(stat_col[...])[0:8, :]
    ph("k_dhn")
    acc[...] = dot_nn(dlog[...], emb[...])
    stat_copies = [
        pltpu.make_async_remote_copy(
            src_ref=stat.at[me], dst_ref=stat.at[me], send_sem=st_s.at[k], recv_sem=st_r.at[k], device_id=(peer,), device_id_type=MESH
        )
        for k, peer in enumerate(peers)
    ]
    for copy in stat_copies:
        copy.start()
    ph("l_dhidden")

    def dhidden(i, _):
        at = pl.ds(pl.multiple_of(i * NB, NB), NB)
        h, scaled = h_wide[at, :], acc[at, :] * g2
        inv = lax.rsqrt(jnp.mean(h * h, axis=-1, keepdims=True) + NORM_EPS)
        grad = inv * (scaled - h * (inv * inv) * jnp.mean(scaled * h, axis=-1, keepdims=True))
        de_o[at, :] = grad
        dh[pl.ds(pl.multiple_of(me * rows + i * NB, NB), NB), :] = grad.astype(BF16)
        return 0

    lax.fori_loop(0, rows // NB, dhidden, 0, unroll=2)
    dh_g.start()

    ph("n_norm")
    for dev in [pd] + [flip(dev, 1) for dev in devs]:
        norm_rows(dev)
    ph("o_slice")

    def slice_forward(s, _):
        a = a_all[block(s), :]
        dlog[p_at(s)] = dot_nn(a, wg[me]).astype(BF16)
        q_all[s] = dot_nn(a, wu[me]).astype(BF16)
        return 0

    lax.fori_loop(0, n, slice_forward, 0, unroll=2)

    ph("m_hnnear")
    hn_g.wait_recv(0, 1)
    hn_g.forward_pair()

    ph("p_back")
    acc[...] = jnp.zeros_like(acc)

    def act_back(dact, p, q):
        sig = jax.nn.sigmoid(p)
        gated = p * sig
        dq = (dact * gated).astype(BF16)
        dp = (dact * q * sig * (1.0 + p * (1.0 - sig))).astype(BF16)
        return dp, dq, (gated * q).astype(BF16)

    def backward(j, _):
        dact = dot_nt(dh[mine, :], wd[j])
        dp, dq, _u = act_back(dact, p_own[j].astype(F32), q_own[j].astype(F32))
        acc[...] += dot_nt(dp, wg[j]) + dot_nt(dq, wu[j])
        return 0

    lax.fori_loop(0, n // 2, backward, 0, unroll=2)
    dh_g.forward_cross()
    lax.fori_loop(n // 2, n, backward, 0, unroll=2)
    ph("q_dinput")

    def dinput(i, _):
        at = pl.ds(pl.multiple_of(i * NB, NB), NB)
        x, scaled = emb[pl.ds(pl.multiple_of(me * rows + i * NB, NB), NB), :].astype(F32), acc[at, :] * g1
        inv = lax.rsqrt(jnp.mean(x * x, axis=-1, keepdims=True) + NORM_EPS)
        de_o[at, :] += inv * (scaled - x * (inv * inv) * jnp.mean(scaled * x, axis=-1, keepdims=True))
        return 0

    lax.fori_loop(0, rows // NB, dinput, 0, unroll=2)
    ph("r_stat")
    for copy in stat_copies:
        copy.wait_recv()
    col_counts.wait()

    def head(dev):
        low = dev - lax.rem(dev, 2)
        pair = pl.ds(pl.multiple_of(low * rows, 2 * rows), 2 * rows)
        for k in range(2 * rows // 256):
            source, cut = low + k * 256 // rows, slice(k * 256 % rows, k * 256 % rows + 256)
            lt = dot_nt(emb[mine, :], hn[pl.ds(pl.multiple_of(low * rows + k * 256, 256), 256), :])
            tile = low * (rows // 128) + 2 * k
            num = jnp.concatenate([cnt[:, tile].reshape(rows, 128), cnt[:, tile + 1].reshape(rows, 128)], axis=1)
            prob = jnp.exp(lt - stat[source, 0:1, cut]) * stat[source, 1:2, cut]
            dlog[:, k * 256:(k + 1) * 256] = (prob - num * coef).astype(BF16)
        de_o[...] += dot_nn(dlog[:, 0:2 * rows], hn[pair, :])

    dwg[...] = jnp.zeros_like(dwg)
    dwu[...] = jnp.zeros_like(dwu)
    dwd_o[...] = jnp.zeros_like(dwd_o)

    def act_grads(dev):
        dact = dot_nt(dh[block(dev), :], wd[me])
        return act_back(dact, dlog[p_at(dev)].astype(F32), q_all[dev].astype(F32))

    def weights(dev):
        dp, dq, u = act_grads(dev)
        dwd_o[...] += dot_tn(u, dh[block(dev), :])
        dwg[...] += dot_tn(a_all[block(dev), :], dp)
        dwu[...] += dot_tn(a_all[block(dev), :], dq)

    def exchange(k, peer, src, dst, row):
        return pltpu.make_async_remote_copy(
            src_ref=src.at[pl.ds(pl.multiple_of(peer * out_rows, out_rows), out_rows), :],
            dst_ref=dst.at[me],
            send_sem=ws.at[row, k], recv_sem=wr.at[row, k], device_id=(peer,), device_id_type=MESH,
        )

    swaps_g = [exchange(k, peer, dwg, got_g, 0) for k, peer in enumerate(peers)]
    swaps_u = [exchange(k, peer, dwu, got_u, 1) for k, peer in enumerate(peers)]

    ph("s_w01")
    dh_g.wait_recv(4)
    weights(me)
    weights(pc)
    ph("t_dhnear")
    dh_g.forward_pair()
    hn_g.forward_cross(wait=False)
    ph("u_w23")
    weights(px)
    weights(py)
    ph("v_w45")
    dh_g.wait_recv(5, 6)
    weights(flip(px, 1))
    weights(flip(py, 1))
    ph("w_heads")
    hn_g.wait_recv(4, 5, 6)
    head(me)
    head(px)
    head(py)
    ph("x_dhfar")
    dh_g.forward_far()
    ph("y_late")
    late = [pd, flip(pd, 1)]
    for k, kinds in ((0, ()), (1, (7, 8))):
        dh_g.wait_recv(*kinds)
        dev = late[k]
        dlog[p_at(dev)], q_all[dev], dlog[p_at(n + k)] = act_grads(dev)
        dwg[...] += dot_tn(a_all[block(dev), :], dlog[p_at(dev)])
    for swap in swaps_g:
        swap.start()
    for dev in late:
        dwu[...] += dot_tn(a_all[block(dev), :], q_all[dev])
    for swap in swaps_u:
        swap.start()
    keep = pl.ds(pl.multiple_of(me * out_rows, out_rows), out_rows)
    outs = [pltpu.make_async_copy(dwg.at[keep, :], got_g.at[me], out_sem.at[0]), pltpu.make_async_copy(dwu.at[keep, :], got_u.at[me], out_sem.at[1])]
    for out in outs:
        out.start()
    for k, dev in enumerate(late):
        dwd_o[...] += dot_tn(dlog[p_at(n + k)], dh[block(dev), :])
    ph("z_hnfar")
    hn_g.forward_far()
    outs.append(pltpu.make_async_copy(dwd_o, dwd_out, out_sem.at[2]))
    outs[-1].start()
    hn_g.wait_recv(7, 8)
    ph("za_head")
    head(pd)
    outs.append(pltpu.make_async_copy(de_o, de_out, out_sem.at[3]))
    outs[-1].start()
    total_loss = jnp.zeros((1, rows), F32)
    for s in range(n):
        total_loss = total_loss + stat[s, 2:3, :]
    loss_o[...] = jnp.sum(total_loss, axis=-1, keepdims=True) * coef + jnp.zeros((1, 128), F32)
    ph("zd_waits")
    for copy in stat_copies:
        copy.wait_send()
    emb_g.wait_sends(2, 3, 7, 8)
    hn_g.wait_sends()
    dh_g.wait_sends()
    for pair in pairs:
        pair.wait_send()
    for out in outs:
        out.wait()
    for swap in swaps_g + swaps_u:
        swap.wait()
    ph()


def run_step(coef, embs, gus, downs, crow, ccol, g1, g2):
    n = N_DEV
    rows, width = embs[0].shape
    fs = gus[0].shape[2]
    out_rows = width // n
    any_spec = pl.BlockSpec(memory_space=pl.ANY)
    vmem = pl.BlockSpec(memory_space=pltpu.VMEM)
    dma = pltpu.SemaphoreType.DMA
    return pl.pallas_call(
        step_kernel,
        out_shape=(
            jax.ShapeDtypeStruct((1, 128), F32),
            jax.ShapeDtypeStruct((rows, width), F32),
            jax.ShapeDtypeStruct((n, out_rows, fs), F32),
            jax.ShapeDtypeStruct((n, out_rows, fs), F32),
            jax.ShapeDtypeStruct((fs, width), F32),
        ),
        in_specs=[pl.BlockSpec(memory_space=pltpu.SMEM)] + [any_spec] * 13 + [vmem] * 2,
        out_specs=(vmem,) + (any_spec,) * 4,
        scratch_shapes=[
            pltpu.VMEM((rows, width), F32),
            pltpu.VMEM((fs, width), F32),
            pltpu.VMEM((n * rows, width), BF16),
            pltpu.VMEM((n, width, fs), BF16),
            pltpu.VMEM((n, width, fs), BF16),
            pltpu.VMEM((n, fs, width), BF16),
            pltpu.VMEM((rows // 8, n * rows // 128, 8, 128), F32),
            pltpu.VMEM((n * rows, width), BF16),
            pltpu.VMEM((n * rows, width), BF16),
            pltpu.VMEM((n * rows, width), BF16),
            pltpu.VMEM((n, rows, fs), BF16),
            pltpu.VMEM((n, rows, fs), BF16),
            pltpu.VMEM((n, rows, fs), BF16),
            pltpu.VMEM((n // 2, rows, 2 * rows), F32),
            pltpu.VMEM((rows, n * rows), BF16),
            pltpu.VMEM((rows, width), F32),
            pltpu.VMEM((rows, width), F32),
            pltpu.VMEM((n, 8, rows), F32),
            pltpu.VMEM((rows, 128), F32),
            pltpu.VMEM((rows, 128), F32),
            pltpu.VMEM((3, rows, 128), F32),
            pltpu.VMEM((width, fs), F32),
            pltpu.VMEM((width, fs), F32),
            dma((25,)), dma((23,)), dma((23,)), dma((11,)), dma((11,)), dma((11,)), dma((11,)), dma((11,)), dma((11,)), dma((n - 1,)), dma((n - 1,)), dma((2, n - 1)), dma((2, n - 1)), dma((4,)),
        ],
        compiler_params=pltpu.CompilerParams(collective_id=1, has_side_effects=True, vmem_limit_bytes=VMEM_MAX),
        name="step",
    )(coef, *embs, *gus, *downs, crow, ccol, g1, g2)


def solution(mesh):
    def device_step(tok_ids, tok_labels, loss_mask, emb, g1, g2, w_gate, w_up, w_down):
        n = N_DEV
        rows, width = emb.shape
        vocab = rows * n
        n_tok = tok_ids.shape[0]
        me = lax.axis_index("fsdp")

        def send(bit):
            pairs = [(d, d ^ bit) for d in range(n)]
            return lambda val: lax.ppermute(val, "fsdp", pairs)

        along_x, along_y = send(2), send(4)
        gu = slice_weights(w_gate, w_up)
        gus, downs = [[val, along_x(val), along_y(val)] for val in (gu, w_down)]

        live = loss_mask != 0
        by_id = lax.sort(jnp.where(live, tok_ids * 65536 + tok_labels, vocab * 65536), is_stable=False)
        by_label = lax.sort(jnp.where(live, tok_labels * 65536 + tok_ids, vocab * 65536), is_stable=False)
        tok = [part.reshape(n_tok // 128, 128) for part in (by_id >> 16, by_id & 65535, by_label >> 16, by_label & 65535)]
        tok = gather_tokens(jnp.concatenate(tok).astype(jnp.int16))
        tok, gus[2], downs[1], emb_later = lax.optimization_barrier((tok, gus[2], downs[1], emb))
        embs = [emb, along_x(emb_later), along_y(emb_later)]
        gus.append(along_x(gus[2]))
        downs.append(along_y(downs[1]))
        ids, labels, labels2, ids2 = [tok[:, k * (n_tok // 128):(k + 1) * (n_tok // 128)].astype(I32) for k in range(4)]
        crow, ccol = count([(ids, labels), (labels2, ids2)], me * rows, rows, vocab)
        n_live = jnp.sum(ids < vocab).astype(F32)
        coef = (1.0 / n_live).reshape(1, 1)
        loss, *grads = run_step(coef, embs, gus, downs, crow, ccol, g1.reshape(1, width), g2.reshape(1, width))
        return (loss[0, 0], *finish(*grads))

    row_spec = P("fsdp", None)
    tok_spec = P("fsdp")
    return jax.shard_map(device_step, mesh=mesh, in_specs=(tok_spec, tok_spec, tok_spec, row_spec, P(), P(), row_spec, row_spec, row_spec), out_specs=(P(), row_spec, row_spec, row_spec, row_spec), check_vma=False)
```

```python
import functools

import jax
import jax.numpy as jnp
from jax import lax
from jax.experimental import pallas as pl
from jax.experimental.pallas import tpu as pltpu
from jax.sharding import PartitionSpec as P


NORM_EPS = 1e-6
N_DEV = 8
F32, BF16, I32 = jnp.float32, jnp.bfloat16, jnp.int32
MESH = pl.DeviceIdType.MESH
VMEM_MAX = 66_000_000
VMEM_ALL = 67_000_000


class Phases:
    def __init__(self):
        self.now = None

    def __call__(self, name=None):
        if self.now is not None:
            self.now.__exit__(None, None, None)
        self.now = jax.named_scope(name) if name else None
        if self.now is not None:
            self.now.__enter__()


def dot_nn(a, b):
    return jnp.dot(a, b, preferred_element_type=F32)


def dot_nt(a, b):
    return lax.dot_general(a, b, (((1,), (1,)), ((), ())), preferred_element_type=F32)


def dot_tn(a, b):
    return lax.dot_general(a, b, (((0,), (0,)), ((), ())), preferred_element_type=F32)


def flip(me, bit):
    return me + bit - 2 * bit * lax.rem(me // bit, 2)


def barrier_with(peers):
    sem = pltpu.get_barrier_semaphore()
    for peer in peers:
        pl.semaphore_signal(sem, inc=1, device_id=(peer,), device_id_type=MESH)
    pl.semaphore_wait(sem, len(peers))


class Gather:
    def __init__(self, slot, half, send_sem, recv_sem, me):
        self.slot, self.half, self.ss, self.rs, self.me = slot, half, send_sem, recv_sem, me
        self.pc, self.px, self.py = flip(me, 1), flip(me, 2), flip(me, 4)
        self.pd = flip(self.px, 4)

    def copy(self, kind, src, dst, peer):
        return pltpu.make_async_remote_copy(
            src_ref=src, dst_ref=dst, send_sem=self.ss(kind), recv_sem=self.rs(kind), device_id=(peer,), device_id_type=MESH
        )

    def describe(self, kind):
        me, px, py, pd, pc = self.me, self.px, self.py, self.pd, self.pc
        if kind in (0, 9):
            return self.copy(kind, self.half(me, kind // 9), self.half(me, kind // 9), px)
        if kind in (1, 10):
            return self.copy(kind, self.half(me, 1 - kind // 10), self.half(me, 1 - kind // 10), py)
        if kind == 2:
            return self.copy(2, self.half(px, 0), self.half(px, 0), py)
        if kind == 3:
            return self.copy(3, self.half(py, 1), self.half(py, 1), px)
        if kind == 4:
            return self.copy(4, self.slot(me), self.slot(me), pc)
        if kind == 5:
            return self.copy(5, self.slot(px), self.slot(px), pc)
        if kind == 6:
            return self.copy(6, self.slot(py), self.slot(py), pc)
        return self.copy(kind, self.half(pd, kind - 7), self.half(pd, kind - 7), pc)

    def start(self):
        for kind in (0, 1, 9, 10, 4):
            self.describe(kind).start()

    def forward_pair(self):
        for kind in (0, 1):
            self.describe(9 + kind).wait_recv()
            self.describe(5 + kind).start()

    def forward_cross(self, wait=True):
        for kind in (0, 1):
            if wait:
                self.describe(kind).wait_recv()
            self.describe(2 + kind).start()

    def forward_far(self):
        self.describe(2).wait_recv()
        self.describe(7).start()
        self.describe(3).wait_recv()
        self.describe(8).start()

    def wait_recv(self, *kinds):
        for kind in kinds:
            self.describe(kind).wait_recv()

    def wait_sends(self, *kinds):
        for kind in kinds or range(11):
            self.describe(kind).wait_send()


def slice_kernel(gate, up, out):
    n, _, fs = out.shape
    rows = gate.shape[0]
    for k in range(n):
        out[k, 0:rows, :] = gate[:, k * fs:(k + 1) * fs]
        out[k, rows:2 * rows, :] = up[:, k * fs:(k + 1) * fs]


def slice_weights(gate, up):
    rows, width = gate.shape
    return pl.pallas_call(
        slice_kernel,
        out_shape=jax.ShapeDtypeStruct((N_DEV, 2 * rows, width // N_DEV), gate.dtype),
        cost_estimate=pl.CostEstimate(flops=1_000_000, bytes_accessed=1_000_000, transcendentals=0),
        name="slices",
    )(gate, up)


def token_kernel(tok, tok_o, send_sem, recv_sem, local_sem):
    me = lax.axis_index("fsdp")
    n = tok_o.shape[0]
    peers = [lax.rem(me + k, n) for k in range(1, n)]
    barrier_with(peers)
    copies = [
        pltpu.make_async_remote_copy(
            src_ref=tok, dst_ref=tok_o.at[me], send_sem=send_sem.at[k], recv_sem=recv_sem.at[k], device_id=(peer,), device_id_type=MESH
        )
        for k, peer in enumerate(peers)
    ]
    local = pltpu.make_async_copy(tok, tok_o.at[me], local_sem)
    for copy in copies:
        copy.start()
    local.start()
    for copy in copies:
        copy.wait()
    local.wait()


def gather_tokens(tok):
    dma = pltpu.SemaphoreType.DMA
    return pl.pallas_call(
        token_kernel,
        out_shape=jax.ShapeDtypeStruct((N_DEV,) + tok.shape, tok.dtype),
        in_specs=[pl.BlockSpec(memory_space=pltpu.VMEM)],
        out_specs=pl.BlockSpec(memory_space=pl.ANY),
        scratch_shapes=[dma((N_DEV - 1,)), dma((N_DEV - 1,)), dma],
        compiler_params=pltpu.CompilerParams(collective_id=0, has_side_effects=True, vmem_limit_bytes=VMEM_ALL),
        cost_estimate=pl.CostEstimate(flops=5_000_000_000, bytes_accessed=1_000_000, transcendentals=0),
        name="tokens",
    )(tok)


def count_kernel(bounds, keys_a, keys_b, out_a, out_b, list_a, list_b, acc_a, acc_b, in_sem, out_sem):
    n_src = N_DEV
    per = list_a.shape[0] // n_src
    size = acc_a.shape[0]
    BLK = 256
    unroll = 8
    jobs = [(keys_a, out_a, list_a, acc_a), (keys_b, out_b, list_b, acc_b)]
    stores = [pltpu.make_async_copy(acc, out, out_sem.at[k]) for k, (_k, out, _h, acc) in enumerate(jobs)]
    PART = 1024

    def segment(which, src):
        begin = bounds[which * 2 * n_src + src] + src * per
        return begin, bounds[which * 2 * n_src + n_src + src] + src * per

    def fetch(src, run):
        for which, (keys, _o, held, _a) in enumerate(jobs):
            begin, end = segment(which, src)

            def one(t, _):
                at = pl.ds(pl.multiple_of(t * PART, PART), PART)
                run(pltpu.make_async_copy(keys.at[at], held.at[at], in_sem.at[which]))
                return 0

            lax.fori_loop(lax.shift_right_logical(begin, 10), jnp.where(begin < end, lax.shift_right_logical(end + PART - 1, 10), 0), one, 0)

    lax.fori_loop(0, n_src, lambda src, _: (fetch(src, lambda copy: copy.start()), 0)[1], 0)
    lanes = lax.broadcasted_iota(I32, (1, 128), 1)

    def clear(i, _):
        acc_a[pl.ds(i * BLK, BLK), :] = jnp.zeros((BLK, 128), F32)
        acc_b[pl.ds(i * BLK, BLK), :] = jnp.zeros((BLK, 128), F32)
        return 0

    lax.fori_loop(0, size // BLK, clear, 0)
    lax.fori_loop(0, n_src, lambda src, _: (fetch(src, lambda copy: copy.wait()), 0)[1], 0)

    def group(streams, whole):
        done = []
        for held, acc, pos, end in streams:
            places, vals, delta = [], [], None
            for k in range(unroll):
                key = held[pos + k] if whole else held[jnp.minimum(pos + k, end - 1)]
                places.append(key >> 7)
                spread = jnp.full((1, 128), key, I32)
                here = jnp.where(lanes == (spread & 127), 1.0 if whole else jnp.where(pos + k < end, 1.0, 0.0), 0.0)
                delta = here if k == 0 else here + jnp.where((spread ^ before) < 128, delta, 0.0)
                before = spread
                vals.append(acc[pl.ds(places[k], 1), :] + delta)
            done.append((acc, places, vals))
        for acc, places, vals in done:
            for place, val in zip(places, vals):
                acc[pl.ds(place, 1), :] = val

    def source(src, _):
        ranges = []
        for which, (_k, _o, held, acc) in enumerate(jobs):
            begin, end = segment(which, src)
            ranges.append((held, acc, begin, end, lax.shift_right_logical(end - begin, 3)))
        both = jnp.minimum(ranges[0][4], ranges[1][4])

        def step(i, _):
            group([(held, acc, begin + i * unroll, end) for held, acc, begin, end, _n in ranges], True)
            return 0

        lax.fori_loop(0, both, step, 0)
        for held, acc, begin, end, n_whole in ranges:
            def rest(i, _):
                group([(held, acc, begin + i * unroll, end)], True)
                return 0

            lax.fori_loop(both, n_whole, rest, 0)

            @pl.when(begin + n_whole * unroll < end)
            def _():
                group([(held, acc, begin + n_whole * unroll, end)], False)

        return 0

    lax.fori_loop(0, n_src, source, 0)
    for store in stores:
        store.start()
    for store in stores:
        store.wait()


def count(pairs, first, rows, cols):
    bounds, keys, tiles = [], [], cols // 128
    for major, minor in pairs:
        bounds.append(jnp.sum(major < first, axis=(1, 2), dtype=I32))
        bounds.append(jnp.sum(major < first + rows, axis=(1, 2), dtype=I32))
        row = major - first
        keys.append(((((row >> 3) * tiles + (minor >> 7)) * 8 + (row & 7)) * 128 + (minor & 127)).reshape(-1))
    any_spec = pl.BlockSpec(memory_space=pl.ANY)
    tall = (rows * cols // 128, 128)
    outs = pl.pallas_call(
        count_kernel,
        out_shape=(jax.ShapeDtypeStruct(tall, F32),) * 2,
        in_specs=[pl.BlockSpec(memory_space=pltpu.SMEM), any_spec, any_spec],
        out_specs=(any_spec,) * 2,
        scratch_shapes=[pltpu.SMEM(keys[0].shape, I32)] * 2 + [pltpu.VMEM(tall, F32)] * 2 + [pltpu.SemaphoreType.DMA((2,))] * 2,
        compiler_params=pltpu.CompilerParams(vmem_limit_bytes=VMEM_ALL),
        cost_estimate=pl.CostEstimate(flops=30_000_000_000, bytes_accessed=16_000_000, transcendentals=0),
        name="count",
    )(jnp.concatenate(bounds), *keys)
    return [out.reshape(rows // 8, tiles, 8, 128) for out in outs]


def finish_kernel(de, got_g, got_u, dwd, de_o, dwg_o, dwu_o, dwd_o, de_v, g_v, u_v, dwd_v, wg_v, wu_v, in_sem, out_sem):
    n, _, fs = g_v.shape
    ins = [pltpu.make_async_copy(src, dst, in_sem.at[k]) for k, (src, dst) in enumerate([(got_g, g_v), (got_u, u_v), (de, de_v), (dwd, dwd_v)])]
    outs = [pltpu.make_async_copy(src, dst, out_sem.at[k]) for k, (src, dst) in enumerate([(wg_v, dwg_o), (wu_v, dwu_o), (de_v, de_o), (dwd_v, dwd_o)])]
    for copy in ins:
        copy.start()
    for which, (src, dst) in enumerate([(g_v, wg_v), (u_v, wu_v)]):
        ins[which].wait()
        for k in range(n):
            dst[:, k * fs:(k + 1) * fs] = src[k]
        if which == 1:
            outs[0].start()
    for which in (2, 3):
        ins[which].wait()
        outs[which].start()
    outs[1].start()
    for copy in outs:
        copy.wait()


def finish(de, got_g, got_u, dwd):
    n, out_rows, fs = got_g.shape
    wide = jax.ShapeDtypeStruct((out_rows, n * fs), F32)
    any_spec = pl.BlockSpec(memory_space=pl.ANY)
    held = [pltpu.VMEM(val.shape, F32) for val in (de, got_g, got_u, dwd, wide, wide)]
    return pl.pallas_call(
        finish_kernel,
        out_shape=(jax.ShapeDtypeStruct(de.shape, F32), wide, wide, jax.ShapeDtypeStruct(dwd.shape, F32)),
        in_specs=[any_spec] * 4,
        out_specs=(any_spec,) * 4,
        scratch_shapes=held + [pltpu.SemaphoreType.DMA((4,)), pltpu.SemaphoreType.DMA((4,))],
        compiler_params=pltpu.CompilerParams(vmem_limit_bytes=VMEM_ALL),
        name="finish",
    )(de, got_g, got_u, dwd)


def step_kernel(
    coef_ref, emb_me, emb_x, emb_y, gu_me, gu_x, gu_y, gu_d, wd_me, wd_x, wd_y, wd_d, crow_hbm, ccol_hbm, g1_ref, g2_ref,
    loss_o, de_out, got_g, got_u, dwd_out,
    de_o, dwd_o, emb, wg, wu, wd, cnt, hn, dh, a_all, p_own, q_own, q_all, logits, dlog, h_wide, acc, stat, stat_col, top, sums,
    dwg, dwu, load_sem, pair_s, pair_r, es, er, hs, hr, ds_, dr, st_s, st_r, ws, wr, out_sem,
):
    me = lax.axis_index("fsdp")
    n = wg.shape[0]
    rows, width = h_wide.shape
    fs = wg.shape[2]
    out_rows = got_g.shape[1]
    coef = coef_ref[0, 0]
    ph = Phases()
    ph("a_start")
    NB = 128
    RB = 64
    wide = logits.shape[2]
    tiles = wide // 128
    peers = [lax.rem(me + k, n) for k in range(1, n)]

    def block(dev):
        return pl.ds(pl.multiple_of(dev * rows, rows), rows)

    def p_at(s):
        return (slice(None), pl.ds(pl.multiple_of(2 * rows + s * 256, 256), fs))

    mine = block(me)
    pc, px, py = flip(me, 1), flip(me, 2), flip(me, 4)
    pd = flip(px, 4)
    devs = [me, px, py, pd]
    parts = []
    for dev, down in zip(devs, [wd_me, wd_x, wd_y, wd_d]):
        parts.append((down, wd.at[dev]))
    for wave in range(2):
        part = pl.ds(wave * (n // 2), n // 2)
        for dev, gu in zip(devs, [gu_me, gu_x, gu_y, gu_d]):
            at = pl.ds(dev * out_rows, out_rows)
            parts.append((gu.at[part, 0:out_rows, :], wg.at[part, at, :]))
            parts.append((gu.at[part, out_rows:2 * out_rows, :], wu.at[part, at, :]))
    n_first = len(parts) - 2 * len(devs)
    n_weight = len(parts)
    for dev, part in zip(devs, [emb_me, emb_x, emb_y]):
        parts.append((part, emb.at[block(dev), :]))
    loads = [pltpu.make_async_copy(src, dst, load_sem.at[k]) for k, (src, dst) in enumerate(parts)]
    pairs = [
        pltpu.make_async_remote_copy(
            src_ref=src, dst_ref=dst, send_sem=pair_s.at[k], recv_sem=pair_r.at[k], device_id=(pc,), device_id_type=MESH
        )
        for k, (src, dst) in enumerate(parts)
    ]
    row_counts = pltpu.make_async_copy(crow_hbm, cnt, load_sem.at[len(parts)])
    col_counts = pltpu.make_async_copy(ccol_hbm, cnt, load_sem.at[len(parts) + 1])

    barrier = pltpu.get_barrier_semaphore()
    for peer in peers:
        pl.semaphore_signal(barrier, inc=1, device_id=(peer,), device_id_type=MESH)
    for load in loads[n_weight:] + loads[:n_weight]:
        load.start()
    def gather_of(buf, ss, rs):
        half = rows // 2
        return Gather(
            lambda d: buf.at[block(d), :],
            lambda d, i: buf.at[pl.ds(pl.multiple_of(d * rows + i * half, half), half), :],
            lambda c: ss.at[c], lambda c: rs.at[c], me,
        )

    emb_g, hn_g, dh_g = gather_of(emb, es, er), gather_of(hn, hs, hr), gather_of(dh, ds_, dr)
    g1, g2 = g1_ref[...], g2_ref[...]

    ph("d_norm")

    def norm_rows(dev):
        def norm(i, _):
            at = pl.ds(pl.multiple_of(dev * rows + i * NB, NB), NB)
            x = emb[at, :].astype(F32)
            inv = lax.rsqrt(jnp.mean(x * x, axis=-1, keepdims=True) + NORM_EPS)
            a_all[at, :] = (x * inv * g1).astype(BF16)
            return 0

        lax.fori_loop(0, rows // NB, norm, 0, unroll=2)

    for load in loads[n_weight:]:
        load.wait()
    norm_rows(me)
    ph("b_barrier")
    pl.semaphore_wait(barrier, len(peers))
    for pair in pairs:
        pair.start()
    emb_g.forward_cross(wait=False)
    row_counts.start()
    norm_rows(px)
    norm_rows(py)

    ph("e_waitW")
    def weights_here(low, high):
        for load, pair in zip(loads[low:high], pairs[low:high]):
            load.wait()
            pair.wait_recv()

    weights_here(0, n_first)
    ph("f_fwd")
    acc[...] = jnp.zeros_like(acc)

    def forward(j, _):
        a = a_all[mine, :]
        p = dot_nn(a, wg[j]).astype(BF16)
        q = dot_nn(a, wu[j]).astype(BF16)
        p_own[j], q_own[j] = p, q
        p, q = p.astype(F32), q.astype(F32)
        u = (p * jax.nn.sigmoid(p) * q).astype(BF16)
        acc[...] += dot_nn(u, wd[j])
        return 0

    lax.fori_loop(0, n // 2, forward, 0, unroll=2)
    emb_g.forward_far()
    weights_here(n_first, n_weight)
    lax.fori_loop(n // 2, n, forward, 0, unroll=2)
    ph("g_hidden")

    def hidden(i, _):
        at = pl.ds(pl.multiple_of(i * NB, NB), NB)
        row = pl.ds(pl.multiple_of(me * rows + i * NB, NB), NB)
        h = (emb[row, :].astype(F32) + acc[at, :]).astype(BF16).astype(F32)
        h_wide[at, :] = h
        inv = lax.rsqrt(jnp.mean(h * h, axis=-1, keepdims=True) + NORM_EPS)
        hn[row, :] = (h * inv * g2).astype(BF16)
        return 0

    lax.fori_loop(0, rows // NB, hidden, 0, unroll=2)
    hn_g.start()
    ph("h_waitE")
    for pair in pairs[n_weight:]:
        pair.wait_recv()
    emb_g.wait_recv(7, 8)

    ph("i_logit")
    top[...] = jnp.full_like(top, -jnp.inf)

    def logit(v, _):
        val = dot_nt(hn[mine, :], emb[pl.ds(pl.multiple_of(v * wide, wide), wide), :])
        logits[v] = val
        m = top[...]
        for k in range(tiles):
            m = jnp.maximum(m, val[:, k * 128:(k + 1) * 128])
        top[...] = m
        return 0

    lax.fori_loop(0, n * rows // wide, logit, 0)
    row_counts.wait()
    ph("j_softmax")
    top[...] = jnp.max(top[...], axis=-1, keepdims=True) + jnp.zeros((rows, 128), F32)

    def counts(i, v, k):
        return cnt[pl.ds(i * (RB // 8), RB // 8), v * tiles + k].reshape(RB, 128)

    def total(i, _):
        at = pl.ds(pl.multiple_of(i * RB, RB), RB)
        m = top[at, :]

        def part(v, carry):
            s, c, pick = carry
            for k in range(tiles):
                cut = slice(k * 128, (k + 1) * 128)
                val, num = logits[v, at, cut], counts(i, v, k)
                ex = jnp.exp(val - m)
                logits[v, at, cut] = ex
                s, c, pick = s + ex, c + num, pick + num * val
            return s, c, pick

        zero = jnp.zeros((RB, 128), F32)
        sums[0, at, :], sums[1, at, :], sums[2, at, :] = lax.fori_loop(0, n * rows // wide, part, (zero, zero, zero))
        return 0

    lax.fori_loop(0, rows // RB, total, 0)
    s, c, pick = [jnp.sum(sums[k], axis=-1, keepdims=True) for k in range(3)]
    lse = top[:, 0:1] + jnp.log(s)
    lane = lax.broadcasted_iota(I32, (rows, 128), 1)
    stat_col[...] = jnp.where(lane == 0, lse, jnp.where(lane == 1, c * coef, jnp.where(lane == 2, c * lse - pick, 0.0)))
    sums[0] = c * coef / s + jnp.zeros((rows, 128), F32)

    def grad(i, _):
        at = pl.ds(pl.multiple_of(i * RB, RB), RB)
        scale = sums[0, at, :]

        def part(v, _):
            for k in range(tiles):
                cut = slice(k * 128, (k + 1) * 128)
                here = pl.ds(pl.multiple_of(v * wide + k * 128, 128), 128)
                dlog[at, here] = (logits[v, at, cut] * scale - counts(i, v, k) * coef).astype(BF16)
            return 0

        lax.fori_loop(0, n * rows // wide, part, 0)
        return 0

    lax.fori_loop(0, rows // RB, grad, 0)
    col_counts.start()
    stat[me] = jnp.transpose(stat_col[...])[0:8, :]
    ph("k_dhn")
    acc[...] = dot_nn(dlog[...], emb[...])
    stat_copies = [
        pltpu.make_async_remote_copy(
            src_ref=stat.at[me], dst_ref=stat.at[me], send_sem=st_s.at[k], recv_sem=st_r.at[k], device_id=(peer,), device_id_type=MESH
        )
        for k, peer in enumerate(peers)
    ]
    for copy in stat_copies:
        copy.start()
    ph("l_dhidden")

    def dhidden(i, _):
        at = pl.ds(pl.multiple_of(i * NB, NB), NB)
        h, scaled = h_wide[at, :], acc[at, :] * g2
        inv = lax.rsqrt(jnp.mean(h * h, axis=-1, keepdims=True) + NORM_EPS)
        grad = inv * (scaled - h * (inv * inv) * jnp.mean(scaled * h, axis=-1, keepdims=True))
        de_o[at, :] = grad
        dh[pl.ds(pl.multiple_of(me * rows + i * NB, NB), NB), :] = grad.astype(BF16)
        return 0

    lax.fori_loop(0, rows // NB, dhidden, 0, unroll=2)
    dh_g.start()

    ph("n_norm")
    for dev in [pd] + [flip(dev, 1) for dev in devs]:
        norm_rows(dev)
    ph("o_slice")

    def slice_forward(s, _):
        a = a_all[block(s), :]
        dlog[p_at(s)] = dot_nn(a, wg[me]).astype(BF16)
        q_all[s] = dot_nn(a, wu[me]).astype(BF16)
        return 0

    lax.fori_loop(0, n, slice_forward, 0, unroll=2)

    ph("m_hnnear")
    hn_g.wait_recv(0, 1)
    hn_g.forward_pair()

    ph("p_back")
    acc[...] = jnp.zeros_like(acc)

    def act_back(dact, p, q):
        sig = jax.nn.sigmoid(p)
        gated = p * sig
        dq = (dact * gated).astype(BF16)
        dp = (dact * q * sig * (1.0 + p * (1.0 - sig))).astype(BF16)
        return dp, dq, (gated * q).astype(BF16)

    def backward(j, _):
        dact = dot_nt(dh[mine, :], wd[j])
        dp, dq, _u = act_back(dact, p_own[j].astype(F32), q_own[j].astype(F32))
        acc[...] += dot_nt(dp, wg[j]) + dot_nt(dq, wu[j])
        return 0

    lax.fori_loop(0, n, backward, 0, unroll=2)
    dh_g.forward_cross()
    ph("q_dinput")

    def dinput(i, _):
        at = pl.ds(pl.multiple_of(i * NB, NB), NB)
        x, scaled = emb[pl.ds(pl.multiple_of(me * rows + i * NB, NB), NB), :].astype(F32), acc[at, :] * g1
        inv = lax.rsqrt(jnp.mean(x * x, axis=-1, keepdims=True) + NORM_EPS)
        de_o[at, :] += inv * (scaled - x * (inv * inv) * jnp.mean(scaled * x, axis=-1, keepdims=True))
        return 0

    lax.fori_loop(0, rows // NB, dinput, 0, unroll=2)
    ph("r_stat")
    for copy in stat_copies:
        copy.wait_recv()
    col_counts.wait()

    def head(dev):
        low = dev - lax.rem(dev, 2)
        pair = pl.ds(pl.multiple_of(low * rows, 2 * rows), 2 * rows)
        for k in range(2 * rows // 256):
            source, cut = low + k * 256 // rows, slice(k * 256 % rows, k * 256 % rows + 256)
            lt = dot_nt(emb[mine, :], hn[pl.ds(pl.multiple_of(low * rows + k * 256, 256), 256), :])
            tile = low * (rows // 128) + 2 * k
            num = jnp.concatenate([cnt[:, tile].reshape(rows, 128), cnt[:, tile + 1].reshape(rows, 128)], axis=1)
            prob = jnp.exp(lt - stat[source, 0:1, cut]) * stat[source, 1:2, cut]
            dlog[:, k * 256:(k + 1) * 256] = (prob - num * coef).astype(BF16)
        de_o[...] += dot_nn(dlog[:, 0:2 * rows], hn[pair, :])

    dwg[...] = jnp.zeros_like(dwg)
    dwu[...] = jnp.zeros_like(dwu)
    dwd_o[...] = jnp.zeros_like(dwd_o)

    def act_grads(dev):
        dact = dot_nt(dh[block(dev), :], wd[me])
        return act_back(dact, dlog[p_at(dev)].astype(F32), q_all[dev].astype(F32))

    def weights(dev):
        dp, dq, u = act_grads(dev)
        dwd_o[...] += dot_tn(u, dh[block(dev), :])
        dwg[...] += dot_tn(a_all[block(dev), :], dp)
        dwu[...] += dot_tn(a_all[block(dev), :], dq)

    def exchange(k, peer, src, dst, row):
        return pltpu.make_async_remote_copy(
            src_ref=src.at[pl.ds(pl.multiple_of(peer * out_rows, out_rows), out_rows), :],
            dst_ref=dst.at[me],
            send_sem=ws.at[row, k], recv_sem=wr.at[row, k], device_id=(peer,), device_id_type=MESH,
        )

    swaps_g = [exchange(k, peer, dwg, got_g, 0) for k, peer in enumerate(peers)]
    swaps_u = [exchange(k, peer, dwu, got_u, 1) for k, peer in enumerate(peers)]

    ph("s_w01")
    dh_g.wait_recv(4)
    weights(me)
    weights(pc)
    ph("t_dhnear")
    dh_g.forward_pair()
    hn_g.forward_cross(wait=False)
    ph("u_w23")
    weights(px)
    weights(py)
    ph("v_w45")
    dh_g.wait_recv(5, 6)
    weights(flip(px, 1))
    weights(flip(py, 1))
    ph("w_heads")
    hn_g.wait_recv(4, 5)
    head(me)
    head(px)
    ph("x_dhfar")
    dh_g.forward_far()
    ph("y_late")
    late = [pd, flip(pd, 1)]
    for k, kinds in ((0, ()), (1, (7, 8))):
        dh_g.wait_recv(*kinds)
        dev = late[k]
        dlog[p_at(dev)], q_all[dev], dlog[p_at(n + k)] = act_grads(dev)
        dwg[...] += dot_tn(a_all[block(dev), :], dlog[p_at(dev)])
    for swap in swaps_g:
        swap.start()
    for dev in late:
        dwu[...] += dot_tn(a_all[block(dev), :], q_all[dev])
    for swap in swaps_u:
        swap.start()
    keep = pl.ds(pl.multiple_of(me * out_rows, out_rows), out_rows)
    outs = [pltpu.make_async_copy(dwg.at[keep, :], got_g.at[me], out_sem.at[0]), pltpu.make_async_copy(dwu.at[keep, :], got_u.at[me], out_sem.at[1])]
    for out in outs:
        out.start()
    for k, dev in enumerate(late):
        dwd_o[...] += dot_tn(dlog[p_at(n + k)], dh[block(dev), :])
    ph("z_hnfar")
    hn_g.wait_recv(6)
    head(py)
    hn_g.forward_far()
    outs.append(pltpu.make_async_copy(dwd_o, dwd_out, out_sem.at[2]))
    outs[-1].start()
    hn_g.wait_recv(7, 8)
    ph("za_head")
    head(pd)
    outs.append(pltpu.make_async_copy(de_o, de_out, out_sem.at[3]))
    outs[-1].start()
    total_loss = jnp.zeros((1, rows), F32)
    for s in range(n):
        total_loss = total_loss + stat[s, 2:3, :]
    loss_o[...] = jnp.sum(total_loss, axis=-1, keepdims=True) * coef + jnp.zeros((1, 128), F32)
    ph("zd_waits")
    for copy in stat_copies:
        copy.wait_send()
    emb_g.wait_sends(2, 3, 7, 8)
    hn_g.wait_sends()
    dh_g.wait_sends()
    for pair in pairs:
        pair.wait_send()
    for out in outs:
        out.wait()
    for swap in swaps_g + swaps_u:
        swap.wait()
    ph()


def run_step(coef, embs, gus, downs, crow, ccol, g1, g2):
    n = N_DEV
    rows, width = embs[0].shape
    fs = gus[0].shape[2]
    out_rows = width // n
    any_spec = pl.BlockSpec(memory_space=pl.ANY)
    vmem = pl.BlockSpec(memory_space=pltpu.VMEM)
    dma = pltpu.SemaphoreType.DMA
    return pl.pallas_call(
        step_kernel,
        out_shape=(
            jax.ShapeDtypeStruct((1, 128), F32),
            jax.ShapeDtypeStruct((rows, width), F32),
            jax.ShapeDtypeStruct((n, out_rows, fs), F32),
            jax.ShapeDtypeStruct((n, out_rows, fs), F32),
            jax.ShapeDtypeStruct((fs, width), F32),
        ),
        in_specs=[pl.BlockSpec(memory_space=pltpu.SMEM)] + [any_spec] * 13 + [vmem] * 2,
        out_specs=(vmem,) + (any_spec,) * 4,
        scratch_shapes=[
            pltpu.VMEM((rows, width), F32),
            pltpu.VMEM((fs, width), F32),
            pltpu.VMEM((n * rows, width), BF16),
            pltpu.VMEM((n, width, fs), BF16),
            pltpu.VMEM((n, width, fs), BF16),
            pltpu.VMEM((n, fs, width), BF16),
            pltpu.VMEM((rows // 8, n * rows // 128, 8, 128), F32),
            pltpu.VMEM((n * rows, width), BF16),
            pltpu.VMEM((n * rows, width), BF16),
            pltpu.VMEM((n * rows, width), BF16),
            pltpu.VMEM((n, rows, fs), BF16),
            pltpu.VMEM((n, rows, fs), BF16),
            pltpu.VMEM((n, rows, fs), BF16),
            pltpu.VMEM((n // 2, rows, 2 * rows), F32),
            pltpu.VMEM((rows, n * rows), BF16),
            pltpu.VMEM((rows, width), F32),
            pltpu.VMEM((rows, width), F32),
            pltpu.VMEM((n, 8, rows), F32),
            pltpu.VMEM((rows, 128), F32),
            pltpu.VMEM((rows, 128), F32),
            pltpu.VMEM((3, rows, 128), F32),
            pltpu.VMEM((width, fs), F32),
            pltpu.VMEM((width, fs), F32),
            dma((25,)), dma((23,)), dma((23,)), dma((11,)), dma((11,)), dma((11,)), dma((11,)), dma((11,)), dma((11,)), dma((n - 1,)), dma((n - 1,)), dma((2, n - 1)), dma((2, n - 1)), dma((4,)),
        ],
        compiler_params=pltpu.CompilerParams(collective_id=1, has_side_effects=True, vmem_limit_bytes=VMEM_MAX),
        name="step",
    )(coef, *embs, *gus, *downs, crow, ccol, g1, g2)


def solution(mesh):
    def device_step(tok_ids, tok_labels, loss_mask, emb, g1, g2, w_gate, w_up, w_down):
        n = N_DEV
        rows, width = emb.shape
        vocab = rows * n
        n_tok = tok_ids.shape[0]
        me = lax.axis_index("fsdp")

        def send(bit):
            pairs = [(d, d ^ bit) for d in range(n)]
            return lambda val: lax.ppermute(val, "fsdp", pairs)

        along_x, along_y = send(2), send(4)
        gu = slice_weights(w_gate, w_up)
        gus, downs = [[val, along_x(val), along_y(val)] for val in (gu, w_down)]

        live = loss_mask != 0
        by_id = lax.sort(jnp.where(live, tok_ids * 65536 + tok_labels, vocab * 65536), is_stable=False)
        by_label = lax.sort(jnp.where(live, tok_labels * 65536 + tok_ids, vocab * 65536), is_stable=False)
        tok = [part.reshape(n_tok // 128, 128) for part in (by_id >> 16, by_id & 65535, by_label >> 16, by_label & 65535)]
        tok = gather_tokens(jnp.concatenate(tok).astype(jnp.int16))
        tok, gus[2], downs[1], emb_later = lax.optimization_barrier((tok, gus[2], downs[1], emb))
        embs = [emb, along_x(emb_later), along_y(emb_later)]
        gus.append(along_x(gus[2]))
        downs.append(along_y(downs[1]))
        ids, labels, labels2, ids2 = [tok[:, k * (n_tok // 128):(k + 1) * (n_tok // 128)].astype(I32) for k in range(4)]
        crow, ccol = count([(ids, labels), (labels2, ids2)], me * rows, rows, vocab)
        n_live = jnp.sum(ids < vocab).astype(F32)
        coef = (1.0 / n_live).reshape(1, 1)
        loss, *grads = run_step(coef, embs, gus, downs, crow, ccol, g1.reshape(1, width), g2.reshape(1, width))
        return (loss[0, 0], *finish(*grads))

    row_spec = P("fsdp", None)
    tok_spec = P("fsdp")
    return jax.shard_map(device_step, mesh=mesh, in_specs=(tok_spec, tok_spec, tok_spec, row_spec, P(), P(), row_spec, row_spec, row_spec), out_specs=(P(), row_spec, row_spec, row_spec, row_spec), check_vma=False)
```

```python
import functools

import jax
import jax.numpy as jnp
from jax import lax
from jax.experimental import pallas as pl
from jax.experimental.pallas import tpu as pltpu
from jax.sharding import PartitionSpec as P


NORM_EPS = 1e-6
N_DEV = 8
F32, BF16, I32 = jnp.float32, jnp.bfloat16, jnp.int32
MESH = pl.DeviceIdType.MESH
VMEM_MAX = 66_000_000
VMEM_ALL = 67_000_000


class Phases:
    def __init__(self):
        self.now = None

    def __call__(self, name=None):
        if self.now is not None:
            self.now.__exit__(None, None, None)
        self.now = jax.named_scope(name) if name else None
        if self.now is not None:
            self.now.__enter__()


def dot_nn(a, b):
    return jnp.dot(a, b, preferred_element_type=F32)


def dot_nt(a, b):
    return lax.dot_general(a, b, (((1,), (1,)), ((), ())), preferred_element_type=F32)


def dot_tn(a, b):
    return lax.dot_general(a, b, (((0,), (0,)), ((), ())), preferred_element_type=F32)


def flip(me, bit):
    return me + bit - 2 * bit * lax.rem(me // bit, 2)


def barrier_with(peers):
    sem = pltpu.get_barrier_semaphore()
    for peer in peers:
        pl.semaphore_signal(sem, inc=1, device_id=(peer,), device_id_type=MESH)
    pl.semaphore_wait(sem, len(peers))


class Gather:
    def __init__(self, slot, half, send_sem, recv_sem, me):
        self.slot, self.half, self.ss, self.rs, self.me = slot, half, send_sem, recv_sem, me
        self.pc, self.px, self.py = flip(me, 1), flip(me, 2), flip(me, 4)
        self.pd = flip(self.px, 4)

    def copy(self, kind, src, dst, peer):
        return pltpu.make_async_remote_copy(
            src_ref=src, dst_ref=dst, send_sem=self.ss(kind), recv_sem=self.rs(kind), device_id=(peer,), device_id_type=MESH
        )

    def describe(self, kind):
        me, px, py, pd, pc = self.me, self.px, self.py, self.pd, self.pc
        if kind in (0, 9):
            return self.copy(kind, self.half(me, kind // 9), self.half(me, kind // 9), px)
        if kind in (1, 10):
            return self.copy(kind, self.half(me, 1 - kind // 10), self.half(me, 1 - kind // 10), py)
        if kind == 2:
            return self.copy(2, self.half(px, 0), self.half(px, 0), py)
        if kind == 3:
            return self.copy(3, self.half(py, 1), self.half(py, 1), px)
        if kind == 4:
            return self.copy(4, self.slot(me), self.slot(me), pc)
        if kind == 5:
            return self.copy(5, self.slot(px), self.slot(px), pc)
        if kind == 6:
            return self.copy(6, self.slot(py), self.slot(py), pc)
        return self.copy(kind, self.half(pd, kind - 7), self.half(pd, kind - 7), pc)

    def start(self):
        for kind in (0, 1, 9, 10, 4):
            self.describe(kind).start()

    def forward_pair(self):
        for kind in (0, 1):
            self.describe(9 + kind).wait_recv()
            self.describe(5 + kind).start()

    def forward_cross(self, wait=True):
        for kind in (0, 1):
            if wait:
                self.describe(kind).wait_recv()
            self.describe(2 + kind).start()

    def forward_far(self):
        self.describe(2).wait_recv()
        self.describe(7).start()
        self.describe(3).wait_recv()
        self.describe(8).start()

    def wait_recv(self, *kinds):
        for kind in kinds:
            self.describe(kind).wait_recv()

    def wait_sends(self, *kinds):
        for kind in kinds or range(11):
            self.describe(kind).wait_send()


def slice_kernel(gate, up, out):
    n, _, fs = out.shape
    rows = gate.shape[0]
    for k in range(n):
        out[k, 0:rows, :] = gate[:, k * fs:(k + 1) * fs]
        out[k, rows:2 * rows, :] = up[:, k * fs:(k + 1) * fs]


def slice_weights(gate, up):
    rows, width = gate.shape
    return pl.pallas_call(
        slice_kernel,
        out_shape=jax.ShapeDtypeStruct((N_DEV, 2 * rows, width // N_DEV), gate.dtype),
        cost_estimate=pl.CostEstimate(flops=1_000_000, bytes_accessed=1_000_000, transcendentals=0),
        name="slices",
    )(gate, up)


def token_kernel(tok, tok_o, send_sem, recv_sem, local_sem):
    me = lax.axis_index("fsdp")
    n = tok_o.shape[0]
    peers = [lax.rem(me + k, n) for k in range(1, n)]
    barrier_with(peers)
    copies = [
        pltpu.make_async_remote_copy(
            src_ref=tok, dst_ref=tok_o.at[me], send_sem=send_sem.at[k], recv_sem=recv_sem.at[k], device_id=(peer,), device_id_type=MESH
        )
        for k, peer in enumerate(peers)
    ]
    local = pltpu.make_async_copy(tok, tok_o.at[me], local_sem)
    for copy in copies:
        copy.start()
    local.start()
    for copy in copies:
        copy.wait()
    local.wait()


def gather_tokens(tok):
    dma = pltpu.SemaphoreType.DMA
    return pl.pallas_call(
        token_kernel,
        out_shape=jax.ShapeDtypeStruct((N_DEV,) + tok.shape, tok.dtype),
        in_specs=[pl.BlockSpec(memory_space=pltpu.VMEM)],
        out_specs=pl.BlockSpec(memory_space=pl.ANY),
        scratch_shapes=[dma((N_DEV - 1,)), dma((N_DEV - 1,)), dma],
        compiler_params=pltpu.CompilerParams(collective_id=0, has_side_effects=True, vmem_limit_bytes=VMEM_ALL),
        cost_estimate=pl.CostEstimate(flops=5_000_000_000, bytes_accessed=1_000_000, transcendentals=0),
        name="tokens",
    )(tok)


def count_kernel(bounds, keys_a, keys_b, out_a, out_b, list_a, list_b, acc_a, acc_b, in_sem, out_sem):
    n_src = N_DEV
    per = list_a.shape[0] // n_src
    size = acc_a.shape[0]
    BLK = 256
    unroll = 8
    jobs = [(keys_a, out_a, list_a, acc_a), (keys_b, out_b, list_b, acc_b)]
    stores = [pltpu.make_async_copy(acc, out, out_sem.at[k]) for k, (_k, out, _h, acc) in enumerate(jobs)]
    PART = 1024

    def segment(which, src):
        both = bounds[which * n_src + src]
        return (both & 65535) + src * per, lax.shift_right_logical(both, 16) + src * per

    def fetch(src, run):
        for which, (keys, _o, held, _a) in enumerate(jobs):
            begin, end = segment(which, src)

            def one(t, _):
                at = pl.ds(pl.multiple_of(t * PART, PART), PART)
                run(pltpu.make_async_copy(keys.at[at], held.at[at], in_sem.at[which]))
                return 0

            lax.fori_loop(lax.shift_right_logical(begin, 10), jnp.where(begin < end, lax.shift_right_logical(end + PART - 1, 10), 0), one, 0)

    lax.fori_loop(0, n_src, lambda src, _: (fetch(src, lambda copy: copy.start()), 0)[1], 0)
    lanes = lax.broadcasted_iota(I32, (1, 128), 1)

    def clear(i, _):
        acc_a[pl.ds(i * BLK, BLK), :] = jnp.zeros((BLK, 128), F32)
        acc_b[pl.ds(i * BLK, BLK), :] = jnp.zeros((BLK, 128), F32)
        return 0

    lax.fori_loop(0, size // BLK, clear, 0)
    lax.fori_loop(0, n_src, lambda src, _: (fetch(src, lambda copy: copy.wait()), 0)[1], 0)

    def group(streams, whole):
        done = []
        for held, acc, pos, end in streams:
            places, vals, delta = [], [], None
            for k in range(unroll):
                key = held[pos + k] if whole else held[jnp.minimum(pos + k, end - 1)]
                places.append(key >> 7)
                spread = jnp.full((1, 128), key, I32)
                here = jnp.where(lanes == (spread & 127), 1.0 if whole else jnp.where(pos + k < end, 1.0, 0.0), 0.0)
                delta = here if k == 0 else here + jnp.where((spread ^ before) < 128, delta, 0.0)
                before = spread
                vals.append(acc[pl.ds(places[k], 1), :] + delta)
            done.append((acc, places, vals))
        for acc, places, vals in done:
            for place, val in zip(places, vals):
                acc[pl.ds(place, 1), :] = val

    def source(src, _):
        ranges = []
        for which, (_k, _o, held, acc) in enumerate(jobs):
            begin, end = segment(which, src)
            ranges.append((held, acc, begin, end, lax.shift_right_logical(end - begin, 3)))
        both = jnp.minimum(ranges[0][4], ranges[1][4])

        def step(i, _):
            group([(held, acc, begin + i * unroll, end) for held, acc, begin, end, _n in ranges], True)
            return 0

        lax.fori_loop(0, both, step, 0)
        for held, acc, begin, end, n_whole in ranges:
            def rest(i, _):
                group([(held, acc, begin + i * unroll, end)], True)
                return 0

            lax.fori_loop(both, n_whole, rest, 0)

            @pl.when(begin + n_whole * unroll < end)
            def _():
                group([(held, acc, begin + n_whole * unroll, end)], False)

        return 0

    lax.fori_loop(0, n_src, source, 0)
    for store in stores:
        store.start()
    for store in stores:
        store.wait()


def count(pairs, first, rows, cols):
    bounds, keys, tiles = [], [], cols // 128
    for major, minor in pairs:
        bounds.append(jnp.sum(jnp.where(major < first, 1, 0) + jnp.where(major < first + rows, 65536, 0), axis=(1, 2), dtype=I32))
        row = major - first
        keys.append(((((row >> 3) * tiles + (minor >> 7)) * 8 + (row & 7)) * 128 + (minor & 127)).reshape(-1))
    any_spec = pl.BlockSpec(memory_space=pl.ANY)
    tall = (rows * cols // 128, 128)
    outs = pl.pallas_call(
        count_kernel,
        out_shape=(jax.ShapeDtypeStruct(tall, F32),) * 2,
        in_specs=[pl.BlockSpec(memory_space=pltpu.SMEM), any_spec, any_spec],
        out_specs=(any_spec,) * 2,
        scratch_shapes=[pltpu.SMEM(keys[0].shape, I32)] * 2 + [pltpu.VMEM(tall, F32)] * 2 + [pltpu.SemaphoreType.DMA((2,))] * 2,
        compiler_params=pltpu.CompilerParams(vmem_limit_bytes=VMEM_ALL),
        cost_estimate=pl.CostEstimate(flops=30_000_000_000, bytes_accessed=16_000_000, transcendentals=0),
        name="count",
    )(jnp.concatenate(bounds), *keys)
    return [out.reshape(rows // 8, tiles, 8, 128) for out in outs]


def finish_kernel(de, got_g, got_u, dwd, de_o, dwg_o, dwu_o, dwd_o, de_v, g_v, u_v, dwd_v, wg_v, wu_v, in_sem, out_sem):
    n, _, fs = g_v.shape
    ins = [pltpu.make_async_copy(src, dst, in_sem.at[k]) for k, (src, dst) in enumerate([(got_g, g_v), (got_u, u_v), (de, de_v), (dwd, dwd_v)])]
    outs = [pltpu.make_async_copy(src, dst, out_sem.at[k]) for k, (src, dst) in enumerate([(wg_v, dwg_o), (wu_v, dwu_o), (de_v, de_o), (dwd_v, dwd_o)])]
    for copy in ins:
        copy.start()
    for which, (src, dst) in enumerate([(g_v, wg_v), (u_v, wu_v)]):
        ins[which].wait()
        for k in range(n):
            dst[:, k * fs:(k + 1) * fs] = src[k]
        if which == 1:
            outs[0].start()
    for which in (2, 3):
        ins[which].wait()
        outs[which].start()
    outs[1].start()
    for copy in outs:
        copy.wait()


def finish(de, got_g, got_u, dwd):
    n, out_rows, fs = got_g.shape
    wide = jax.ShapeDtypeStruct((out_rows, n * fs), F32)
    any_spec = pl.BlockSpec(memory_space=pl.ANY)
    held = [pltpu.VMEM(val.shape, F32) for val in (de, got_g, got_u, dwd, wide, wide)]
    return pl.pallas_call(
        finish_kernel,
        out_shape=(jax.ShapeDtypeStruct(de.shape, F32), wide, wide, jax.ShapeDtypeStruct(dwd.shape, F32)),
        in_specs=[any_spec] * 4,
        out_specs=(any_spec,) * 4,
        scratch_shapes=held + [pltpu.SemaphoreType.DMA((4,)), pltpu.SemaphoreType.DMA((4,))],
        compiler_params=pltpu.CompilerParams(vmem_limit_bytes=VMEM_ALL),
        name="finish",
    )(de, got_g, got_u, dwd)


def step_kernel(
    coef_ref, emb_me, emb_x, emb_y, gu_me, gu_x, gu_y, gu_d, wd_me, wd_x, wd_y, wd_d, crow_hbm, ccol_hbm, g1_ref, g2_ref,
    loss_o, de_out, got_g, got_u, dwd_out,
    de_o, dwd_o, emb, wg, wu, wd, cnt, hn, dh, a_all, p_own, q_own, q_all, logits, dlog, h_wide, acc, stat, stat_col, top, sums,
    dwg, dwu, load_sem, pair_s, pair_r, es, er, hs, hr, ds_, dr, st_s, st_r, ws, wr, out_sem,
):
    me = lax.axis_index("fsdp")
    n = wg.shape[0]
    rows, width = h_wide.shape
    fs = wg.shape[2]
    out_rows = got_g.shape[1]
    coef = coef_ref[0, 0]
    ph = Phases()
    ph("a_start")
    NB = 128
    RB = 64
    wide = logits.shape[2]
    tiles = wide // 128
    peers = [lax.rem(me + k, n) for k in range(1, n)]

    def block(dev):
        return pl.ds(pl.multiple_of(dev * rows, rows), rows)

    def p_at(s):
        return (slice(None), pl.ds(pl.multiple_of(2 * rows + s * 256, 256), fs))

    mine = block(me)
    pc, px, py = flip(me, 1), flip(me, 2), flip(me, 4)
    pd = flip(px, 4)
    devs = [me, px, py, pd]
    parts = []
    waves = []
    for dev, down in zip(devs, [wd_me, wd_x, wd_y, wd_d]):
        low = dev - lax.rem(dev, 2)
        part = pl.ds(low, 2)
        parts.append((down, wd.at[dev]))
        for owner, gu in zip(devs, [gu_me, gu_x, gu_y, gu_d]):
            at = pl.ds(owner * out_rows, out_rows)
            parts.append((gu.at[part, 0:out_rows, :], wg.at[part, at, :]))
            parts.append((gu.at[part, out_rows:2 * out_rows, :], wu.at[part, at, :]))
        waves.append((low, len(parts)))
    n_weight = len(parts)
    for dev, part in zip(devs, [emb_me, emb_x, emb_y]):
        parts.append((part, emb.at[block(dev), :]))
    loads = [pltpu.make_async_copy(src, dst, load_sem.at[k]) for k, (src, dst) in enumerate(parts)]
    pairs = [
        pltpu.make_async_remote_copy(
            src_ref=src, dst_ref=dst, send_sem=pair_s.at[k], recv_sem=pair_r.at[k], device_id=(pc,), device_id_type=MESH
        )
        for k, (src, dst) in enumerate(parts)
    ]
    row_counts = pltpu.make_async_copy(crow_hbm, cnt, load_sem.at[len(parts)])
    col_counts = pltpu.make_async_copy(ccol_hbm, cnt, load_sem.at[len(parts) + 1])

    barrier = pltpu.get_barrier_semaphore()
    for peer in peers:
        pl.semaphore_signal(barrier, inc=1, device_id=(peer,), device_id_type=MESH)
    for load in loads[n_weight:] + loads[:n_weight]:
        load.start()
    def gather_of(buf, ss, rs):
        half = rows // 2
        return Gather(
            lambda d: buf.at[block(d), :],
            lambda d, i: buf.at[pl.ds(pl.multiple_of(d * rows + i * half, half), half), :],
            lambda c: ss.at[c], lambda c: rs.at[c], me,
        )

    emb_g, hn_g, dh_g = gather_of(emb, es, er), gather_of(hn, hs, hr), gather_of(dh, ds_, dr)
    g1, g2 = g1_ref[...], g2_ref[...]

    ph("d_norm")

    def norm_rows(dev):
        def norm(i, _):
            at = pl.ds(pl.multiple_of(dev * rows + i * NB, NB), NB)
            x = emb[at, :].astype(F32)
            inv = lax.rsqrt(jnp.mean(x * x, axis=-1, keepdims=True) + NORM_EPS)
            a_all[at, :] = (x * inv * g1).astype(BF16)
            return 0

        lax.fori_loop(0, rows // NB, norm, 0, unroll=2)

    for load in loads[n_weight:]:
        load.wait()
    norm_rows(me)
    ph("b_barrier")
    pl.semaphore_wait(barrier, len(peers))
    for pair in pairs:
        pair.start()
    emb_g.forward_cross(wait=False)
    row_counts.start()
    norm_rows(px)
    norm_rows(py)

    ph("e_waitW")
    def weights_here(first, last):
        for load, pair in zip(loads[first:last], pairs[first:last]):
            load.wait()
            pair.wait_recv()

    acc[...] = jnp.zeros_like(acc)

    def forward(j, _):
        a = a_all[mine, :]
        p = dot_nn(a, wg[j]).astype(BF16)
        q = dot_nn(a, wu[j]).astype(BF16)
        p_own[j], q_own[j] = p, q
        p, q = p.astype(F32), q.astype(F32)
        u = (p * jax.nn.sigmoid(p) * q).astype(BF16)
        acc[...] += dot_nn(u, wd[j])
        return 0

    first = 0
    for k, (low, last) in enumerate(waves):
        weights_here(first, last)
        first = last
        forward(low, 0)
        forward(low + 1, 0)
        if k == 2:
            emb_g.forward_far()
    ph("g_hidden")

    def hidden(i, _):
        at = pl.ds(pl.multiple_of(i * NB, NB), NB)
        row = pl.ds(pl.multiple_of(me * rows + i * NB, NB), NB)
        h = (emb[row, :].astype(F32) + acc[at, :]).astype(BF16).astype(F32)
        h_wide[at, :] = h
        inv = lax.rsqrt(jnp.mean(h * h, axis=-1, keepdims=True) + NORM_EPS)
        hn[row, :] = (h * inv * g2).astype(BF16)
        return 0

    lax.fori_loop(0, rows // NB, hidden, 0, unroll=2)
    hn_g.start()
    ph("h_waitE")
    for pair in pairs[n_weight:]:
        pair.wait_recv()
    emb_g.wait_recv(7, 8)

    ph("i_logit")
    top[...] = jnp.full_like(top, -jnp.inf)

    def logit(v, _):
        val = dot_nt(hn[mine, :], emb[pl.ds(pl.multiple_of(v * wide, wide), wide), :])
        logits[v] = val
        m = top[...]
        for k in range(tiles):
            m = jnp.maximum(m, val[:, k * 128:(k + 1) * 128])
        top[...] = m
        return 0

    lax.fori_loop(0, n * rows // wide, logit, 0)
    row_counts.wait()
    ph("j_softmax")
    top[...] = jnp.max(top[...], axis=-1, keepdims=True) + jnp.zeros((rows, 128), F32)

    def counts(i, v, k):
        return cnt[pl.ds(i * (RB // 8), RB // 8), v * tiles + k].reshape(RB, 128)

    def total(i, _):
        at = pl.ds(pl.multiple_of(i * RB, RB), RB)
        m = top[at, :]

        def part(v, carry):
            s, c, pick = carry
            for k in range(tiles):
                cut = slice(k * 128, (k + 1) * 128)
                val, num = logits[v, at, cut], counts(i, v, k)
                ex = jnp.exp(val - m)
                logits[v, at, cut] = ex
                s, c, pick = s + ex, c + num, pick + num * val
            return s, c, pick

        zero = jnp.zeros((RB, 128), F32)
        sums[0, at, :], sums[1, at, :], sums[2, at, :] = lax.fori_loop(0, n * rows // wide, part, (zero, zero, zero))
        return 0

    lax.fori_loop(0, rows // RB, total, 0)
    s, c, pick = [jnp.sum(sums[k], axis=-1, keepdims=True) for k in range(3)]
    lse = top[:, 0:1] + jnp.log(s)
    lane = lax.broadcasted_iota(I32, (rows, 128), 1)
    stat_col[...] = jnp.where(lane == 0, lse, jnp.where(lane == 1, c * coef, jnp.where(lane == 2, c * lse - pick, 0.0)))
    sums[0] = c * coef / s + jnp.zeros((rows, 128), F32)

    def grad(i, _):
        at = pl.ds(pl.multiple_of(i * RB, RB), RB)
        scale = sums[0, at, :]

        def part(v, _):
            for k in range(tiles):
                cut = slice(k * 128, (k + 1) * 128)
                here = pl.ds(pl.multiple_of(v * wide + k * 128, 128), 128)
                dlog[at, here] = (logits[v, at, cut] * scale - counts(i, v, k) * coef).astype(BF16)
            return 0

        lax.fori_loop(0, n * rows // wide, part, 0)
        return 0

    lax.fori_loop(0, rows // RB, grad, 0)
    col_counts.start()
    stat[me] = jnp.transpose(stat_col[...])[0:8, :]
    ph("k_dhn")
    acc[...] = dot_nn(dlog[...], emb[...])
    stat_copies = [
        pltpu.make_async_remote_copy(
            src_ref=stat.at[me], dst_ref=stat.at[me], send_sem=st_s.at[k], recv_sem=st_r.at[k], device_id=(peer,), device_id_type=MESH
        )
        for k, peer in enumerate(peers)
    ]
    for copy in stat_copies:
        copy.start()
    ph("l_dhidden")

    def dhidden(i, _):
        at = pl.ds(pl.multiple_of(i * NB, NB), NB)
        h, scaled = h_wide[at, :], acc[at, :] * g2
        inv = lax.rsqrt(jnp.mean(h * h, axis=-1, keepdims=True) + NORM_EPS)
        grad = inv * (scaled - h * (inv * inv) * jnp.mean(scaled * h, axis=-1, keepdims=True))
        de_o[at, :] = grad
        dh[pl.ds(pl.multiple_of(me * rows + i * NB, NB), NB), :] = grad.astype(BF16)
        return 0

    lax.fori_loop(0, rows // NB, dhidden, 0, unroll=2)
    dh_g.start()

    ph("n_norm")
    for dev in [pd] + [flip(dev, 1) for dev in devs]:
        norm_rows(dev)
    ph("o_slice")

    def slice_forward(s, _):
        a = a_all[block(s), :]
        dlog[p_at(s)] = dot_nn(a, wg[me]).astype(BF16)
        q_all[s] = dot_nn(a, wu[me]).astype(BF16)
        return 0

    lax.fori_loop(0, n, slice_forward, 0, unroll=2)

    ph("m_hnnear")
    hn_g.wait_recv(0, 1)
    hn_g.forward_pair()

    ph("p_back")
    acc[...] = jnp.zeros_like(acc)

    def act_back(dact, p, q):
        sig = jax.nn.sigmoid(p)
        gated = p * sig
        dq = (dact * gated).astype(BF16)
        dp = (dact * q * sig * (1.0 + p * (1.0 - sig))).astype(BF16)
        return dp, dq, (gated * q).astype(BF16)

    def backward(j, _):
        dact = dot_nt(dh[mine, :], wd[j])
        dp, dq, _u = act_back(dact, p_own[j].astype(F32), q_own[j].astype(F32))
        acc[...] += dot_nt(dp, wg[j]) + dot_nt(dq, wu[j])
        return 0

    lax.fori_loop(0, n, backward, 0, unroll=2)
    dh_g.forward_cross()
    ph("q_dinput")

    def dinput(i, _):
        at = pl.ds(pl.multiple_of(i * NB, NB), NB)
        x, scaled = emb[pl.ds(pl.multiple_of(me * rows + i * NB, NB), NB), :].astype(F32), acc[at, :] * g1
        inv = lax.rsqrt(jnp.mean(x * x, axis=-1, keepdims=True) + NORM_EPS)
        de_o[at, :] += inv * (scaled - x * (inv * inv) * jnp.mean(scaled * x, axis=-1, keepdims=True))
        return 0

    lax.fori_loop(0, rows // NB, dinput, 0, unroll=2)
    ph("r_stat")
    for copy in stat_copies:
        copy.wait_recv()
    col_counts.wait()

    def head(dev):
        low = dev - lax.rem(dev, 2)
        pair = pl.ds(pl.multiple_of(low * rows, 2 * rows), 2 * rows)
        for k in range(2 * rows // 256):
            source, cut = low + k * 256 // rows, slice(k * 256 % rows, k * 256 % rows + 256)
            lt = dot_nt(emb[mine, :], hn[pl.ds(pl.multiple_of(low * rows + k * 256, 256), 256), :])
            tile = low * (rows // 128) + 2 * k
            num = jnp.concatenate([cnt[:, tile].reshape(rows, 128), cnt[:, tile + 1].reshape(rows, 128)], axis=1)
            prob = jnp.exp(lt - stat[source, 0:1, cut]) * stat[source, 1:2, cut]
            dlog[:, k * 256:(k + 1) * 256] = (prob - num * coef).astype(BF16)
        de_o[...] += dot_nn(dlog[:, 0:2 * rows], hn[pair, :])

    dwg[...] = jnp.zeros_like(dwg)
    dwu[...] = jnp.zeros_like(dwu)
    dwd_o[...] = jnp.zeros_like(dwd_o)

    def act_grads(dev):
        dact = dot_nt(dh[block(dev), :], wd[me])
        return act_back(dact, dlog[p_at(dev)].astype(F32), q_all[dev].astype(F32))

    def weights(dev):
        dp, dq, u = act_grads(dev)
        dwd_o[...] += dot_tn(u, dh[block(dev), :])
        dwg[...] += dot_tn(a_all[block(dev), :], dp)
        dwu[...] += dot_tn(a_all[block(dev), :], dq)

    def exchange(k, peer, src, dst, row):
        return pltpu.make_async_remote_copy(
            src_ref=src.at[pl.ds(pl.multiple_of(peer * out_rows, out_rows), out_rows), :],
            dst_ref=dst.at[me],
            send_sem=ws.at[row, k], recv_sem=wr.at[row, k], device_id=(peer,), device_id_type=MESH,
        )

    swaps_g = [exchange(k, peer, dwg, got_g, 0) for k, peer in enumerate(peers)]
    swaps_u = [exchange(k, peer, dwu, got_u, 1) for k, peer in enumerate(peers)]

    ph("s_w01")
    dh_g.wait_recv(4)
    weights(me)
    weights(pc)
    ph("t_dhnear")
    dh_g.forward_pair()
    hn_g.forward_cross(wait=False)
    ph("u_w23")
    weights(px)
    weights(py)
    ph("v_w45")
    dh_g.wait_recv(5, 6)
    weights(flip(px, 1))
    weights(flip(py, 1))
    ph("w_heads")
    hn_g.wait_recv(4, 5)
    head(me)
    head(px)
    ph("x_dhfar")
    dh_g.forward_far()
    ph("y_late")
    late = [pd, flip(pd, 1)]
    for k, kinds in ((0, ()), (1, (7, 8))):
        dh_g.wait_recv(*kinds)
        dev = late[k]
        dlog[p_at(dev)], q_all[dev], dlog[p_at(n + k)] = act_grads(dev)
        dwg[...] += dot_tn(a_all[block(dev), :], dlog[p_at(dev)])
    for swap in swaps_g:
        swap.start()
    for dev in late:
        dwu[...] += dot_tn(a_all[block(dev), :], q_all[dev])
    for swap in swaps_u:
        swap.start()
    keep = pl.ds(pl.multiple_of(me * out_rows, out_rows), out_rows)
    outs = [pltpu.make_async_copy(dwg.at[keep, :], got_g.at[me], out_sem.at[0]), pltpu.make_async_copy(dwu.at[keep, :], got_u.at[me], out_sem.at[1])]
    for out in outs:
        out.start()
    for k, dev in enumerate(late):
        dwd_o[...] += dot_tn(dlog[p_at(n + k)], dh[block(dev), :])
    ph("z_hnfar")
    hn_g.wait_recv(6)
    head(py)
    hn_g.forward_far()
    outs.append(pltpu.make_async_copy(dwd_o, dwd_out, out_sem.at[2]))
    outs[-1].start()
    hn_g.wait_recv(7, 8)
    ph("za_head")
    head(pd)
    outs.append(pltpu.make_async_copy(de_o, de_out, out_sem.at[3]))
    outs[-1].start()
    total_loss = jnp.zeros((1, rows), F32)
    for s in range(n):
        total_loss = total_loss + stat[s, 2:3, :]
    loss_o[...] = jnp.sum(total_loss, axis=-1, keepdims=True) * coef + jnp.zeros((1, 128), F32)
    ph("zd_waits")
    for copy in stat_copies:
        copy.wait_send()
    emb_g.wait_sends(2, 3, 7, 8)
    hn_g.wait_sends()
    dh_g.wait_sends()
    for pair in pairs:
        pair.wait_send()
    for out in outs:
        out.wait()
    for swap in swaps_g + swaps_u:
        swap.wait()
    ph()


def run_step(coef, embs, gus, downs, crow, ccol, g1, g2):
    n = N_DEV
    rows, width = embs[0].shape
    fs = gus[0].shape[2]
    out_rows = width // n
    any_spec = pl.BlockSpec(memory_space=pl.ANY)
    vmem = pl.BlockSpec(memory_space=pltpu.VMEM)
    dma = pltpu.SemaphoreType.DMA
    return pl.pallas_call(
        step_kernel,
        out_shape=(
            jax.ShapeDtypeStruct((1, 128), F32),
            jax.ShapeDtypeStruct((rows, width), F32),
            jax.ShapeDtypeStruct((n, out_rows, fs), F32),
            jax.ShapeDtypeStruct((n, out_rows, fs), F32),
            jax.ShapeDtypeStruct((fs, width), F32),
        ),
        in_specs=[pl.BlockSpec(memory_space=pltpu.SMEM)] + [any_spec] * 13 + [vmem] * 2,
        out_specs=(vmem,) + (any_spec,) * 4,
        scratch_shapes=[
            pltpu.VMEM((rows, width), F32),
            pltpu.VMEM((fs, width), F32),
            pltpu.VMEM((n * rows, width), BF16),
            pltpu.VMEM((n, width, fs), BF16),
            pltpu.VMEM((n, width, fs), BF16),
            pltpu.VMEM((n, fs, width), BF16),
            pltpu.VMEM((rows // 8, n * rows // 128, 8, 128), F32),
            pltpu.VMEM((n * rows, width), BF16),
            pltpu.VMEM((n * rows, width), BF16),
            pltpu.VMEM((n * rows, width), BF16),
            pltpu.VMEM((n, rows, fs), BF16),
            pltpu.VMEM((n, rows, fs), BF16),
            pltpu.VMEM((n, rows, fs), BF16),
            pltpu.VMEM((n // 2, rows, 2 * rows), F32),
            pltpu.VMEM((rows, n * rows), BF16),
            pltpu.VMEM((rows, width), F32),
            pltpu.VMEM((rows, width), F32),
            pltpu.VMEM((n, 8, rows), F32),
            pltpu.VMEM((rows, 128), F32),
            pltpu.VMEM((rows, 128), F32),
            pltpu.VMEM((3, rows, 128), F32),
            pltpu.VMEM((width, fs), F32),
            pltpu.VMEM((width, fs), F32),
            dma((41,)), dma((39,)), dma((39,)), dma((11,)), dma((11,)), dma((11,)), dma((11,)), dma((11,)), dma((11,)), dma((n - 1,)), dma((n - 1,)), dma((2, n - 1)), dma((2, n - 1)), dma((4,)),
        ],
        compiler_params=pltpu.CompilerParams(collective_id=1, has_side_effects=True, vmem_limit_bytes=VMEM_MAX),
        name="step",
    )(coef, *embs, *gus, *downs, crow, ccol, g1, g2)


def solution(mesh):
    def device_step(tok_ids, tok_labels, loss_mask, emb, g1, g2, w_gate, w_up, w_down):
        n = N_DEV
        rows, width = emb.shape
        vocab = rows * n
        n_tok = tok_ids.shape[0]
        me = lax.axis_index("fsdp")

        def send(bit):
            pairs = [(d, d ^ bit) for d in range(n)]
            return lambda val: lax.ppermute(val, "fsdp", pairs)

        along_x, along_y = send(2), send(4)
        gu = slice_weights(w_gate, w_up)
        gus, downs = [[val, along_x(val), along_y(val)] for val in (gu, w_down)]

        live = loss_mask != 0
        by_id = lax.sort(jnp.where(live, tok_ids * 65536 + tok_labels, vocab * 65536), is_stable=False)
        by_label = lax.sort(jnp.where(live, tok_labels * 65536 + tok_ids, vocab * 65536), is_stable=False)
        tok = [part.reshape(n_tok // 128, 128) for part in (by_id >> 16, by_id & 65535, by_label >> 16, by_label & 65535)]
        tok = gather_tokens(jnp.concatenate(tok).astype(jnp.int16))
        tok, gus[2], downs[1], emb_later = lax.optimization_barrier((tok, gus[2], downs[1], emb))
        embs = [emb, along_x(emb_later), along_y(emb_later)]
        gus.append(along_x(gus[2]))
        downs.append(along_y(downs[1]))
        ids, labels, labels2, ids2 = [tok[:, k * (n_tok // 128):(k + 1) * (n_tok // 128)].astype(I32) for k in range(4)]
        crow, ccol = count([(ids, labels), (labels2, ids2)], me * rows, rows, vocab)
        n_live = jnp.sum(ids < vocab).astype(F32)
        coef = (1.0 / n_live).reshape(1, 1)
        loss, *grads = run_step(coef, embs, gus, downs, crow, ccol, g1.reshape(1, width), g2.reshape(1, width))
        return (loss[0, 0], *finish(*grads))

    row_spec = P("fsdp", None)
    tok_spec = P("fsdp")
    return jax.shard_map(device_step, mesh=mesh, in_specs=(tok_spec, tok_spec, tok_spec, row_spec, P(), P(), row_spec, row_spec, row_spec), out_specs=(P(), row_spec, row_spec, row_spec, row_spec), check_vma=False)
```

```python
import functools

import jax
import jax.numpy as jnp
from jax import lax
from jax.experimental import pallas as pl
from jax.experimental.pallas import tpu as pltpu
from jax.sharding import PartitionSpec as P


NORM_EPS = 1e-6
N_DEV = 8
F32, BF16, I32 = jnp.float32, jnp.bfloat16, jnp.int32
MESH = pl.DeviceIdType.MESH
VMEM_MAX = 66_000_000
VMEM_ALL = 67_000_000


class Phases:
    def __init__(self):
        self.now = None

    def __call__(self, name=None):
        if self.now is not None:
            self.now.__exit__(None, None, None)
        self.now = jax.named_scope(name) if name else None
        if self.now is not None:
            self.now.__enter__()


def dot_nn(a, b):
    return jnp.dot(a, b, preferred_element_type=F32)


def dot_nt(a, b):
    return lax.dot_general(a, b, (((1,), (1,)), ((), ())), preferred_element_type=F32)


def dot_tn(a, b):
    return lax.dot_general(a, b, (((0,), (0,)), ((), ())), preferred_element_type=F32)


def flip(me, bit):
    return me + bit - 2 * bit * lax.rem(me // bit, 2)


def barrier_with(peers):
    sem = pltpu.get_barrier_semaphore()
    for peer in peers:
        pl.semaphore_signal(sem, inc=1, device_id=(peer,), device_id_type=MESH)
    pl.semaphore_wait(sem, len(peers))


class Gather:
    def __init__(self, slot, half, send_sem, recv_sem, me):
        self.slot, self.half, self.ss, self.rs, self.me = slot, half, send_sem, recv_sem, me
        self.pc, self.px, self.py = flip(me, 1), flip(me, 2), flip(me, 4)
        self.pd = flip(self.px, 4)

    def copy(self, kind, src, dst, peer):
        return pltpu.make_async_remote_copy(
            src_ref=src, dst_ref=dst, send_sem=self.ss(kind), recv_sem=self.rs(kind), device_id=(peer,), device_id_type=MESH
        )

    def describe(self, kind):
        me, px, py, pd, pc = self.me, self.px, self.py, self.pd, self.pc
        if kind in (0, 9):
            return self.copy(kind, self.half(me, kind // 9), self.half(me, kind // 9), px)
        if kind in (1, 10):
            return self.copy(kind, self.half(me, 1 - kind // 10), self.half(me, 1 - kind // 10), py)
        if kind == 2:
            return self.copy(2, self.half(px, 0), self.half(px, 0), py)
        if kind == 3:
            return self.copy(3, self.half(py, 1), self.half(py, 1), px)
        if kind == 4:
            return self.copy(4, self.slot(me), self.slot(me), pc)
        if kind == 5:
            return self.copy(5, self.slot(px), self.slot(px), pc)
        if kind == 6:
            return self.copy(6, self.slot(py), self.slot(py), pc)
        return self.copy(kind, self.half(pd, kind - 7), self.half(pd, kind - 7), pc)

    def start(self):
        for kind in (0, 1, 9, 10, 4):
            self.describe(kind).start()

    def forward_pair(self):
        for kind in (0, 1):
            self.describe(9 + kind).wait_recv()
            self.describe(5 + kind).start()

    def forward_cross(self, wait=True):
        for kind in (0, 1):
            if wait:
                self.describe(kind).wait_recv()
            self.describe(2 + kind).start()

    def forward_far(self):
        self.describe(2).wait_recv()
        self.describe(7).start()
        self.describe(3).wait_recv()
        self.describe(8).start()

    def wait_recv(self, *kinds):
        for kind in kinds:
            self.describe(kind).wait_recv()

    def wait_sends(self, *kinds):
        for kind in kinds or range(11):
            self.describe(kind).wait_send()


def slice_kernel(gate, up, out):
    n, _, fs = out.shape
    rows = gate.shape[0]
    for k in range(n):
        out[k, 0:rows, :] = gate[:, k * fs:(k + 1) * fs]
        out[k, rows:2 * rows, :] = up[:, k * fs:(k + 1) * fs]


def slice_weights(gate, up):
    rows, width = gate.shape
    return pl.pallas_call(
        slice_kernel,
        out_shape=jax.ShapeDtypeStruct((N_DEV, 2 * rows, width // N_DEV), gate.dtype),
        cost_estimate=pl.CostEstimate(flops=1_000_000, bytes_accessed=1_000_000, transcendentals=0),
        name="slices",
    )(gate, up)


def token_kernel(tok, tok_o, send_sem, recv_sem, local_sem):
    me = lax.axis_index("fsdp")
    n = tok_o.shape[0]
    peers = [lax.rem(me + k, n) for k in range(1, n)]
    barrier_with(peers)
    copies = [
        pltpu.make_async_remote_copy(
            src_ref=tok, dst_ref=tok_o.at[me], send_sem=send_sem.at[k], recv_sem=recv_sem.at[k], device_id=(peer,), device_id_type=MESH
        )
        for k, peer in enumerate(peers)
    ]
    local = pltpu.make_async_copy(tok, tok_o.at[me], local_sem)
    for copy in copies:
        copy.start()
    local.start()
    for copy in copies:
        copy.wait()
    local.wait()


def gather_tokens(tok):
    dma = pltpu.SemaphoreType.DMA
    return pl.pallas_call(
        token_kernel,
        out_shape=jax.ShapeDtypeStruct((N_DEV,) + tok.shape, tok.dtype),
        in_specs=[pl.BlockSpec(memory_space=pltpu.VMEM)],
        out_specs=pl.BlockSpec(memory_space=pl.ANY),
        scratch_shapes=[dma((N_DEV - 1,)), dma((N_DEV - 1,)), dma],
        compiler_params=pltpu.CompilerParams(collective_id=0, has_side_effects=True, vmem_limit_bytes=VMEM_ALL),
        cost_estimate=pl.CostEstimate(flops=5_000_000_000, bytes_accessed=1_000_000, transcendentals=0),
        name="tokens",
    )(tok)


def count_kernel(bounds, keys_a, keys_b, out_a, out_b, list_a, list_b, acc_a, acc_b, in_sem, out_sem):
    n_src = N_DEV
    per = list_a.shape[0] // n_src
    size = acc_a.shape[0]
    BLK = 256
    unroll = 8
    jobs = [(keys_a, out_a, list_a, acc_a), (keys_b, out_b, list_b, acc_b)]
    stores = [pltpu.make_async_copy(acc, out, out_sem.at[k]) for k, (_k, out, _h, acc) in enumerate(jobs)]
    PART = 1024

    def segment(which, src):
        both = bounds[which * n_src + src]
        return (both & 65535) + src * per, lax.shift_right_logical(both, 16) + src * per

    def fetch(src, run):
        for which, (keys, _o, held, _a) in enumerate(jobs):
            begin, end = segment(which, src)

            def one(t, _):
                at = pl.ds(pl.multiple_of(t * PART, PART), PART)
                run(pltpu.make_async_copy(keys.at[at], held.at[at], in_sem.at[which]))
                return 0

            lax.fori_loop(lax.shift_right_logical(begin, 10), jnp.where(begin < end, lax.shift_right_logical(end + PART - 1, 10), 0), one, 0)

    lax.fori_loop(0, n_src, lambda src, _: (fetch(src, lambda copy: copy.start()), 0)[1], 0)
    lanes = lax.broadcasted_iota(I32, (1, 128), 1)

    def clear(i, _):
        acc_a[pl.ds(i * BLK, BLK), :] = jnp.zeros((BLK, 128), F32)
        acc_b[pl.ds(i * BLK, BLK), :] = jnp.zeros((BLK, 128), F32)
        return 0

    lax.fori_loop(0, size // BLK, clear, 0)
    lax.fori_loop(0, n_src, lambda src, _: (fetch(src, lambda copy: copy.wait()), 0)[1], 0)

    def group(streams, whole):
        done = []
        for held, acc, pos, end in streams:
            places, vals, delta = [], [], None
            for k in range(unroll):
                key = held[pos + k] if whole else held[jnp.minimum(pos + k, end - 1)]
                places.append(key >> 7)
                spread = jnp.full((1, 128), key, I32)
                here = jnp.where(lanes == (spread & 127), 1.0 if whole else jnp.where(pos + k < end, 1.0, 0.0), 0.0)
                delta = here if k == 0 else here + jnp.where((spread ^ before) < 128, delta, 0.0)
                before = spread
                vals.append(acc[pl.ds(places[k], 1), :] + delta)
            done.append((acc, places, vals))
        for acc, places, vals in done:
            for place, val in zip(places, vals):
                acc[pl.ds(place, 1), :] = val

    def source(src, _):
        ranges = []
        for which, (_k, _o, held, acc) in enumerate(jobs):
            begin, end = segment(which, src)
            ranges.append((held, acc, begin, end, lax.shift_right_logical(end - begin, 3)))
        both = jnp.minimum(ranges[0][4], ranges[1][4])

        def step(i, _):
            group([(held, acc, begin + i * unroll, end) for held, acc, begin, end, _n in ranges], True)
            return 0

        lax.fori_loop(0, both, step, 0)
        for held, acc, begin, end, n_whole in ranges:
            def rest(i, _):
                group([(held, acc, begin + i * unroll, end)], True)
                return 0

            lax.fori_loop(both, n_whole, rest, 0)

            @pl.when(begin + n_whole * unroll < end)
            def _():
                group([(held, acc, begin + n_whole * unroll, end)], False)

        return 0

    lax.fori_loop(0, n_src, source, 0)
    for store in stores:
        store.start()
    for store in stores:
        store.wait()


def count(pairs, first, rows, cols):
    bounds, keys, tiles = [], [], cols // 128
    for major, minor in pairs:
        bounds.append(jnp.sum(jnp.where(major < first, 1, 0) + jnp.where(major < first + rows, 65536, 0), axis=(1, 2), dtype=I32))
        row = major - first
        keys.append(((((row >> 3) * tiles + (minor >> 7)) * 8 + (row & 7)) * 128 + (minor & 127)).reshape(-1))
    any_spec = pl.BlockSpec(memory_space=pl.ANY)
    tall = (rows * cols // 128, 128)
    outs = pl.pallas_call(
        count_kernel,
        out_shape=(jax.ShapeDtypeStruct(tall, F32),) * 2,
        in_specs=[pl.BlockSpec(memory_space=pltpu.SMEM), any_spec, any_spec],
        out_specs=(any_spec,) * 2,
        scratch_shapes=[pltpu.SMEM(keys[0].shape, I32)] * 2 + [pltpu.VMEM(tall, F32)] * 2 + [pltpu.SemaphoreType.DMA((2,))] * 2,
        compiler_params=pltpu.CompilerParams(vmem_limit_bytes=VMEM_ALL),
        cost_estimate=pl.CostEstimate(flops=30_000_000_000, bytes_accessed=16_000_000, transcendentals=0),
        name="count",
    )(jnp.concatenate(bounds), *keys)
    return [out.reshape(rows // 8, tiles, 8, 128) for out in outs]


def finish_kernel(de, got_g, got_u, dwd, de_o, dwg_o, dwu_o, dwd_o, de_v, g_v, u_v, dwd_v, wg_v, wu_v, in_sem, out_sem):
    n, _, fs = g_v.shape
    ins = [pltpu.make_async_copy(src, dst, in_sem.at[k]) for k, (src, dst) in enumerate([(got_g, g_v), (got_u, u_v), (de, de_v), (dwd, dwd_v)])]
    outs = [pltpu.make_async_copy(src, dst, out_sem.at[k]) for k, (src, dst) in enumerate([(wg_v, dwg_o), (wu_v, dwu_o), (de_v, de_o), (dwd_v, dwd_o)])]
    for copy in ins:
        copy.start()
    for which, (src, dst) in enumerate([(g_v, wg_v), (u_v, wu_v)]):
        ins[which].wait()
        for k in range(n):
            dst[:, k * fs:(k + 1) * fs] = src[k]
        if which == 1:
            outs[0].start()
    for which in (2, 3):
        ins[which].wait()
        outs[which].start()
    outs[1].start()
    for copy in outs:
        copy.wait()


def finish(de, got_g, got_u, dwd):
    n, out_rows, fs = got_g.shape
    wide = jax.ShapeDtypeStruct((out_rows, n * fs), F32)
    any_spec = pl.BlockSpec(memory_space=pl.ANY)
    held = [pltpu.VMEM(val.shape, F32) for val in (de, got_g, got_u, dwd, wide, wide)]
    return pl.pallas_call(
        finish_kernel,
        out_shape=(jax.ShapeDtypeStruct(de.shape, F32), wide, wide, jax.ShapeDtypeStruct(dwd.shape, F32)),
        in_specs=[any_spec] * 4,
        out_specs=(any_spec,) * 4,
        scratch_shapes=held + [pltpu.SemaphoreType.DMA((4,)), pltpu.SemaphoreType.DMA((4,))],
        compiler_params=pltpu.CompilerParams(vmem_limit_bytes=VMEM_ALL),
        name="finish",
    )(de, got_g, got_u, dwd)


def step_kernel(
    coef_ref, emb_me, emb_x, emb_y, gu_me, gu_x, gu_y, gu_d, wd_me, wd_x, wd_y, wd_d, crow_hbm, ccol_hbm, g1_ref, g2_ref,
    loss_o, de_out, got_g, got_u, dwd_out,
    de_o, dwd_o, emb, wg, wu, wd, cnt, hn, dh, a_all, p_own, q_own, q_all, logits, dlog, h_wide, acc, stat, stat_col, top, sums,
    dwg, dwu, load_sem, pair_s, pair_r, es, er, hs, hr, ds_, dr, st_s, st_r, ws, wr, out_sem,
):
    me = lax.axis_index("fsdp")
    n = wg.shape[0]
    rows, width = h_wide.shape
    fs = wg.shape[2]
    out_rows = got_g.shape[1]
    coef = coef_ref[0, 0]
    ph = Phases()
    ph("a_start")
    NB = 128
    RB = 64
    wide = logits.shape[2]
    tiles = wide // 128
    peers = [lax.rem(me + k, n) for k in range(1, n)]

    def block(dev):
        return pl.ds(pl.multiple_of(dev * rows, rows), rows)

    def p_at(s):
        return (slice(None), pl.ds(pl.multiple_of(2 * rows + s * 256, 256), fs))

    mine = block(me)
    pc, px, py = flip(me, 1), flip(me, 2), flip(me, 4)
    pd = flip(px, 4)
    devs = [me, px, py, pd]
    parts = []
    waves = []
    for dev, down in zip(devs, [wd_me, wd_x, wd_y, wd_d]):
        low = dev - lax.rem(dev, 2)
        part = pl.ds(low, 2)
        parts.append((down, wd.at[dev]))
        for owner, gu in zip(devs, [gu_me, gu_x, gu_y, gu_d]):
            at = pl.ds(owner * out_rows, out_rows)
            parts.append((gu.at[part, 0:out_rows, :], wg.at[part, at, :]))
            parts.append((gu.at[part, out_rows:2 * out_rows, :], wu.at[part, at, :]))
        waves.append((low, len(parts)))
    n_weight = len(parts)
    for dev, part in zip(devs, [emb_me, emb_x, emb_y]):
        parts.append((part, emb.at[block(dev), :]))
    loads = [pltpu.make_async_copy(src, dst, load_sem.at[k]) for k, (src, dst) in enumerate(parts)]
    pairs = [
        pltpu.make_async_remote_copy(
            src_ref=src, dst_ref=dst, send_sem=pair_s.at[k], recv_sem=pair_r.at[k], device_id=(pc,), device_id_type=MESH
        )
        for k, (src, dst) in enumerate(parts)
    ]
    row_counts = pltpu.make_async_copy(crow_hbm, cnt, load_sem.at[len(parts)])
    col_counts = pltpu.make_async_copy(ccol_hbm, cnt, load_sem.at[len(parts) + 1])

    barrier = pltpu.get_barrier_semaphore()
    for peer in peers:
        pl.semaphore_signal(barrier, inc=1, device_id=(peer,), device_id_type=MESH)
    for load in loads[n_weight:] + loads[:n_weight]:
        load.start()
    def gather_of(buf, ss, rs):
        half = rows // 2
        return Gather(
            lambda d: buf.at[block(d), :],
            lambda d, i: buf.at[pl.ds(pl.multiple_of(d * rows + i * half, half), half), :],
            lambda c: ss.at[c], lambda c: rs.at[c], me,
        )

    emb_g, hn_g, dh_g = gather_of(emb, es, er), gather_of(hn, hs, hr), gather_of(dh, ds_, dr)
    g1, g2 = g1_ref[...], g2_ref[...]

    ph("d_norm")

    def norm_rows(dev):
        def norm(i, _):
            at = pl.ds(pl.multiple_of(dev * rows + i * NB, NB), NB)
            x = emb[at, :].astype(F32)
            inv = lax.rsqrt(jnp.mean(x * x, axis=-1, keepdims=True) + NORM_EPS)
            a_all[at, :] = (x * inv * g1).astype(BF16)
            return 0

        lax.fori_loop(0, rows // NB, norm, 0, unroll=2)

    for load in loads[n_weight:]:
        load.wait()
    norm_rows(me)
    ph("b_barrier")
    pl.semaphore_wait(barrier, len(peers))
    for pair in pairs:
        pair.start()
    emb_g.forward_cross(wait=False)
    row_counts.start()
    norm_rows(px)
    norm_rows(py)

    ph("e_waitW")
    def weights_here(first, last):
        for load, pair in zip(loads[first:last], pairs[first:last]):
            load.wait()
            pair.wait_recv()

    acc[...] = jnp.zeros_like(acc)

    def forward(j, _):
        a = a_all[mine, :]
        p = dot_nn(a, wg[j]).astype(BF16)
        q = dot_nn(a, wu[j]).astype(BF16)
        p_own[j], q_own[j] = p, q
        p, q = p.astype(F32), q.astype(F32)
        u = (p * jax.nn.sigmoid(p) * q).astype(BF16)
        acc[...] += dot_nn(u, wd[j])
        return 0

    first = 0
    for k, (low, last) in enumerate(waves):
        weights_here(first, last)
        first = last
        forward(low, 0)
        forward(low + 1, 0)
        if k == 2:
            emb_g.forward_far()
    ph("g_hidden")

    def hidden(i, _):
        at = pl.ds(pl.multiple_of(i * NB, NB), NB)
        row = pl.ds(pl.multiple_of(me * rows + i * NB, NB), NB)
        h = (emb[row, :].astype(F32) + acc[at, :]).astype(BF16).astype(F32)
        h_wide[at, :] = h
        inv = lax.rsqrt(jnp.mean(h * h, axis=-1, keepdims=True) + NORM_EPS)
        hn[row, :] = (h * inv * g2).astype(BF16)
        return 0

    lax.fori_loop(0, rows // NB, hidden, 0, unroll=2)
    hn_g.start()
    ph("h_waitE")
    for pair in pairs[n_weight:]:
        pair.wait_recv()
    emb_g.wait_recv(7, 8)

    ph("i_logit")
    top[...] = jnp.full_like(top, -jnp.inf)

    def logit(v, _):
        val = dot_nt(hn[mine, :], emb[pl.ds(pl.multiple_of(v * wide, wide), wide), :])
        logits[v] = val
        m = top[...]
        for k in range(tiles):
            m = jnp.maximum(m, val[:, k * 128:(k + 1) * 128])
        top[...] = m
        return 0

    lax.fori_loop(0, n * rows // wide, logit, 0, unroll=2)
    row_counts.wait()
    ph("j_softmax")
    top[...] = jnp.max(top[...], axis=-1, keepdims=True) + jnp.zeros((rows, 128), F32)

    def counts(i, v, k):
        return cnt[pl.ds(i * (RB // 8), RB // 8), v * tiles + k].reshape(RB, 128)

    def total(i, _):
        at = pl.ds(pl.multiple_of(i * RB, RB), RB)
        m = top[at, :]

        def part(v, carry):
            s, c, pick = carry
            for k in range(tiles):
                cut = slice(k * 128, (k + 1) * 128)
                val, num = logits[v, at, cut], counts(i, v, k)
                ex = jnp.exp(val - m)
                logits[v, at, cut] = ex
                s, c, pick = s + ex, c + num, pick + num * val
            return s, c, pick

        zero = jnp.zeros((RB, 128), F32)
        sums[0, at, :], sums[1, at, :], sums[2, at, :] = lax.fori_loop(0, n * rows // wide, part, (zero, zero, zero))
        return 0

    lax.fori_loop(0, rows // RB, total, 0)
    s, c, pick = [jnp.sum(sums[k], axis=-1, keepdims=True) for k in range(3)]
    lse = top[:, 0:1] + jnp.log(s)
    lane = lax.broadcasted_iota(I32, (rows, 128), 1)
    stat_col[...] = jnp.where(lane == 0, lse, jnp.where(lane == 1, c * coef, jnp.where(lane == 2, c * lse - pick, 0.0)))
    sums[0] = c * coef / s + jnp.zeros((rows, 128), F32)

    stat[me] = jnp.transpose(stat_col[...])[0:8, :]
    ph("k_dhn")
    for v in range(n * rows // wide):
        for k in range(tiles):
            here = slice(v * wide + k * 128, v * wide + (k + 1) * 128)
            num = cnt[:, v * tiles + k].reshape(rows, 128)
            dlog[:, here] = (logits[v, :, k * 128:(k + 1) * 128] * sums[0] - num * coef).astype(BF16)
        here = slice(v * wide, (v + 1) * wide)
        part = dot_nn(dlog[:, here], emb[here, :])
        acc[...] = part if v == 0 else acc[...] + part
    col_counts.start()
    stat_copies = [
        pltpu.make_async_remote_copy(
            src_ref=stat.at[me], dst_ref=stat.at[me], send_sem=st_s.at[k], recv_sem=st_r.at[k], device_id=(peer,), device_id_type=MESH
        )
        for k, peer in enumerate(peers)
    ]
    for copy in stat_copies:
        copy.start()
    ph("l_dhidden")

    def dhidden(i, _):
        at = pl.ds(pl.multiple_of(i * NB, NB), NB)
        h, scaled = h_wide[at, :], acc[at, :] * g2
        inv = lax.rsqrt(jnp.mean(h * h, axis=-1, keepdims=True) + NORM_EPS)
        grad = inv * (scaled - h * (inv * inv) * jnp.mean(scaled * h, axis=-1, keepdims=True))
        de_o[at, :] = grad
        dh[pl.ds(pl.multiple_of(me * rows + i * NB, NB), NB), :] = grad.astype(BF16)
        return 0

    lax.fori_loop(0, rows // NB, dhidden, 0, unroll=2)
    dh_g.start()

    ph("n_norm")
    for dev in [pd] + [flip(dev, 1) for dev in devs]:
        norm_rows(dev)
    ph("o_slice")

    def slice_forward(s, _):
        a = a_all[block(s), :]
        dlog[p_at(s)] = dot_nn(a, wg[me]).astype(BF16)
        q_all[s] = dot_nn(a, wu[me]).astype(BF16)
        return 0

    lax.fori_loop(0, n, slice_forward, 0, unroll=2)

    ph("m_hnnear")
    hn_g.wait_recv(0, 1)
    hn_g.forward_pair()

    ph("p_back")
    acc[...] = jnp.zeros_like(acc)

    def act_back(dact, p, q):
        sig = jax.nn.sigmoid(p)
        gated = p * sig
        dq = (dact * gated).astype(BF16)
        dp = (dact * q * sig * (1.0 + p * (1.0 - sig))).astype(BF16)
        return dp, dq, (gated * q).astype(BF16)

    def backward(j, _):
        dact = dot_nt(dh[mine, :], wd[j])
        dp, dq, _u = act_back(dact, p_own[j].astype(F32), q_own[j].astype(F32))
        acc[...] += dot_nt(dp, wg[j]) + dot_nt(dq, wu[j])
        return 0

    lax.fori_loop(0, n, backward, 0, unroll=2)
    dh_g.forward_cross()
    ph("q_dinput")

    def dinput(i, _):
        at = pl.ds(pl.multiple_of(i * NB, NB), NB)
        x, scaled = emb[pl.ds(pl.multiple_of(me * rows + i * NB, NB), NB), :].astype(F32), acc[at, :] * g1
        inv = lax.rsqrt(jnp.mean(x * x, axis=-1, keepdims=True) + NORM_EPS)
        de_o[at, :] += inv * (scaled - x * (inv * inv) * jnp.mean(scaled * x, axis=-1, keepdims=True))
        return 0

    lax.fori_loop(0, rows // NB, dinput, 0, unroll=2)
    ph("r_stat")
    for copy in stat_copies:
        copy.wait_recv()
    col_counts.wait()

    def head(dev):
        low = dev - lax.rem(dev, 2)
        pair = pl.ds(pl.multiple_of(low * rows, 2 * rows), 2 * rows)
        for k in range(2 * rows // 256):
            source, cut = low + k * 256 // rows, slice(k * 256 % rows, k * 256 % rows + 256)
            lt = dot_nt(emb[mine, :], hn[pl.ds(pl.multiple_of(low * rows + k * 256, 256), 256), :])
            tile = low * (rows // 128) + 2 * k
            num = jnp.concatenate([cnt[:, tile].reshape(rows, 128), cnt[:, tile + 1].reshape(rows, 128)], axis=1)
            prob = jnp.exp(lt - stat[source, 0:1, cut]) * stat[source, 1:2, cut]
            dlog[:, k * 256:(k + 1) * 256] = (prob - num * coef).astype(BF16)
        de_o[...] += dot_nn(dlog[:, 0:2 * rows], hn[pair, :])

    dwg[...] = jnp.zeros_like(dwg)
    dwu[...] = jnp.zeros_like(dwu)
    dwd_o[...] = jnp.zeros_like(dwd_o)

    def act_grads(dev):
        dact = dot_nt(dh[block(dev), :], wd[me])
        return act_back(dact, dlog[p_at(dev)].astype(F32), q_all[dev].astype(F32))

    def weights(dev):
        dp, dq, u = act_grads(dev)
        dwd_o[...] += dot_tn(u, dh[block(dev), :])
        dwg[...] += dot_tn(a_all[block(dev), :], dp)
        dwu[...] += dot_tn(a_all[block(dev), :], dq)

    def exchange(k, peer, src, dst, row):
        return pltpu.make_async_remote_copy(
            src_ref=src.at[pl.ds(pl.multiple_of(peer * out_rows, out_rows), out_rows), :],
            dst_ref=dst.at[me],
            send_sem=ws.at[row, k], recv_sem=wr.at[row, k], device_id=(peer,), device_id_type=MESH,
        )

    swaps_g = [exchange(k, peer, dwg, got_g, 0) for k, peer in enumerate(peers)]
    swaps_u = [exchange(k, peer, dwu, got_u, 1) for k, peer in enumerate(peers)]

    ph("s_w01")
    dh_g.wait_recv(4)
    weights(me)
    weights(pc)
    ph("t_dhnear")
    dh_g.forward_pair()
    hn_g.forward_cross(wait=False)
    ph("u_w23")
    weights(px)
    weights(py)
    ph("v_w45")
    dh_g.wait_recv(5, 6)
    weights(flip(px, 1))
    weights(flip(py, 1))
    ph("w_heads")
    hn_g.wait_recv(4, 5)
    head(me)
    head(px)
    ph("x_dhfar")
    dh_g.forward_far()
    ph("y_late")
    late = [pd, flip(pd, 1)]
    for k, kinds in ((0, ()), (1, (7, 8))):
        dh_g.wait_recv(*kinds)
        dev = late[k]
        dlog[p_at(dev)], q_all[dev], dlog[p_at(n + k)] = act_grads(dev)
        dwg[...] += dot_tn(a_all[block(dev), :], dlog[p_at(dev)])
    for swap in swaps_g:
        swap.start()
    for dev in late:
        dwu[...] += dot_tn(a_all[block(dev), :], q_all[dev])
    for swap in swaps_u:
        swap.start()
    keep = pl.ds(pl.multiple_of(me * out_rows, out_rows), out_rows)
    outs = [pltpu.make_async_copy(dwg.at[keep, :], got_g.at[me], out_sem.at[0]), pltpu.make_async_copy(dwu.at[keep, :], got_u.at[me], out_sem.at[1])]
    for out in outs:
        out.start()
    for k, dev in enumerate(late):
        dwd_o[...] += dot_tn(dlog[p_at(n + k)], dh[block(dev), :])
    ph("z_hnfar")
    hn_g.wait_recv(6)
    head(py)
    hn_g.forward_far()
    outs.append(pltpu.make_async_copy(dwd_o, dwd_out, out_sem.at[2]))
    outs[-1].start()
    hn_g.wait_recv(7, 8)
    ph("za_head")
    head(pd)
    outs.append(pltpu.make_async_copy(de_o, de_out, out_sem.at[3]))
    outs[-1].start()
    total_loss = jnp.zeros((1, rows), F32)
    for s in range(n):
        total_loss = total_loss + stat[s, 2:3, :]
    loss_o[...] = jnp.sum(total_loss, axis=-1, keepdims=True) * coef + jnp.zeros((1, 128), F32)
    ph("zd_waits")
    for copy in stat_copies:
        copy.wait_send()
    emb_g.wait_sends(2, 3, 7, 8)
    hn_g.wait_sends()
    dh_g.wait_sends()
    for pair in pairs:
        pair.wait_send()
    for out in outs:
        out.wait()
    for swap in swaps_g + swaps_u:
        swap.wait()
    ph()


def run_step(coef, embs, gus, downs, crow, ccol, g1, g2):
    n = N_DEV
    rows, width = embs[0].shape
    fs = gus[0].shape[2]
    out_rows = width // n
    any_spec = pl.BlockSpec(memory_space=pl.ANY)
    vmem = pl.BlockSpec(memory_space=pltpu.VMEM)
    dma = pltpu.SemaphoreType.DMA
    return pl.pallas_call(
        step_kernel,
        out_shape=(
            jax.ShapeDtypeStruct((1, 128), F32),
            jax.ShapeDtypeStruct((rows, width), F32),
            jax.ShapeDtypeStruct((n, out_rows, fs), F32),
            jax.ShapeDtypeStruct((n, out_rows, fs), F32),
            jax.ShapeDtypeStruct((fs, width), F32),
        ),
        in_specs=[pl.BlockSpec(memory_space=pltpu.SMEM)] + [any_spec] * 13 + [vmem] * 2,
        out_specs=(vmem,) + (any_spec,) * 4,
        scratch_shapes=[
            pltpu.VMEM((rows, width), F32),
            pltpu.VMEM((fs, width), F32),
            pltpu.VMEM((n * rows, width), BF16),
            pltpu.VMEM((n, width, fs), BF16),
            pltpu.VMEM((n, width, fs), BF16),
            pltpu.VMEM((n, fs, width), BF16),
            pltpu.VMEM((rows // 8, n * rows // 128, 8, 128), F32),
            pltpu.VMEM((n * rows, width), BF16),
            pltpu.VMEM((n * rows, width), BF16),
            pltpu.VMEM((n * rows, width), BF16),
            pltpu.VMEM((n, rows, fs), BF16),
            pltpu.VMEM((n, rows, fs), BF16),
            pltpu.VMEM((n, rows, fs), BF16),
            pltpu.VMEM((n // 2, rows, 2 * rows), F32),
            pltpu.VMEM((rows, n * rows), BF16),
            pltpu.VMEM((rows, width), F32),
            pltpu.VMEM((rows, width), F32),
            pltpu.VMEM((n, 8, rows), F32),
            pltpu.VMEM((rows, 128), F32),
            pltpu.VMEM((rows, 128), F32),
            pltpu.VMEM((3, rows, 128), F32),
            pltpu.VMEM((width, fs), F32),
            pltpu.VMEM((width, fs), F32),
            dma((41,)), dma((39,)), dma((39,)), dma((11,)), dma((11,)), dma((11,)), dma((11,)), dma((11,)), dma((11,)), dma((n - 1,)), dma((n - 1,)), dma((2, n - 1)), dma((2, n - 1)), dma((4,)),
        ],
        compiler_params=pltpu.CompilerParams(collective_id=1, has_side_effects=True, vmem_limit_bytes=VMEM_MAX),
        name="step",
    )(coef, *embs, *gus, *downs, crow, ccol, g1, g2)


def solution(mesh):
    def device_step(tok_ids, tok_labels, loss_mask, emb, g1, g2, w_gate, w_up, w_down):
        n = N_DEV
        rows, width = emb.shape
        vocab = rows * n
        n_tok = tok_ids.shape[0]
        me = lax.axis_index("fsdp")

        def send(bit):
            pairs = [(d, d ^ bit) for d in range(n)]
            return lambda val: lax.ppermute(val, "fsdp", pairs)

        along_x, along_y = send(2), send(4)
        gu = slice_weights(w_gate, w_up)
        gus, downs = [[val, along_x(val), along_y(val)] for val in (gu, w_down)]

        live = loss_mask != 0
        by_id = lax.sort(jnp.where(live, tok_ids * 65536 + tok_labels, vocab * 65536), is_stable=False)
        by_label = lax.sort(jnp.where(live, tok_labels * 65536 + tok_ids, vocab * 65536), is_stable=False)
        tok = [part.reshape(n_tok // 128, 128) for part in (by_id >> 16, by_id & 65535, by_label >> 16, by_label & 65535)]
        tok = gather_tokens(jnp.concatenate(tok).astype(jnp.int16))
        tok, gus[2], downs[1], emb_later = lax.optimization_barrier((tok, gus[2], downs[1], emb))
        embs = [emb, along_x(emb_later), along_y(emb_later)]
        gus.append(along_x(gus[2]))
        downs.append(along_y(downs[1]))
        ids, labels, labels2, ids2 = [tok[:, k * (n_tok // 128):(k + 1) * (n_tok // 128)].astype(I32) for k in range(4)]
        crow, ccol = count([(ids, labels), (labels2, ids2)], me * rows, rows, vocab)
        n_live = jnp.sum(ids < vocab).astype(F32)
        coef = (1.0 / n_live).reshape(1, 1)
        loss, *grads = run_step(coef, embs, gus, downs, crow, ccol, g1.reshape(1, width), g2.reshape(1, width))
        return (loss[0, 0], *finish(*grads))

    row_spec = P("fsdp", None)
    tok_spec = P("fsdp")
    return jax.shard_map(device_step, mesh=mesh, in_specs=(tok_spec, tok_spec, tok_spec, row_spec, P(), P(), row_spec, row_spec, row_spec), out_specs=(P(), row_spec, row_spec, row_spec, row_spec), check_vma=False)
```
